32 devices in a mesh: dp: 1 (over z), tp: 4 (over y), pp: 8 (over x, core).
Axes of the slice: x: 4, y: 4, z: 1, core: 2. Of those that a mesh axis runs over, the one named last changes fastest.
The devices are a block of a 4x4x8 slice.
Arguments:
- x_in: bfloat16 [16, 8, 128, 1024], P(None, 'dp', 'tp')
- ln_params: float32 [8, 4, 1024], P('pp')
- w_q: bfloat16 [8, 1024, 16, 1, 64], P('pp', None, 'tp')
- w_k: bfloat16 [8, 1024, 16, 64], P('pp', None, 'tp')
- w_v: bfloat16 [8, 1024, 16, 64], P('pp', None, 'tp')
- w_o: bfloat16 [8, 16, 1, 64, 1024], P('pp', 'tp')
- w_up: bfloat16 [8, 1024, 4096], P('pp', None, 'tp')
- w_down: bfloat16 [8, 4096, 1024], P('pp', 'tp')
Outputs:
- output: bfloat16 [8, 16, 8, 128, 1024], P('pp', None, 'dp', 'tp')
All inputs are finite; a program needn't handle non-finite values.
Results may differ from the reference program's by a relative error of at most 0.02.
Values are sent between devices in bfloat16 or wider.
A program may use at most 768 MiB of HBM per device.

```python
import jax
import jax.numpy as jnp
from jax import lax

STAGES = 8
MICRO_BATCHES = 16
BATCH_SIZE = 8
SEQ_LEN = 128
D_MODEL = 1024
NUM_HEADS = 16
KV_COUNT = 16
HEAD_DIM = 64
FF_DIM = 4096

GROUP_SIZE = NUM_HEADS // KV_COUNT
LN_EPS = 1e-5
ROPE_BASE = 10000.0


def setup_inputs(seed: int = 0, part: int = 0) -> dict:
    rng_keys = jax.random.split(jax.random.key(seed), 8)
    x_key = jax.random.fold_in(rng_keys[0], part)
    x_in = jax.random.normal(x_key, (MICRO_BATCHES, BATCH_SIZE, SEQ_LEN, D_MODEL), jnp.float32)
    ln_offset = jnp.array([1.0, 0.0, 1.0, 0.0], jnp.float32)[None, :, None]
    ln_params = ln_offset + 0.5 * jax.random.normal(rng_keys[1], (STAGES, 4, D_MODEL), jnp.float32)
    in_scale = D_MODEL ** -0.5
    w_q = (1.25 * in_scale) * jax.random.normal(rng_keys[2], (STAGES, D_MODEL, KV_COUNT, GROUP_SIZE, HEAD_DIM), jnp.float32)
    w_k = (1.25 * in_scale) * jax.random.normal(rng_keys[3], (STAGES, D_MODEL, KV_COUNT, HEAD_DIM), jnp.float32)
    w_v = in_scale * jax.random.normal(rng_keys[4], (STAGES, D_MODEL, KV_COUNT, HEAD_DIM), jnp.float32)
    w_o = (3.0 * (NUM_HEADS * HEAD_DIM) ** -0.5) * jax.random.normal(rng_keys[5], (STAGES, KV_COUNT, GROUP_SIZE, HEAD_DIM, D_MODEL), jnp.float32)
    w_up = in_scale * jax.random.normal(rng_keys[6], (STAGES, D_MODEL, FF_DIM), jnp.float32)
    w_down = (FF_DIM ** -0.5) * jax.random.normal(rng_keys[7], (STAGES, FF_DIM, D_MODEL), jnp.float32)
    return {"x_in": x_in.astype(jnp.bfloat16), "ln_params": ln_params, "w_q": w_q.astype(jnp.bfloat16), "w_k": w_k.astype(jnp.bfloat16), "w_v": w_v.astype(jnp.bfloat16), "w_o": w_o.astype(jnp.bfloat16), "w_up": w_up.astype(jnp.bfloat16), "w_down": w_down.astype(jnp.bfloat16)}


def layer_norm(x_act, ln_gain, ln_bias):
    x_f32 = x_act.astype(jnp.float32)
    row_mean = jnp.mean(x_f32, axis=-1, keepdims=True)
    centred = x_f32 - row_mean
    variance = jnp.mean(centred * centred, axis=-1, keepdims=True)
    return (centred * lax.rsqrt(variance + LN_EPS) * ln_gain + ln_bias).astype(jnp.bfloat16)


def rope_tables():
    positions = jnp.arange(SEQ_LEN, dtype=jnp.float32)
    inv_freq = ROPE_BASE ** (-2.0 * jnp.arange(HEAD_DIM // 2, dtype=jnp.float32) / HEAD_DIM)
    angles = positions[:, None] * inv_freq[None, :]
    return jnp.cos(angles), jnp.sin(angles)


def apply_rope(proj, cos_tab, sin_tab):
    half_dim = HEAD_DIM // 2
    table_shape = (1, SEQ_LEN) + (1,) * (proj.ndim - 3) + (half_dim,)
    cos_bcast = cos_tab.reshape(table_shape)
    sin_bcast = sin_tab.reshape(table_shape)
    first_half = proj[..., :half_dim]
    second_half = proj[..., half_dim:]
    return jnp.concatenate([first_half * cos_bcast - second_half * sin_bcast, second_half * cos_bcast + first_half * sin_bcast], axis=-1)


def parallel_block(x_act, ln_par, w_q, w_k, w_v, w_o, w_up, w_down):
    num_rows = BATCH_SIZE * SEQ_LEN
    h_attn = layer_norm(x_act, ln_par[0], ln_par[1]).reshape(num_rows, D_MODEL)
    h_mlp = layer_norm(x_act, ln_par[2], ln_par[3]).reshape(num_rows, D_MODEL)
    cos_tab, sin_tab = rope_tables()
    q_proj = jnp.dot(h_attn, w_q.reshape(D_MODEL, NUM_HEADS * HEAD_DIM), preferred_element_type=jnp.float32)
    q_proj = apply_rope(q_proj.reshape(BATCH_SIZE, SEQ_LEN, KV_COUNT, GROUP_SIZE, HEAD_DIM), cos_tab, sin_tab).astype(jnp.bfloat16)
    k_proj = jnp.dot(h_attn, w_k.reshape(D_MODEL, KV_COUNT * HEAD_DIM), preferred_element_type=jnp.float32)
    k_proj = apply_rope(k_proj.reshape(BATCH_SIZE, SEQ_LEN, KV_COUNT, HEAD_DIM), cos_tab, sin_tab).astype(jnp.bfloat16)
    v_proj = jnp.dot(h_attn, w_v.reshape(D_MODEL, KV_COUNT * HEAD_DIM), preferred_element_type=jnp.float32).astype(jnp.bfloat16)
    v_proj = v_proj.reshape(BATCH_SIZE, SEQ_LEN, KV_COUNT, HEAD_DIM)
    allowed = jnp.arange(SEQ_LEN)[:, None, None] >= jnp.arange(SEQ_LEN)[None, None, :]

    def group_attention(operands):
        q_grp, k_grp, v_grp = operands
        scores = jnp.einsum("btgh,bsh->btgs", q_grp.astype(jnp.float32), k_grp.astype(jnp.float32)) * (HEAD_DIM ** -0.5)
        probs_bf = jax.nn.softmax(jnp.where(allowed, scores, -1e30), axis=-1).astype(jnp.bfloat16)
        return jnp.einsum("btgs,bsh->btgh", probs_bf.astype(jnp.float32), v_grp.astype(jnp.float32)).astype(jnp.bfloat16)

    context = lax.map(group_attention, (jnp.moveaxis(q_proj, 2, 0), jnp.moveaxis(k_proj, 2, 0), jnp.moveaxis(v_proj, 2, 0)))
    context = jnp.moveaxis(context, 0, 2).reshape(num_rows, NUM_HEADS * HEAD_DIM)
    attn_out = jnp.dot(context, w_o.reshape(NUM_HEADS * HEAD_DIM, D_MODEL), preferred_element_type=jnp.float32)
    hidden = jax.nn.gelu(jnp.dot(h_mlp, w_up, preferred_element_type=jnp.float32), approximate=False).astype(jnp.bfloat16)
    mlp_out = jnp.dot(hidden, w_down, preferred_element_type=jnp.float32)
    summed = x_act.reshape(num_rows, D_MODEL).astype(jnp.float32) + attn_out + mlp_out
    return summed.astype(jnp.bfloat16).reshape(BATCH_SIZE, SEQ_LEN, D_MODEL)


def reference(x_in, ln_params, w_q, w_k, w_v, w_o, w_up, w_down):
    def one_micro(x_act):
        def stage_step(x_cur, weights):
            ln_par, wq_s, wk_s, wv_s, wo_s, wup_s, wdown_s = weights
            y_next = parallel_block(x_cur, ln_par, wq_s, wk_s, wv_s, wo_s, wup_s, wdown_s)
            return y_next, y_next
        _, per_stage = lax.scan(stage_step, x_act, (ln_params, w_q, w_k, w_v, w_o, w_up, w_down))
        return per_stage
    stacked = lax.map(one_micro, x_in)
    return jnp.swapaxes(stacked, 0, 1)
```

```python
import functools

import jax
import jax.numpy as jnp
import numpy as np
from jax import lax
from jax.experimental import pallas as pl
from jax.experimental.pallas import tpu as pltpu
from jax.sharding import PartitionSpec as P

LN_EPS = 1e-5
ROPE_BASE = 10000.0
F32, BF16 = jnp.float32, jnp.bfloat16
MESH = pl.DeviceIdType.MESH
X_AHEAD = 2


def rope_tables(seq_len, head_dim, heads):
    half = head_dim // 2
    inv_freq = (ROPE_BASE ** (-2.0 * np.arange(half) / head_dim)).astype(np.float32)
    angles = np.arange(seq_len, dtype=np.float32)[:, None] * inv_freq[None, :]
    cos = np.tile(np.cos(angles.astype(np.float64)), (1, heads)).astype(np.float32)
    sin = np.tile(np.sin(angles.astype(np.float64)), (1, heads)).astype(np.float32)
    scale = np.float32(head_dim ** -0.5)
    return np.stack([cos * scale, sin * scale, cos, sin])


def head_masks(head_dim, heads):
    half = head_dim // 2
    lanes = np.arange(heads * head_dim)
    roped = np.stack([(lanes % (heads * half)) // half == head for head in range(heads)])
    plain = np.stack([lanes // head_dim == head for head in range(heads)])
    return np.stack([roped, plain]).astype(np.float32)


def layer_norms(x, ln_ref, h_attn, h_mlp, acc):
    x_f32 = x.astype(F32)
    acc[...] = x_f32
    centred = x_f32 - jnp.mean(x_f32, axis=-1, keepdims=True)
    variance = jnp.mean(centred * centred, axis=-1, keepdims=True)
    normed = centred * lax.rsqrt(variance + LN_EPS)
    h_attn[...] = (normed * ln_ref[0:1, :] + ln_ref[1:2, :]).astype(BF16)
    h_mlp[...] = (normed * ln_ref[2:3, :] + ln_ref[3:4, :]).astype(BF16)


def add_quarter(heads, h_attn, h_mlp, acc, w_qkv, w_up, w_out, rope, masks, mixed):
    seq_len = h_attn.shape[0]
    width = w_qkv.shape[1] // 3
    half = width // 2
    qkv = jnp.dot(h_attn[...], w_qkv[...], preferred_element_type=F32)
    q1, q2 = qkv[:, :half], qkv[:, half:width]
    k1, k2 = qkv[:, width:width + half], qkv[:, width + half:2 * width]
    v = qkv[:, 2 * width:].astype(BF16)
    cos_q, sin_q, cos_k, sin_k = rope[0], rope[1], rope[2], rope[3]
    q = jnp.concatenate([q1 * cos_q - q2 * sin_q, q2 * cos_q + q1 * sin_q], axis=1).astype(BF16)
    k = jnp.concatenate([k1 * cos_k - k2 * sin_k, k2 * cos_k + k1 * sin_k], axis=1).astype(BF16)
    k_heads = jnp.concatenate([k * masks[0, h:h + 1, :] for h in range(heads)], axis=0)
    v_heads = jnp.concatenate([v * masks[1, h:h + 1, :] for h in range(heads)], axis=0)
    scores = lax.dot_general(q, k_heads, (((1,), (1,)), ((), ())), preferred_element_type=F32)
    row = lax.broadcasted_iota(jnp.int32, (seq_len, seq_len), 0)
    col = lax.broadcasted_iota(jnp.int32, (seq_len, seq_len), 1)
    allowed = row >= col
    probs = []
    for h in range(heads):
        masked = jnp.where(allowed, scores[:, h * seq_len:(h + 1) * seq_len], -1e30)
        top = jnp.max(masked, axis=1, keepdims=True)
        weight = jnp.exp(masked - top)
        probs.append((weight * (1.0 / jnp.sum(weight, axis=1, keepdims=True))).astype(BF16))
    context = jnp.dot(jnp.concatenate(probs, axis=1), v_heads, preferred_element_type=F32)
    mixed[:, :width] = context.astype(BF16)
    up = jnp.dot(h_mlp[...], w_up[...], preferred_element_type=F32)
    mixed[:, width:] = ((0.5 * up) * (1.0 + lax.erf(up * np.float32(0.5 ** 0.5)))).astype(BF16)
    acc[...] += jnp.dot(mixed[...], w_out[...], preferred_element_type=F32)


def kernel(tp_size, pp_size, heads, x_hbm, ln_ref, wq_hbm, wk_hbm, wv_hbm, wo_hbm, wup_hbm, wdown_hbm, rope, masks, out_hbm,
           w_qkv, w_up, w_out, raw, xs, ys, h_attn, h_mlp, acc, mixed,
           load_sem, own_send, fwd_send, near_recv, far_recv, x_send, x_recv, x_local,
           pp_send, pp_recv, o_send, o_recv, o_local):
    me = lax.axis_index("tp")
    stage = lax.axis_index("pp")
    right, left = lax.rem(me + 1, tp_size), lax.rem(me + tp_size - 1, tp_size)
    far = lax.rem(me + 2, tp_size)
    nxt = lax.rem(stage + 1, pp_size)
    prv = lax.rem(stage + pp_size - 1, pp_size)
    num_micro, num_seq, seq_len, d_model = xs.shape
    tokens = seq_len // tp_size
    width = raw.shape[1]

    barrier = pltpu.get_barrier_semaphore()
    for step in range(1, tp_size):
        pl.semaphore_signal(barrier, inc=1, device_id={"tp": lax.rem(me + step, tp_size)}, device_id_type=MESH)
    for peer in (nxt, prv):
        pl.semaphore_signal(barrier, inc=1, device_id={"pp": peer}, device_id_type=MESH)

    loads = [
        pltpu.make_async_copy(wo_hbm, w_out.at[me, pl.ds(0, width)], load_sem.at[0]),
        pltpu.make_async_copy(wdown_hbm, w_out.at[me, pl.ds(width, wdown_hbm.shape[0])], load_sem.at[1]),
        pltpu.make_async_copy(wup_hbm, w_up.at[me], load_sem.at[2]),
        pltpu.make_async_copy(wq_hbm, raw.at[0], load_sem.at[3]),
        pltpu.make_async_copy(wk_hbm, raw.at[1], load_sem.at[4]),
        pltpu.make_async_copy(wv_hbm, raw.at[2], load_sem.at[5]),
    ]
    for load in loads:
        load.start()
    pl.semaphore_wait(barrier, tp_size + 1)

    def x_copy(micro, step):
        peer = lax.rem(me + step, tp_size)
        return pltpu.make_async_remote_copy(
            src_ref=x_hbm.at[micro, pl.ds(peer * num_seq, num_seq)],
            dst_ref=xs.at[micro, :, pl.ds(pl.multiple_of(me * tokens, tokens), tokens), :],
            send_sem=x_send.at[micro, step - 1], recv_sem=x_recv.at[micro, step - 1],
            device_id={"tp": peer}, device_id_type=MESH)

    def x_own(micro):
        return pltpu.make_async_copy(
            x_hbm.at[micro, pl.ds(me * num_seq, num_seq)],
            xs.at[micro, :, pl.ds(pl.multiple_of(me * tokens, tokens), tokens), :], x_local.at[micro])

    def send_x(micro):
        x_own(micro).start()
        for step in range(1, tp_size):
            x_copy(micro, step).start()

    @pl.when(stage == 0)
    def _():
        for micro in range(X_AHEAD):
            send_x(micro)

    def halves(ref):
        rows = ref.shape[1] // 2
        return [(ref, 0, rows), (ref, rows, rows)]

    chunks = halves(w_out) + halves(w_up) + halves(w_qkv)

    def shard_copy(index, owner, send_sem, recv_sem, peer):
        ref, start, rows = chunks[index]
        piece = ref.at[owner, pl.ds(start, rows)]
        return pltpu.make_async_remote_copy(
            src_ref=piece, dst_ref=piece, send_sem=send_sem, recv_sem=recv_sem, device_id={"tp": peer}, device_id_type=MESH)

    def own_copy(index, way):
        return shard_copy(index, me, own_send.at[way, index], near_recv.at[way, index], right if way == 0 else left)

    def near_copy(index, way):
        return shard_copy(index, left if way == 0 else right, own_send.at[way, index], near_recv.at[way, index],
                          right if way == 0 else left)

    def fwd_copy(index):
        way = index % 2
        return shard_copy(index, left if way == 0 else right, fwd_send.at[index], far_recv.at[index],
                          right if way == 0 else left)

    def far_copy(index):
        return shard_copy(index, far, fwd_send.at[index], far_recv.at[index], right)

    for load in loads[:2]:
        load.wait()
    for way in range(2):
        own_copy(way, way).start()
    for way in range(2):
        own_copy(1 - way, way).start()
    loads[2].wait()
    for way in range(2):
        own_copy(2 + way, way).start()
    for way in range(2):
        own_copy(3 - way, way).start()
    for load in loads[3:]:
        load.wait()
    head_dim = width // heads
    part = head_dim // 2
    for which in range(3):
        starts = [head * head_dim + side * part for side in range(2) for head in range(heads)]
        if which == 2:
            starts = list(range(0, width, part))
        for col in range(0, d_model, width):
            block = jnp.concatenate([raw[which, start:start + part, col:col + width] for start in starts], axis=0)
            w_qkv[me, col:col + width, which * width:(which + 1) * width] = block.T
    for way in range(2):
        near_copy(way, way).wait_recv()
        fwd_copy(way).start()
    for way in range(2):
        own_copy(4 + way, way).start()
    for way in range(2):
        own_copy(5 - way, way).start()
    for way in range(2):
        near_copy(2 + way, way).wait_recv()
        fwd_copy(2 + way).start()
    for way in range(2):
        near_copy(4 + way, way).wait_recv()
        fwd_copy(4 + way).start()
    for way in range(2):
        for index in range(0, len(chunks), 2):
            near_copy(index + 1 - way, way).wait_recv()
    for index in range(len(chunks)):
        far_copy(index).wait_recv()

    def pp_copy(micro, seq):
        return pltpu.make_async_remote_copy(
            src_ref=ys.at[micro, seq], dst_ref=xs.at[micro, seq], send_sem=pp_send.at[micro, seq],
            recv_sem=pp_recv.at[micro, seq], device_id={"pp": nxt}, device_id_type=MESH)

    def o_copy(micro, step):
        peer = lax.rem(me + step, tp_size)
        return pltpu.make_async_remote_copy(
            src_ref=ys.at[micro, :, pl.ds(pl.multiple_of(peer * tokens, tokens), tokens), :],
            dst_ref=out_hbm.at[micro, pl.ds(me * num_seq, num_seq)],
            send_sem=o_send.at[micro, step - 1], recv_sem=o_recv.at[micro, step - 1],
            device_id={"tp": peer}, device_id_type=MESH)

    def o_own(micro):
        return pltpu.make_async_copy(
            ys.at[micro, :, pl.ds(pl.multiple_of(me * tokens, tokens), tokens), :],
            out_hbm.at[micro, pl.ds(me * num_seq, num_seq)], o_local.at[micro])

    def unit(index, _):
        micro = index // num_seq
        seq = lax.rem(index, num_seq)

        @pl.when((stage == 0) & (seq == 0))
        def _():
            @pl.when(micro + X_AHEAD < num_micro)
            def _():
                send_x(micro + X_AHEAD)
            x_own(micro).wait()
            for step in range(1, tp_size):
                x_copy(micro, step).wait_recv()

        @pl.when(stage > 0)
        def _():
            pp_copy(micro, seq).wait_recv()

        layer_norms(xs[micro, seq], ln_ref, h_attn, h_mlp, acc)
        for shard in range(tp_size):
            add_quarter(heads, h_attn, h_mlp, acc, w_qkv.at[shard], w_up.at[shard], w_out.at[shard], rope, masks, mixed)
        ys[micro, seq] = acc[...].astype(BF16)

        @pl.when(stage < pp_size - 1)
        def _():
            pp_copy(micro, seq).start()

        @pl.when(seq == num_seq - 1)
        def _():
            o_own(micro).start()
            for step in range(1, tp_size):
                o_copy(micro, step).start()
        return 0

    lax.fori_loop(0, num_micro * num_seq, unit, 0)

    for index in range(len(chunks)):
        for way in range(2):
            own_copy(index, way).wait_send()
        fwd_copy(index).wait_send()

    def drain(micro, _):
        @pl.when(stage == 0)
        def _():
            for step in range(1, tp_size):
                x_copy(micro, step).wait_send()

        @pl.when(stage < pp_size - 1)
        def _():
            for seq in range(num_seq):
                pp_copy(micro, seq).wait_send()
        o_own(micro).wait()
        for step in range(1, tp_size):
            o_copy(micro, step).wait_send()
            o_copy(micro, step).wait_recv()
        return 0

    lax.fori_loop(0, num_micro, drain, 0)


def solution(mesh):
    tp_size, pp_size = mesh.shape["tp"], mesh.shape["pp"]

    def stage_body(x_in, ln_params, w_q, w_k, w_v, w_o, w_up, w_down):
        num_micro, batch, tokens, d_model = x_in.shape
        heads, head_dim = w_k.shape[2:]
        width = heads * head_dim
        hidden = w_up.shape[2]
        seq_len = tokens * tp_size
        num_seq = batch // tp_size
        rope = jnp.asarray(rope_tables(seq_len, head_dim, heads))
        masks = jnp.asarray(head_masks(head_dim, heads), dtype=BF16)
        wq_t = jnp.transpose(w_q[0], (1, 2, 3, 0)).reshape(width, d_model)
        wk_t = jnp.transpose(w_k[0], (1, 2, 0)).reshape(width, d_model)
        wv_t = jnp.transpose(w_v[0], (1, 2, 0)).reshape(width, d_model)
        vmem = pl.BlockSpec(memory_space=pltpu.VMEM)
        hbm = pl.BlockSpec(memory_space=pl.ANY)
        dma = pltpu.SemaphoreType.DMA
        others = tp_size - 1
        out = pl.pallas_call(
            functools.partial(kernel, tp_size, pp_size, heads),
            out_shape=jax.ShapeDtypeStruct(x_in.shape, BF16),
            in_specs=[hbm, vmem, hbm, hbm, hbm, hbm, hbm, hbm, vmem, vmem],
            out_specs=hbm,
            scratch_shapes=[
                pltpu.VMEM((tp_size, d_model, 3 * width), BF16),
                pltpu.VMEM((tp_size, d_model, hidden), BF16),
                pltpu.VMEM((tp_size, width + hidden, d_model), BF16),
                pltpu.VMEM((3, width, d_model), BF16),
                pltpu.VMEM((num_micro, num_seq, seq_len, d_model), BF16),
                pltpu.VMEM((num_micro, num_seq, seq_len, d_model), BF16),
                pltpu.VMEM((seq_len, d_model), BF16),
                pltpu.VMEM((seq_len, d_model), BF16),
                pltpu.VMEM((seq_len, d_model), F32),
                pltpu.VMEM((seq_len, width + hidden), BF16),
                dma((6,)), dma((2, 6)), dma((6,)), dma((2, 6)), dma((6,)),
                dma((num_micro, others)), dma((num_micro, others)), dma((num_micro,)),
                dma((num_micro, num_seq)), dma((num_micro, num_seq)),
                dma((num_micro, others)), dma((num_micro, others)), dma((num_micro,)),
            ],
            compiler_params=pltpu.CompilerParams(
                collective_id=0, has_side_effects=True, vmem_limit_bytes=63 * 1024 * 1024),
            name="stage",
        )(x_in, ln_params[0], wq_t, wk_t, wv_t, w_o[0].reshape(width, d_model), w_up[0], w_down[0], rope, masks)
        return out[None]

    in_specs = (P(None, "dp", "tp", None), P("pp", None, None), P("pp", None, "tp", None, None), P("pp", None, "tp", None), P("pp", None, "tp", None), P("pp", "tp", None, None, None), P("pp", None, "tp"), P("pp", "tp", None))
    return jax.shard_map(stage_body, mesh=mesh, in_specs=in_specs, out_specs=P("pp", None, "dp", "tp", None), check_vma=False)
```

```python
import functools

import jax
import jax.numpy as jnp
import numpy as np
from jax import lax
from jax.experimental import pallas as pl
from jax.experimental.pallas import tpu as pltpu
from jax.sharding import PartitionSpec as P

LN_EPS = 1e-5
ROPE_BASE = 10000.0
F32, BF16 = jnp.float32, jnp.bfloat16
MESH = pl.DeviceIdType.MESH


def rope_tables(seq_len, head_dim, heads):
    half = head_dim // 2
    inv_freq = (ROPE_BASE ** (-2.0 * np.arange(half) / head_dim)).astype(np.float32)
    angles = np.arange(seq_len, dtype=np.float32)[:, None] * inv_freq[None, :]
    cos = np.tile(np.cos(angles.astype(np.float64)), (1, heads)).astype(np.float32)
    sin = np.tile(np.sin(angles.astype(np.float64)), (1, heads)).astype(np.float32)
    scale = np.float32(head_dim ** -0.5)
    return np.stack([cos * scale, sin * scale, cos, sin])


def head_masks(head_dim, heads):
    half = head_dim // 2
    lanes = np.arange(heads * head_dim)
    roped = np.stack([(lanes % (heads * half)) // half == head for head in range(heads)])
    plain = np.stack([lanes // head_dim == head for head in range(heads)])
    return np.stack([roped, plain]).astype(np.float32)


def dot(lhs, rhs):
    return jnp.dot(lhs, rhs, preferred_element_type=F32)


def layer_norms(x, ln_ref, h_attn, h_mlp, acc):
    x_f32 = x.astype(F32)
    acc[...] = x_f32
    centred = x_f32 - jnp.mean(x_f32, axis=-1, keepdims=True)
    variance = jnp.mean(centred * centred, axis=-1, keepdims=True)
    normed = centred * lax.rsqrt(variance + LN_EPS)
    h_attn[...] = (normed * ln_ref[0:1, :] + ln_ref[1:2, :]).astype(BF16)
    h_mlp[...] = (normed * ln_ref[2:3, :] + ln_ref[3:4, :]).astype(BF16)


def roped(first, second, cos, sin):
    return jnp.concatenate([first * cos - second * sin, second * cos + first * sin], axis=1).astype(BF16)


def causal_softmax(scores, allowed):
    masked = jnp.where(allowed, scores, -1e30)
    weight = jnp.exp(masked - jnp.max(masked, axis=1, keepdims=True))
    return (weight * (1.0 / jnp.sum(weight, axis=1, keepdims=True))).astype(BF16)


def gelu_of_half(half_x):
    return (half_x * (1.0 + lax.erf(half_x * np.float32(2.0 ** 0.5)))).astype(BF16)


def add_layer(heads, shards, h_attn, h_mlp, acc, w_qkv, w_up, w_out, rope, masks, mixed):
    seq_len, d_model = acc.shape
    width = w_qkv.shape[2] // 3
    half = width // 2
    cols = d_model // heads
    hidden = w_up.shape[2] // heads
    allowed = lax.broadcasted_iota(jnp.int32, (seq_len, seq_len), 0) >= lax.broadcasted_iota(jnp.int32, (seq_len, seq_len), 1)

    def add_out(turn, part):
        piece = pl.ds(part * cols, cols)
        acc[:, piece] += dot(mixed[turn % 2], w_out[shards[turn], :, piece])

    def add_up(turn, part):
        up = dot(h_mlp[...], w_up[shards[turn], :, pl.ds(part * hidden, hidden)])
        mixed[turn % 2, :, pl.ds(width + part * hidden, hidden)] = gelu_of_half(up)

    for turn, shard in enumerate(shards):
        weights = w_qkv.at[shard]
        q = dot(h_attn[...], weights[:, :width])
        k = dot(h_attn[...], weights[:, width:2 * width])
        v = dot(h_attn[...], weights[:, 2 * width:]).astype(BF16)
        q = roped(q[:, :half], q[:, half:], rope[0], rope[1])
        k = roped(k[:, :half], k[:, half:], rope[2], rope[3])
        probs = []
        for head in range(heads):
            if head % 2 == 0:
                k_pair = jnp.concatenate([k * masks[0, h:h + 1, :] for h in (head, head + 1)], axis=0)
                scores = lax.dot_general(q, k_pair, (((1,), (1,)), ((), ())), preferred_element_type=F32)
            if turn == 0:
                add_up(turn, head)
            else:
                add_out(turn - 1, head)
            side = head % 2 * seq_len
            probs.append(causal_softmax(scores[:, side:side + seq_len], allowed))

        def add_context():
            v_heads = jnp.concatenate([v * masks[1, h:h + 1, :] for h in range(heads)], axis=0)
            mixed[turn % 2, :, :width] = dot(jnp.concatenate(probs, axis=1), v_heads).astype(BF16)

        if turn == 0:
            add_context()
        else:
            for part in range(heads):
                add_up(turn, part)
                if part == 1:
                    add_context()
    for part in range(heads):
        add_out(len(shards) - 1, part)


def kernel(tp_size, pp_size, heads, x_hbm, ln_ref, wq_hbm, wk_hbm, wv_hbm, wo_hbm, wup_hbm, wdown_hbm, rope, masks, out,
           w_qkv, w_up, w_out, raw, xs, ys, relay, h_attn, h_mlp, acc, mixed,
           load_sem, own_send, fwd_send, near_recv, far_recv, x_send, x_recv, x_local,
           pp_send, pp_recv, o_send, o_recv, o_local, relay_send, relay_recv):
    me = lax.axis_index("tp")
    stage = lax.axis_index("pp")
    right, left = lax.rem(me + 1, tp_size), lax.rem(me + tp_size - 1, tp_size)
    far = lax.rem(me + 2, tp_size)
    odd = lax.rem(me, 2) == 1
    nxt = lax.rem(stage + 1, pp_size)
    prv = lax.rem(stage + pp_size - 1, pp_size)
    last_stage = pp_size - 1
    num_micro, num_seq, seq_len, d_model = xs.shape
    tokens = seq_len // tp_size
    width = raw.shape[1]

    barrier = pltpu.get_barrier_semaphore()
    for step in range(1, tp_size):
        pl.semaphore_signal(barrier, inc=1, device_id={"tp": lax.rem(me + step, tp_size)}, device_id_type=MESH)
    for peer in (nxt, prv):
        pl.semaphore_signal(barrier, inc=1, device_id={"pp": peer}, device_id_type=MESH)

    loads = [
        pltpu.make_async_copy(wo_hbm, w_out.at[me, pl.ds(0, width)], load_sem.at[0]),
        pltpu.make_async_copy(wdown_hbm, w_out.at[me, pl.ds(width, wdown_hbm.shape[0])], load_sem.at[1]),
        pltpu.make_async_copy(wup_hbm, w_up.at[me], load_sem.at[2]),
        pltpu.make_async_copy(wq_hbm, raw.at[0], load_sem.at[3]),
        pltpu.make_async_copy(wk_hbm, raw.at[1], load_sem.at[4]),
        pltpu.make_async_copy(wv_hbm, raw.at[2], load_sem.at[5]),
    ]
    for load in loads:
        load.start()
    pl.semaphore_wait(barrier, tp_size + 1)

    def token_rows(owner):
        return pl.ds(pl.multiple_of(owner * tokens, tokens), tokens)

    def seq_rows(owner):
        return pl.ds(owner * num_seq, num_seq)

    def x_copy(micro, step):
        peer = lax.rem(me + step, tp_size)
        return pltpu.make_async_remote_copy(
            src_ref=x_hbm.at[micro, seq_rows(peer)], dst_ref=ys.at[micro, :, token_rows(me), :],
            send_sem=x_send.at[micro, step - 1], recv_sem=x_recv.at[micro, step - 1],
            device_id={"tp": peer}, device_id_type=MESH)

    def x_own(micro):
        return pltpu.make_async_copy(
            x_hbm.at[micro, seq_rows(me)], ys.at[micro, :, token_rows(me), :], x_local.at[micro])

    def pp_copy(micro, seq):
        return pltpu.make_async_remote_copy(
            src_ref=ys.at[micro, seq], dst_ref=xs.at[micro, seq], send_sem=pp_send.at[micro, seq],
            recv_sem=pp_recv.at[micro, seq], device_id={"pp": nxt}, device_id_type=MESH)

    @pl.when(stage == last_stage)
    def _():
        def collect(micro, _):
            x_own(micro).start()
            for step in range(1, tp_size):
                x_copy(micro, step).start()
            return 0
        lax.fori_loop(0, num_micro, collect, 0)

    def halves(ref):
        rows = ref.shape[1] // 2
        return [(ref, 0, rows), (ref, rows, rows)]

    chunks = halves(w_out) + halves(w_up) + halves(w_qkv)

    def shard_copy(index, owner, send_sem, recv_sem, peer):
        ref, start, rows = chunks[index]
        piece = ref.at[owner, pl.ds(start, rows)]
        return pltpu.make_async_remote_copy(
            src_ref=piece, dst_ref=piece, send_sem=send_sem, recv_sem=recv_sem, device_id={"tp": peer}, device_id_type=MESH)

    def own_copy(index, way):
        return shard_copy(index, me, own_send.at[way, index], near_recv.at[way, index], right if way == 0 else left)

    def near_copy(index, way):
        return shard_copy(index, left if way == 0 else right, own_send.at[way, index], near_recv.at[way, index],
                          right if way == 0 else left)

    def fwd_copy(index):
        way = index % 2
        return shard_copy(index, left if way == 0 else right, fwd_send.at[index], far_recv.at[index],
                          right if way == 0 else left)

    def far_copy(index):
        return shard_copy(index, far, fwd_send.at[index], far_recv.at[index], right)

    def send_own(first):
        for way in range(2):
            own_copy(first + way, way).start()
        for way in range(2):
            own_copy(first + 1 - way, way).start()

    for load in loads[:2]:
        load.wait()
    send_own(0)
    loads[2].wait()
    send_own(2)
    for load in loads[3:]:
        load.wait()
    head_dim = width // heads
    part = head_dim // 2
    for which in range(3):
        starts = [head * head_dim + side * part for side in range(2) for head in range(heads)]
        if which == 2:
            starts = list(range(0, width, part))
        for col in range(0, d_model, width):
            block = jnp.concatenate([raw[which, start:start + part, col:col + width] for start in starts], axis=0)
            w_qkv[me, col:col + width, which * width:(which + 1) * width] = block.T

    @pl.when(stage == last_stage)
    def _():
        def hand_on(micro, _):
            x_own(micro).wait()
            for step in range(1, tp_size):
                x_copy(micro, step).wait_recv()
            for seq in range(num_seq):
                pp_copy(micro, seq).start()
            return 0
        lax.fori_loop(0, num_micro, hand_on, 0)

    for way in range(2):
        near_copy(way, way).wait_recv()
        fwd_copy(way).start()
    send_own(4)
    for first in (2, 4):
        for way in range(2):
            near_copy(first + way, way).wait_recv()
            fwd_copy(first + way).start()
    for way in range(2):
        for index in range(0, len(chunks), 2):
            near_copy(index + 1 - way, way).wait_recv()
    for index in range(len(chunks)):
        far_copy(index).wait_recv()

    @pl.when(stage == last_stage)
    def _():
        def handed(micro, _):
            for seq in range(num_seq):
                pp_copy(micro, seq).wait_send()
            return 0
        lax.fori_loop(0, num_micro, handed, 0)

    def o_copy(micro, step):
        peer = lax.rem(me + step, tp_size)
        return pltpu.make_async_remote_copy(
            src_ref=ys.at[micro, :, token_rows(peer), :], dst_ref=out.at[micro, seq_rows(me)],
            send_sem=o_send.at[micro, step - 1], recv_sem=o_recv.at[micro, step - 1],
            device_id={"tp": peer}, device_id_type=MESH)

    def o_own(micro):
        return pltpu.make_async_copy(ys.at[micro, :, token_rows(me), :], out.at[micro, seq_rows(me)], o_local.at[micro])

    def relay_copy(micro):
        return pltpu.make_async_remote_copy(
            src_ref=ys.at[micro, :, token_rows(far), :], dst_ref=relay.at[micro],
            send_sem=o_send.at[micro, 1], recv_sem=relay_recv.at[micro],
            device_id={"tp": jnp.where(odd, left, right)}, device_id_type=MESH)

    def pass_on(micro):
        return pltpu.make_async_remote_copy(
            src_ref=relay.at[micro], dst_ref=out.at[micro, seq_rows(jnp.where(odd, left, right))],
            send_sem=relay_send.at[micro], recv_sem=o_recv.at[micro, 1],
            device_id={"tp": jnp.where(odd, right, left)}, device_id_type=MESH)

    def unit(index, _):
        micro = index // num_seq
        seq = lax.rem(index, num_seq)
        pp_copy(micro, seq).wait_recv()
        layer_norms(xs[micro, seq], ln_ref, h_attn, h_mlp, acc)
        add_layer(heads, list(range(tp_size)), h_attn, h_mlp, acc, w_qkv, w_up, w_out, rope, masks, mixed)
        ys[micro, seq] = acc[...].astype(BF16)

        @pl.when(stage < last_stage)
        def _():
            pp_copy(micro, seq).start()

        @pl.when((seq == 0) & (micro > 0))
        def _():
            relay_copy(micro - 1).wait_recv()
            pass_on(micro - 1).start()

        @pl.when(seq == num_seq - 1)
        def _():
            o_copy(micro, 1).start()
            o_copy(micro, 3).start()

            @pl.when(micro < num_micro - 1)
            def _():
                relay_copy(micro).start()

            @pl.when(micro == num_micro - 1)
            def _():
                o_copy(micro, 2).start()
            o_own(micro).start()
        return 0

    lax.fori_loop(0, num_micro * num_seq, unit, 0)

    for index in range(len(chunks)):
        for way in range(2):
            own_copy(index, way).wait_send()
        fwd_copy(index).wait_send()

    def drain(micro, _):
        @pl.when(stage == last_stage)
        def _():
            for step in range(1, tp_size):
                x_copy(micro, step).wait_send()

        @pl.when(stage < last_stage)
        def _():
            for seq in range(num_seq):
                pp_copy(micro, seq).wait_send()

        @pl.when(micro < num_micro - 1)
        def _():
            pass_on(micro).wait_send()
        o_own(micro).wait()
        for step in range(1, tp_size):
            o_copy(micro, step).wait_send()
            o_copy(micro, step).wait_recv()
        return 0

    lax.fori_loop(0, num_micro, drain, 0)


def solution(mesh):
    tp_size, pp_size = mesh.shape["tp"], mesh.shape["pp"]

    def stage_body(x_in, ln_params, w_q, w_k, w_v, w_o, w_up, w_down):
        num_micro, batch, tokens, d_model = x_in.shape
        heads, head_dim = w_k.shape[2:]
        width = heads * head_dim
        hidden = w_up.shape[2]
        seq_len = tokens * tp_size
        num_seq = batch // tp_size
        rope = jnp.asarray(rope_tables(seq_len, head_dim, heads))
        masks = jnp.asarray(head_masks(head_dim, heads), dtype=BF16)
        wq_t = jnp.transpose(w_q[0], (1, 2, 3, 0)).reshape(width, d_model)
        wk_t = jnp.transpose(w_k[0], (1, 2, 0)).reshape(width, d_model)
        wv_t = jnp.transpose(w_v[0], (1, 2, 0)).reshape(width, d_model)
        ln_scale = jnp.asarray(np.array([[1.0], [1.0], [0.5], [0.5]], np.float32))
        vmem = pl.BlockSpec(memory_space=pltpu.VMEM)
        hbm = pl.BlockSpec(memory_space=pl.ANY)
        dma = pltpu.SemaphoreType.DMA
        others = tp_size - 1
        out = pl.pallas_call(
            functools.partial(kernel, tp_size, pp_size, heads),
            out_shape=jax.ShapeDtypeStruct(x_in.shape, BF16),
            in_specs=[hbm, vmem, hbm, hbm, hbm, hbm, hbm, hbm, vmem, vmem],
            out_specs=hbm,
            scratch_shapes=[
                pltpu.VMEM((tp_size, d_model, 3 * width), BF16),
                pltpu.VMEM((tp_size, d_model, hidden), BF16),
                pltpu.VMEM((tp_size, width + hidden, d_model), BF16),
                pltpu.VMEM((3, width, d_model), BF16),
                pltpu.VMEM((num_micro, num_seq, seq_len, d_model), BF16),
                pltpu.VMEM((num_micro, num_seq, seq_len, d_model), BF16),
                pltpu.VMEM((num_micro, num_seq, tokens, d_model), BF16),
                pltpu.VMEM((seq_len, d_model), BF16),
                pltpu.VMEM((seq_len, d_model), BF16),
                pltpu.VMEM((seq_len, d_model), F32),
                pltpu.VMEM((2, seq_len, width + hidden), BF16),
                dma((6,)), dma((2, 6)), dma((6,)), dma((2, 6)), dma((6,)),
                dma((num_micro, others)), dma((num_micro, others)), dma((num_micro,)),
                dma((num_micro, num_seq)), dma((num_micro, num_seq)),
                dma((num_micro, others)), dma((num_micro, others)), dma((num_micro,)),
                dma((num_micro,)), dma((num_micro,)),
            ],
            compiler_params=pltpu.CompilerParams(
                collective_id=0, has_side_effects=True, vmem_limit_bytes=63 * 1024 * 1024),
            name="stage",
        )(x_in, ln_params[0] * ln_scale, wq_t, wk_t, wv_t, w_o[0].reshape(width, d_model), w_up[0], w_down[0], rope, masks)
        return out[None]

    in_specs = (P(None, "dp", "tp", None), P("pp", None, None), P("pp", None, "tp", None, None), P("pp", None, "tp", None), P("pp", None, "tp", None), P("pp", "tp", None, None, None), P("pp", None, "tp"), P("pp", "tp", None))
    return jax.shard_map(stage_body, mesh=mesh, in_specs=in_specs, out_specs=P("pp", None, "dp", "tp", None), check_vma=False)
```

```python
import functools

import jax
import jax.numpy as jnp
import numpy as np
from jax import lax
from jax.experimental import pallas as pl
from jax.experimental.pallas import tpu as pltpu
from jax.sharding import PartitionSpec as P

LN_EPS = 1e-5
ROPE_BASE = 10000.0
F32, BF16 = jnp.float32, jnp.bfloat16
MESH = pl.DeviceIdType.MESH


def rope_tables(seq_len, head_dim, heads):
    half = head_dim // 2
    inv_freq = (ROPE_BASE ** (-2.0 * np.arange(half) / head_dim)).astype(np.float32)
    angles = np.arange(seq_len, dtype=np.float32)[:, None] * inv_freq[None, :]
    cos = np.tile(np.cos(angles.astype(np.float64)), (1, heads)).astype(np.float32)
    sin = np.tile(np.sin(angles.astype(np.float64)), (1, heads)).astype(np.float32)
    scale = np.float32(head_dim ** -0.5)
    return np.stack([cos * scale, sin * scale, cos, sin])


def head_masks(head_dim, heads):
    half = head_dim // 2
    lanes = np.arange(heads * head_dim)
    roped = np.stack([(lanes % (heads * half)) // half == head for head in range(heads)])
    plain = np.stack([lanes // head_dim == head for head in range(heads)])
    return np.stack([roped, plain]).astype(np.float32)


def dot(lhs, rhs):
    return jnp.dot(lhs, rhs, preferred_element_type=F32)


def layer_norms(x, ln_ref, h_attn, h_mlp, acc):
    x_f32 = x.astype(F32)
    acc[...] = x_f32
    centred = x_f32 - jnp.mean(x_f32, axis=-1, keepdims=True)
    variance = jnp.mean(centred * centred, axis=-1, keepdims=True)
    normed = centred * lax.rsqrt(variance + LN_EPS)
    h_attn[...] = (normed * ln_ref[0:1, :] + ln_ref[1:2, :]).astype(BF16)
    h_mlp[...] = (normed * ln_ref[2:3, :] + ln_ref[3:4, :]).astype(BF16)


def roped(first, second, cos, sin):
    return jnp.concatenate([first * cos - second * sin, second * cos + first * sin], axis=1).astype(BF16)


def causal_softmax(scores, allowed):
    masked = jnp.where(allowed, scores, -1e30)
    weight = jnp.exp(masked - jnp.max(masked, axis=1, keepdims=True))
    return (weight * (1.0 / jnp.sum(weight, axis=1, keepdims=True))).astype(BF16)


def gelu_of_half(half_x):
    return (half_x * (1.0 + lax.erf(half_x * np.float32(2.0 ** 0.5)))).astype(BF16)


def add_layer(heads, shards, h_attn, h_mlp, acc, w_qkv, w_up, w_out, rope, masks, mixed):
    seq_len, d_model = acc.shape
    width = w_qkv.shape[2] // 3
    half = width // 2
    cols = d_model // heads
    hidden = w_up.shape[2] // heads
    allowed = lax.broadcasted_iota(jnp.int32, (seq_len, seq_len), 0) >= lax.broadcasted_iota(jnp.int32, (seq_len, seq_len), 1)

    def add_out(turn, part):
        piece = pl.ds(part * cols, cols)
        acc[:, piece] += dot(mixed[turn % 2], w_out[shards[turn], :, piece])

    def add_up(turn, part):
        up = dot(h_mlp[...], w_up[shards[turn], :, pl.ds(part * hidden, hidden)])
        mixed[turn % 2, :, pl.ds(width + part * hidden, hidden)] = gelu_of_half(up)

    for turn, shard in enumerate(shards):
        weights = w_qkv.at[shard]
        q = dot(h_attn[...], weights[:, :width])
        k = dot(h_attn[...], weights[:, width:2 * width])
        v = dot(h_attn[...], weights[:, 2 * width:]).astype(BF16)
        q = roped(q[:, :half], q[:, half:], rope[0], rope[1])
        k = roped(k[:, :half], k[:, half:], rope[2], rope[3])
        probs = []
        for head in range(heads):
            if head % 2 == 0:
                k_pair = jnp.concatenate([k * masks[0, h:h + 1, :] for h in (head, head + 1)], axis=0)
                scores = lax.dot_general(q, k_pair, (((1,), (1,)), ((), ())), preferred_element_type=F32)
            if turn == 0:
                add_up(turn, head)
            else:
                add_out(turn - 1, head)
            side = head % 2 * seq_len
            probs.append(causal_softmax(scores[:, side:side + seq_len], allowed))

        def add_context():
            v_heads = jnp.concatenate([v * masks[1, h:h + 1, :] for h in range(heads)], axis=0)
            mixed[turn % 2, :, :width] = dot(jnp.concatenate(probs, axis=1), v_heads).astype(BF16)

        if turn == 0:
            add_context()
        else:
            for part in range(heads):
                add_up(turn, part)
                if part == 1:
                    add_context()
    for part in range(heads):
        add_out(len(shards) - 1, part)


def kernel(tp_size, pp_size, heads, x_hbm, ln_ref, wq_hbm, wk_hbm, wv_hbm, wo_hbm, wup_hbm, wdown_hbm, rope, masks, out,
           w_qkv, w_up, w_out, raw, xs, ys, ln_half, h_attn, h_mlp, acc, mixed,
           load_sem, w_send, near_recv, far_recv, x_send, x_recv, x_local, pp_send, pp_recv, o_send, o_recv):
    me = lax.axis_index("tp")
    stage = lax.axis_index("pp")
    right, left = lax.rem(me + 1, tp_size), lax.rem(me + tp_size - 1, tp_size)
    far = lax.rem(me + 2, tp_size)
    nxt = lax.rem(stage + 1, pp_size)
    prv = lax.rem(stage + pp_size - 1, pp_size)
    last_stage = pp_size - 1
    num_micro, num_seq, seq_len, d_model = xs.shape
    tokens = seq_len // tp_size
    width = raw.shape[1]

    barrier = pltpu.get_barrier_semaphore()
    for step in range(1, tp_size):
        pl.semaphore_signal(barrier, inc=1, device_id={"tp": lax.rem(me + step, tp_size)}, device_id_type=MESH)
    for peer in (nxt, prv):
        pl.semaphore_signal(barrier, inc=1, device_id={"pp": peer}, device_id_type=MESH)

    loads = [
        pltpu.make_async_copy(wo_hbm, w_out.at[me, pl.ds(0, width)], load_sem.at[0]),
        pltpu.make_async_copy(wdown_hbm, w_out.at[me, pl.ds(width, wdown_hbm.shape[0])], load_sem.at[1]),
        pltpu.make_async_copy(wup_hbm, w_up.at[me], load_sem.at[2]),
        pltpu.make_async_copy(wq_hbm, raw.at[0], load_sem.at[3]),
        pltpu.make_async_copy(wk_hbm, raw.at[1], load_sem.at[4]),
        pltpu.make_async_copy(wv_hbm, raw.at[2], load_sem.at[5]),
    ]
    for load in loads:
        load.start()
    ln_half[...] = ln_ref[...]
    ln_half[2:4, :] = 0.5 * ln_ref[2:4, :]
    pl.semaphore_wait(barrier, tp_size + 1)

    def token_rows(owner):
        return pl.ds(pl.multiple_of(owner * tokens, tokens), tokens)

    def seq_rows(owner):
        return pl.ds(owner * num_seq, num_seq)

    def x_copy(micro, step):
        peer = lax.rem(me + step, tp_size)
        return pltpu.make_async_remote_copy(
            src_ref=x_hbm.at[micro, seq_rows(peer)], dst_ref=ys.at[micro, :, token_rows(me), :],
            send_sem=x_send, recv_sem=x_recv,
            device_id={"tp": peer}, device_id_type=MESH)

    def x_own(micro):
        return pltpu.make_async_copy(
            x_hbm.at[micro, seq_rows(me)], ys.at[micro, :, token_rows(me), :], x_local)

    def pp_copy(micro, seq):
        return pltpu.make_async_remote_copy(
            src_ref=ys.at[micro, seq], dst_ref=xs.at[micro, seq], send_sem=pp_send,
            recv_sem=pp_recv.at[micro, seq], device_id={"pp": nxt}, device_id_type=MESH)

    @pl.when(stage == last_stage)
    def _():
        def collect(micro, _):
            x_own(micro).start()
            for step in range(1, tp_size):
                x_copy(micro, step).start()
            return 0
        lax.fori_loop(0, num_micro, collect, 0)

    def halves(ref):
        rows = ref.shape[1] // 2
        return [(ref, 0, rows), (ref, rows, rows)]

    chunks = halves(w_out) + halves(w_up) + halves(w_qkv)

    def shard_copy(index, owner, send_sem, recv_sem, peer):
        ref, start, rows = chunks[index]
        piece = ref.at[owner, pl.ds(start, rows)]
        return pltpu.make_async_remote_copy(
            src_ref=piece, dst_ref=piece, send_sem=send_sem, recv_sem=recv_sem, device_id={"tp": peer}, device_id_type=MESH)

    def own_copy(index, way):
        return shard_copy(index, me, w_send, near_recv.at[way, index], right if way == 0 else left)

    def near_copy(index, way):
        return shard_copy(index, left if way == 0 else right, w_send, near_recv.at[way, index],
                          right if way == 0 else left)

    def fwd_copy(index):
        way = index % 2
        return shard_copy(index, left if way == 0 else right, w_send, far_recv.at[index // 2],
                          right if way == 0 else left)

    def take(sem, *refs):
        for ref in refs:
            pltpu.make_async_copy(ref, ref, sem).wait()

    def send_own(first):
        for way in range(2):
            own_copy(first + way, way).start()
        for way in range(2):
            own_copy(first + 1 - way, way).start()

    for load in loads[:2]:
        load.wait()
    send_own(0)
    loads[2].wait()
    send_own(2)
    for load in loads[3:]:
        load.wait()
    head_dim = width // heads
    part = head_dim // 2
    for which in range(3):
        starts = [head * head_dim + side * part for side in range(2) for head in range(heads)]
        if which == 2:
            starts = list(range(0, width, part))
        for col in range(0, d_model, width):
            block = jnp.concatenate([raw[which, start:start + part, col:col + width] for start in starts], axis=0)
            w_qkv[me, col:col + width, which * width:(which + 1) * width] = block.T

    others = ys.at[pl.ds(0, num_micro // tp_size * (tp_size - 1))]

    @pl.when(stage == last_stage)
    def _():
        take(x_local, ys.at[pl.ds(0, num_micro // tp_size)])
        take(x_recv, others)

        def hand_on(micro, _):
            for seq in range(num_seq):
                pp_copy(micro, seq).start()
            return 0
        lax.fori_loop(0, num_micro, hand_on, 0)

    for way in range(2):
        near_copy(way, way).wait_recv()
        fwd_copy(way).start()
    send_own(4)
    for first in (2, 4):
        for way in range(2):
            near_copy(first + way, way).wait_recv()
            fwd_copy(first + way).start()
    for way in range(2):
        for index in range(0, len(chunks), 2):
            near_copy(index + 1 - way, way).wait_recv()
    for index, ref in enumerate((w_out, w_up, w_qkv)):
        take(far_recv.at[index], ref.at[far])

    @pl.when(stage == last_stage)
    def _():
        take(pp_send, ys)

    def o_copy(micro, step):
        peer = lax.rem(me + step, tp_size)
        return pltpu.make_async_remote_copy(
            src_ref=ys.at[micro, :, token_rows(peer), :], dst_ref=out.at[micro, seq_rows(me)],
            send_sem=o_send, recv_sem=o_recv, device_id={"tp": peer}, device_id_type=MESH)

    def unit(index, _):
        micro = index // num_seq
        seq = lax.rem(index, num_seq)
        pp_copy(micro, seq).wait_recv()
        layer_norms(xs[micro, seq], ln_half, h_attn, h_mlp, acc)
        add_layer(heads, list(range(tp_size)), h_attn, h_mlp, acc, w_qkv, w_up, w_out, rope, masks, mixed)
        ys[micro, seq] = acc[...].astype(BF16)

        @pl.when(stage < last_stage)
        def _():
            pp_copy(micro, seq).start()

        out[micro, me * num_seq + seq] = ys[micro, seq, token_rows(me), :]

        @pl.when(seq == num_seq - 1)
        def _():
            for step in range(1, tp_size):
                o_copy(micro, step).start()
        return 0

    lax.fori_loop(0, num_micro * num_seq, unit, 0)

    take(w_send, w_out, w_up)

    @pl.when(stage == last_stage)
    def _():
        take(x_send, others)

    @pl.when(stage < last_stage)
    def _():
        take(pp_send, ys)
    take(o_send, others)
    take(o_recv, others)


def solution(mesh):
    tp_size, pp_size = mesh.shape["tp"], mesh.shape["pp"]

    def stage_body(x_in, ln_params, w_q, w_k, w_v, w_o, w_up, w_down):
        num_micro, batch, tokens, d_model = x_in.shape
        heads, head_dim = w_k.shape[2:]
        width = heads * head_dim
        hidden = w_up.shape[2]
        seq_len = tokens * tp_size
        num_seq = batch // tp_size
        rope = jnp.asarray(rope_tables(seq_len, head_dim, heads))
        masks = jnp.asarray(head_masks(head_dim, heads), dtype=BF16)
        wq_t = jnp.transpose(w_q[0], (1, 2, 3, 0)).reshape(width, d_model)
        wk_t = jnp.transpose(w_k[0], (1, 2, 0)).reshape(width, d_model)
        wv_t = jnp.transpose(w_v[0], (1, 2, 0)).reshape(width, d_model)
        vmem = pl.BlockSpec(memory_space=pltpu.VMEM)
        hbm = pl.BlockSpec(memory_space=pl.ANY)
        dma = pltpu.SemaphoreType.DMA
        out = pl.pallas_call(
            functools.partial(kernel, tp_size, pp_size, heads),
            out_shape=pltpu.VMEM(x_in.shape, BF16),
            in_specs=[hbm, vmem, hbm, hbm, hbm, hbm, hbm, hbm, vmem, vmem],
            out_specs=vmem,
            scratch_shapes=[
                pltpu.VMEM((tp_size, d_model, 3 * width), BF16),
                pltpu.VMEM((tp_size, d_model, hidden), BF16),
                pltpu.VMEM((tp_size, width + hidden, d_model), BF16),
                pltpu.VMEM((3, width, d_model), BF16),
                pltpu.VMEM((num_micro, num_seq, seq_len, d_model), BF16),
                pltpu.VMEM((num_micro, num_seq, seq_len, d_model), BF16),
                pltpu.VMEM((4, d_model), F32),
                pltpu.VMEM((seq_len, d_model), BF16),
                pltpu.VMEM((seq_len, d_model), BF16),
                pltpu.VMEM((seq_len, d_model), F32),
                pltpu.VMEM((2, seq_len, width + hidden), BF16),
                dma((6,)), dma, dma((2, 6)), dma((3,)), dma, dma, dma, dma, dma((num_micro, num_seq)), dma, dma,
            ],
            compiler_params=pltpu.CompilerParams(
                collective_id=0, has_side_effects=True, vmem_limit_bytes=54 * 1024 * 1024),
            name="stage",
        )(x_in, ln_params[0], wq_t, wk_t, wv_t, w_o[0].reshape(width, d_model), w_up[0], w_down[0], rope, masks)
        return out[None]

    in_specs = (P(None, "dp", "tp", None), P("pp", None, None), P("pp", None, "tp", None, None), P("pp", None, "tp", None), P("pp", None, "tp", None), P("pp", "tp", None, None, None), P("pp", None, "tp"), P("pp", "tp", None))
    return jax.shard_map(stage_body, mesh=mesh, in_specs=in_specs, out_specs=P("pp", None, "dp", "tp", None), check_vma=False)
```

```python
import functools

import jax
import jax.numpy as jnp
import numpy as np
from jax import lax
from jax.experimental import pallas as pl
from jax.experimental.pallas import tpu as pltpu
from jax.sharding import PartitionSpec as P

LN_EPS = 1e-5
ROPE_BASE = 10000.0
F32, BF16 = jnp.float32, jnp.bfloat16
MESH = pl.DeviceIdType.MESH


def rope_tables(seq_len, head_dim, heads):
    half = head_dim // 2
    inv_freq = (ROPE_BASE ** (-2.0 * np.arange(half) / head_dim)).astype(np.float32)
    angles = np.arange(seq_len, dtype=np.float32)[:, None] * inv_freq[None, :]
    cos = np.tile(np.cos(angles.astype(np.float64)), (1, heads)).astype(np.float32)
    sin = np.tile(np.sin(angles.astype(np.float64)), (1, heads)).astype(np.float32)
    scale = np.float32(head_dim ** -0.5)
    return np.stack([cos * scale, sin * scale, cos, sin])


def head_masks(head_dim, heads):
    half = head_dim // 2
    lanes = np.arange(heads * head_dim)
    roped = np.stack([(lanes % (heads * half)) // half == head for head in range(heads)])
    plain = np.stack([lanes // head_dim == head for head in range(heads)])
    return np.stack([roped, plain]).astype(np.float32)


def dot(lhs, rhs):
    return jnp.dot(lhs, rhs, preferred_element_type=F32)


def layer_norms(x, ln_ref, h_attn, h_mlp, acc):
    x_f32 = x.astype(F32)
    acc[...] = x_f32
    centred = x_f32 - jnp.mean(x_f32, axis=-1, keepdims=True)
    variance = jnp.mean(centred * centred, axis=-1, keepdims=True)
    normed = centred * lax.rsqrt(variance + LN_EPS)
    h_attn[...] = (normed * ln_ref[0:1, :] + ln_ref[1:2, :]).astype(BF16)
    h_mlp[...] = (normed * ln_ref[2:3, :] + ln_ref[3:4, :]).astype(BF16)


def roped(first, second, cos, sin):
    return jnp.concatenate([first * cos - second * sin, second * cos + first * sin], axis=1).astype(BF16)


def causal_softmax(scores, allowed):
    masked = jnp.where(allowed, scores, -1e30)
    weight = jnp.exp(masked - jnp.max(masked, axis=1, keepdims=True))
    return (weight * (1.0 / jnp.sum(weight, axis=1, keepdims=True))).astype(BF16)


def gelu_of_half(half_x):
    return (half_x * (1.0 + lax.erf(half_x * np.float32(2.0 ** 0.5)))).astype(BF16)


def add_layer(heads, shards, h_attn, h_mlp, acc, w_qkv, w_up, w_out, rope, masks, mixed, before_last_out=None):
    seq_len, d_model = acc.shape
    width = w_qkv.shape[2] // 3
    half = width // 2
    cols = d_model // heads
    hidden = w_up.shape[2] // heads
    allowed = lax.broadcasted_iota(jnp.int32, (seq_len, seq_len), 0) >= lax.broadcasted_iota(jnp.int32, (seq_len, seq_len), 1)
    raw, ups, score_pairs, probs = {}, {}, {}, {}

    def project(turn, which):
        if turn < len(shards):
            raw[which] = dot(h_attn[...], w_qkv[shards[turn], :, which * width:(which + 1) * width])

    def score(pair):
        k_pair = jnp.concatenate([raw[1] * masks[0, h:h + 1, :] for h in (2 * pair, 2 * pair + 1)], axis=0)
        score_pairs[pair] = lax.dot_general(raw[0], k_pair, (((1,), (1,)), ((), ())), preferred_element_type=F32)

    def soften(head):
        side = head % 2 * seq_len
        probs[head] = causal_softmax(score_pairs[head // 2][:, side:side + seq_len], allowed)

    def context(turn):
        v_heads = jnp.concatenate([v * masks[1, h:h + 1, :] for h in range(heads)], axis=0)
        mixed[turn % 2, :, :width] = dot(jnp.concatenate([probs[h] for h in range(heads)], axis=1), v_heads).astype(BF16)

    def up(turn, part):
        ups[part] = dot(h_mlp[...], w_up[shards[turn], :, part * hidden:(part + 1) * hidden])

    def gelu(turn, part):
        mixed[turn % 2, :, width + part * hidden:width + (part + 1) * hidden] = gelu_of_half(ups[part])

    def add_out(turn, part):
        piece = slice(part * cols, (part + 1) * cols)
        acc[:, piece] += dot(mixed[turn % 2], w_out[shards[turn], :, piece])

    for which in range(3):
        project(0, which)
    for turn in range(len(shards)):
        raw[0] = roped(raw[0][:, :half], raw[0][:, half:], rope[0], rope[1])
        raw[1] = roped(raw[1][:, :half], raw[1][:, half:], rope[2], rope[3])
        v = raw[2].astype(BF16)
        score(0)
        if turn == 0:
            score(1)
            for head in range(heads):
                up(turn, head)
                if head > 0:
                    gelu(turn, head - 1)
                soften(head)
            project(turn + 1, 0)
            project(turn + 1, 1)
            gelu(turn, 3)
            context(turn)
            project(turn + 1, 2)
        else:
            add_out(turn - 1, 0)
            score(1)
            for head in range(heads):
                soften(head)
                if head < 3:
                    add_out(turn - 1, head + 1)
            up(turn, 0)
            up(turn, 1)
            gelu(turn, 0)
            context(turn)
            up(turn, 2)
            gelu(turn, 1)
            up(turn, 3)
            gelu(turn, 2)
            project(turn + 1, 0)
            gelu(turn, 3)
            project(turn + 1, 1)
            project(turn + 1, 2)
    if before_last_out is not None:
        before_last_out()
    for part in range(heads):
        add_out(len(shards) - 1, part)


def kernel(tp_size, pp_size, heads, x_hbm, ln_ref, wq_hbm, wk_hbm, wv_hbm, wo_hbm, wup_hbm, wdown_hbm, rope, masks, out,
           w_qkv, w_up, w_out, raw, xs, ys, ln_half, h_attn, h_mlp, acc, mixed,
           load_sem, w_send, near_recv, far_recv, x_send, x_recv, x_local, pp_send, pp_recv, o_send, o_recv, turn_sem):
    me = lax.axis_index("tp")
    stage = lax.axis_index("pp")
    right, left = lax.rem(me + 1, tp_size), lax.rem(me + tp_size - 1, tp_size)
    far = lax.rem(me + 2, tp_size)
    nxt = lax.rem(stage + 1, pp_size)
    prv = lax.rem(stage + pp_size - 1, pp_size)
    last_stage = pp_size - 1
    num_micro, num_seq, seq_len, d_model = xs.shape
    tokens = seq_len // tp_size
    width = raw.shape[1]

    barrier = pltpu.get_barrier_semaphore()
    for step in range(1, tp_size):
        pl.semaphore_signal(barrier, inc=1, device_id={"tp": lax.rem(me + step, tp_size)}, device_id_type=MESH)
    for peer in (nxt, prv):
        pl.semaphore_signal(barrier, inc=1, device_id={"pp": peer}, device_id_type=MESH)

    loads = [
        pltpu.make_async_copy(wup_hbm, w_up.at[me], load_sem.at[0]),
        pltpu.make_async_copy(wq_hbm, raw.at[0], load_sem.at[1]),
        pltpu.make_async_copy(wk_hbm, raw.at[1], load_sem.at[2]),
        pltpu.make_async_copy(wv_hbm, raw.at[2], load_sem.at[3]),
        pltpu.make_async_copy(wo_hbm, w_out.at[me, pl.ds(0, width)], load_sem.at[4]),
        pltpu.make_async_copy(wdown_hbm, w_out.at[me, pl.ds(width, wdown_hbm.shape[0])], load_sem.at[5]),
    ]
    for load in loads:
        load.start()
    ln_half[...] = ln_ref[...]
    ln_half[2:4, :] = 0.5 * ln_ref[2:4, :]
    pl.semaphore_wait(barrier, tp_size + 1)

    def token_rows(owner):
        return pl.ds(pl.multiple_of(owner * tokens, tokens), tokens)

    def seq_rows(owner):
        return pl.ds(owner * num_seq, num_seq)

    def x_copy(micro, step, dst, recv_sem):
        peer = lax.rem(me + step, tp_size)
        return pltpu.make_async_remote_copy(
            src_ref=x_hbm.at[micro, seq_rows(peer)], dst_ref=dst.at[micro, :, token_rows(me), :],
            send_sem=x_send, recv_sem=recv_sem, device_id={"tp": peer}, device_id_type=MESH)

    def x_own(micro, dst, sem):
        return pltpu.make_async_copy(x_hbm.at[micro, seq_rows(me)], dst.at[micro, :, token_rows(me), :], sem)

    def collect(micro, dst, local_sem, recv_sem):
        x_own(micro, dst, local_sem).start()
        for step in range(1, tp_size):
            x_copy(micro, step, dst, recv_sem).start()

    def pp_copy(micro, seq):
        return pltpu.make_async_remote_copy(
            src_ref=ys.at[micro, seq], dst_ref=xs.at[micro, seq], send_sem=pp_send,
            recv_sem=pp_recv.at[micro, seq], device_id={"pp": nxt}, device_id_type=MESH)

    @pl.when(stage == last_stage)
    def _():
        def early_input(micro, _):
            collect(micro, ys, x_local, x_recv.at[0])
            return 0
        lax.fori_loop(0, num_micro // 2, early_input, 0)

    def halves(ref):
        rows = ref.shape[1] // 2
        return [(ref, 0, rows), (ref, rows, rows)]

    arrays = (w_up, w_qkv, w_out)
    chunks = [chunk for ref in arrays for chunk in halves(ref)]

    def shard_copy(index, owner, send_sem, recv_sem, peer):
        ref, start, rows = chunks[index]
        piece = ref.at[owner, pl.ds(start, rows)]
        return pltpu.make_async_remote_copy(
            src_ref=piece, dst_ref=piece, send_sem=send_sem, recv_sem=recv_sem, device_id={"tp": peer}, device_id_type=MESH)

    def own_copy(index, way):
        return shard_copy(index, me, w_send, near_recv.at[way, index], right if way == 0 else left)

    def near_copy(index, way):
        return shard_copy(index, left if way == 0 else right, w_send, near_recv.at[way, index],
                          right if way == 0 else left)

    def fwd_copy(index):
        way = index % 2
        return shard_copy(index, left if way == 0 else right, w_send, far_recv.at[index // 2],
                          right if way == 0 else left)

    def take(sem, *refs):
        for ref in refs:
            pltpu.make_async_copy(ref, ref, sem).wait()

    def send_own(first):
        for way in range(2):
            own_copy(first + way, way).start()
        for way in range(2):
            own_copy(first + 1 - way, way).start()

    loads[0].wait()

    @pl.when(lax.rem(stage, 2) == 1)
    def _():
        pl.semaphore_wait(turn_sem, 1)
    send_own(0)
    for load in loads[1:4]:
        load.wait()
    head_dim = width // heads
    part = head_dim // 2
    for which in range(3):
        starts = [head * head_dim + side * part for side in range(2) for head in range(heads)]
        if which == 2:
            starts = list(range(0, width, part))
        for col in range(0, d_model, width):
            block = jnp.concatenate([raw[which, start:start + part, col:col + width] for start in starts], axis=0)
            w_qkv[me, col:col + width, which * width:(which + 1) * width] = block.T

    send_own(2)
    for load in loads[4:]:
        load.wait()
    send_own(4)

    def blocks(ref, micros, count):
        return ref.at[pl.ds(0, micros * count // tp_size)]

    early = num_micro // 2

    @pl.when(stage == last_stage)
    def _():
        take(x_local, blocks(ys, early, 1))
        take(x_recv.at[0], blocks(ys, early, tp_size - 1))

        def hand_on(micro, _):
            for seq in range(num_seq):
                pp_copy(micro, seq).start()
            return 0
        lax.fori_loop(0, early, hand_on, 0)

    for first in (0, 2, 4):
        for way in range(2):
            near_copy(first + way, way).wait_recv()
            fwd_copy(first + way).start()
        if first == 0:
            @pl.when(lax.rem(stage, 2) == 0)
            def _():
                pl.semaphore_signal(turn_sem, inc=1, device_id={"pp": nxt}, device_id_type=MESH)
    for way in range(2):
        for index in range(0, len(chunks), 2):
            near_copy(index + 1 - way, way).wait_recv()

    @pl.when(stage == last_stage)
    def _():
        take(pp_send, blocks(ys, early, tp_size))

    def o_copy(micro, seq, step):
        peer = lax.rem(me + step, tp_size)
        return pltpu.make_async_remote_copy(
            src_ref=ys.at[micro, seq, token_rows(peer), :], dst_ref=out.at[micro, me * num_seq + seq],
            send_sem=o_send, recv_sem=o_recv, device_id={"tp": peer}, device_id_type=MESH)

    def ship(micro, seq):
        @pl.when(stage < last_stage)
        def _():
            pp_copy(micro, seq).start()
        out[micro, me * num_seq + seq] = ys[micro, seq, token_rows(me), :]
        for step in range(1, tp_size):
            o_copy(micro, seq, step).start()

    work = (h_attn, h_mlp, acc, w_qkv, w_up, w_out, rope, masks, mixed)

    pp_copy(0, 0).wait_recv()
    layer_norms(xs[0, 0], ln_half, h_attn, h_mlp, acc)
    add_layer(heads, [me, left, right], *work)
    for index in range(2):
        take(far_recv.at[index], arrays[index].at[far])
    add_layer(heads, [far], *work, before_last_out=lambda: take(far_recv.at[2], w_out.at[far]))
    ys[0, 0] = acc[...].astype(BF16)
    ship(0, 0)

    def unit(index, _):
        micro = index // num_seq
        seq = lax.rem(index, num_seq)

        @pl.when((stage > 0) | (micro < early))
        def _():
            pp_copy(micro, seq).wait_recv()

        @pl.when((stage == 0) & (seq == num_seq - 1) & (micro < early))
        def _():
            collect(micro + early, xs, x_recv.at[1 + micro], x_recv.at[1 + micro])

        @pl.when((stage == 0) & (seq == 0) & (micro >= early))
        def _():
            take(x_recv.at[1 + micro - early], xs.at[micro])

        layer_norms(xs[micro, seq], ln_half, h_attn, h_mlp, acc)
        add_layer(heads, list(range(tp_size)), *work)
        ys[micro, seq] = acc[...].astype(BF16)
        ship(micro, seq)
        return 0

    lax.fori_loop(1, num_micro * num_seq, unit, 0)

    take(w_send, w_out, w_up)

    @pl.when((stage == 0) | (stage == last_stage))
    def _():
        take(x_send, blocks(ys, early, tp_size - 1))

    @pl.when(stage < last_stage)
    def _():
        take(pp_send, ys)
    others = blocks(ys, num_micro, tp_size - 1)
    take(o_send, others)
    take(o_recv, others)


def solution(mesh):
    tp_size, pp_size = mesh.shape["tp"], mesh.shape["pp"]

    def stage_body(x_in, ln_params, w_q, w_k, w_v, w_o, w_up, w_down):
        num_micro, batch, tokens, d_model = x_in.shape
        heads, head_dim = w_k.shape[2:]
        width = heads * head_dim
        hidden = w_up.shape[2]
        seq_len = tokens * tp_size
        num_seq = batch // tp_size
        rope = jnp.asarray(rope_tables(seq_len, head_dim, heads))
        masks = jnp.asarray(head_masks(head_dim, heads), dtype=BF16)
        wq_t = jnp.transpose(w_q[0], (1, 2, 3, 0)).reshape(width, d_model)
        wk_t = jnp.transpose(w_k[0], (1, 2, 0)).reshape(width, d_model)
        wv_t = jnp.transpose(w_v[0], (1, 2, 0)).reshape(width, d_model)
        vmem = pl.BlockSpec(memory_space=pltpu.VMEM)
        hbm = pl.BlockSpec(memory_space=pl.ANY)
        dma = pltpu.SemaphoreType.DMA
        out = pl.pallas_call(
            functools.partial(kernel, tp_size, pp_size, heads),
            out_shape=pltpu.VMEM(x_in.shape, BF16),
            in_specs=[hbm, vmem, hbm, hbm, hbm, hbm, hbm, hbm, vmem, vmem],
            out_specs=vmem,
            scratch_shapes=[
                pltpu.VMEM((tp_size, d_model, 3 * width), BF16),
                pltpu.VMEM((tp_size, d_model, hidden), BF16),
                pltpu.VMEM((tp_size, width + hidden, d_model), BF16),
                pltpu.VMEM((3, width, d_model), BF16),
                pltpu.VMEM((num_micro, num_seq, seq_len, d_model), BF16),
                pltpu.VMEM((num_micro, num_seq, seq_len, d_model), BF16),
                pltpu.VMEM((4, d_model), F32),
                pltpu.VMEM((seq_len, d_model), BF16),
                pltpu.VMEM((seq_len, d_model), BF16),
                pltpu.VMEM((seq_len, d_model), F32),
                pltpu.VMEM((2, seq_len, width + hidden), BF16),
                dma((6,)), dma, dma((2, 6)), dma((3,)), dma, dma((1 + num_micro // 2,)), dma, dma, dma((num_micro, num_seq)), dma, dma,
                pltpu.SemaphoreType.REGULAR,
            ],
            compiler_params=pltpu.CompilerParams(
                collective_id=0, has_side_effects=True, vmem_limit_bytes=54 * 1024 * 1024),
            name="stage",
        )(x_in, ln_params[0], wq_t, wk_t, wv_t, w_o[0].reshape(width, d_model), w_up[0], w_down[0], rope, masks)
        return out[None]

    in_specs = (P(None, "dp", "tp", None), P("pp", None, None), P("pp", None, "tp", None, None), P("pp", None, "tp", None), P("pp", None, "tp", None), P("pp", "tp", None, None, None), P("pp", None, "tp"), P("pp", "tp", None))
    return jax.shard_map(stage_body, mesh=mesh, in_specs=in_specs, out_specs=P("pp", None, "dp", "tp", None), check_vma=False)
```

```python
import functools

import jax
import jax.numpy as jnp
import numpy as np
from jax import lax
from jax.experimental import pallas as pl
from jax.experimental.pallas import tpu as pltpu
from jax.sharding import PartitionSpec as P

LN_EPS = 1e-5
ROPE_BASE = 10000.0
F32, BF16 = jnp.float32, jnp.bfloat16
MESH = pl.DeviceIdType.MESH


def rope_tables(seq_len, head_dim, heads):
    half = head_dim // 2
    inv_freq = (ROPE_BASE ** (-2.0 * np.arange(half) / head_dim)).astype(np.float32)
    angles = np.arange(seq_len, dtype=np.float32)[:, None] * inv_freq[None, :]
    cos = np.tile(np.cos(angles.astype(np.float64)), (1, heads)).astype(np.float32)
    sin = np.tile(np.sin(angles.astype(np.float64)), (1, heads)).astype(np.float32)
    scale = np.float32(head_dim ** -0.5)
    return np.stack([cos * scale, sin * scale, cos, sin])


def head_masks(head_dim, heads):
    half = head_dim // 2
    lanes = np.arange(heads * head_dim)
    roped = np.stack([(lanes % (heads * half)) // half == head for head in range(heads)])
    plain = np.stack([lanes // head_dim == head for head in range(heads)])
    return np.stack([roped, plain]).astype(np.float32)


def dot(lhs, rhs):
    return jnp.dot(lhs, rhs, preferred_element_type=F32)


def layer_norms(x, ln_ref, h_attn, h_mlp, acc):
    x_f32 = x.astype(F32)
    acc[...] = x_f32
    centred = x_f32 - jnp.mean(x_f32, axis=-1, keepdims=True)
    variance = jnp.mean(centred * centred, axis=-1, keepdims=True)
    normed = centred * lax.rsqrt(variance + LN_EPS)
    h_attn[...] = (normed * ln_ref[0:1, :] + ln_ref[1:2, :]).astype(BF16)
    h_mlp[...] = (normed * ln_ref[2:3, :] + ln_ref[3:4, :]).astype(BF16)


def roped(first, second, cos, sin):
    return jnp.concatenate([first * cos - second * sin, second * cos + first * sin], axis=1).astype(BF16)


def causal_softmax(scores, allowed):
    masked = jnp.where(allowed, scores, -1e30)
    weight = jnp.exp(masked - jnp.max(masked, axis=1, keepdims=True))
    return (weight * (1.0 / jnp.sum(weight, axis=1, keepdims=True))).astype(BF16)


def gelu_of_half(half_x):
    return (half_x * (1.0 + lax.erf(half_x * np.float32(2.0 ** 0.5)))).astype(BF16)


def add_layer(heads, shards, h_attn, h_mlp, acc, w_qkv, w_up, w_out, rope, masks, mixed, before_last_out=None):
    seq_len, d_model = acc.shape
    width = w_qkv.shape[2] // 3
    half = width // 2
    cols = d_model // heads
    hidden = w_up.shape[2] // heads
    allowed = lax.broadcasted_iota(jnp.int32, (seq_len, seq_len), 0) >= lax.broadcasted_iota(jnp.int32, (seq_len, seq_len), 1)
    raw, ups, score_pairs, probs = {}, {}, {}, {}

    def project(turn, which):
        if turn < len(shards):
            raw[which] = dot(h_attn[...], w_qkv[shards[turn], :, which * width:(which + 1) * width])

    def score(pair):
        k_pair = jnp.concatenate([raw[1] * masks[0, h:h + 1, :] for h in (2 * pair, 2 * pair + 1)], axis=0)
        score_pairs[pair] = lax.dot_general(raw[0], k_pair, (((1,), (1,)), ((), ())), preferred_element_type=F32)

    def soften(head):
        side = head % 2 * seq_len
        probs[head] = causal_softmax(score_pairs[head // 2][:, side:side + seq_len], allowed)

    def context(turn):
        v_heads = jnp.concatenate([v * masks[1, h:h + 1, :] for h in range(heads)], axis=0)
        mixed[turn % 2, :, :width] = dot(jnp.concatenate([probs[h] for h in range(heads)], axis=1), v_heads).astype(BF16)

    def up(turn, part):
        ups[part] = dot(h_mlp[...], w_up[shards[turn], :, part * hidden:(part + 1) * hidden])

    def gelu(turn, part):
        mixed[turn % 2, :, width + part * hidden:width + (part + 1) * hidden] = gelu_of_half(ups[part])

    def add_out(turn, part):
        piece = slice(part * cols, (part + 1) * cols)
        acc[:, piece] += dot(mixed[turn % 2], w_out[shards[turn], :, piece])

    for which in range(3):
        project(0, which)
    for turn in range(len(shards)):
        raw[0] = roped(raw[0][:, :half], raw[0][:, half:], rope[0], rope[1])
        raw[1] = roped(raw[1][:, :half], raw[1][:, half:], rope[2], rope[3])
        v = raw[2].astype(BF16)
        score(0)
        if turn == 0:
            score(1)
            for head in range(heads):
                up(turn, head)
                if head > 0:
                    gelu(turn, head - 1)
                soften(head)
            project(turn + 1, 0)
            project(turn + 1, 1)
            gelu(turn, 3)
            context(turn)
            project(turn + 1, 2)
        else:
            add_out(turn - 1, 0)
            score(1)
            for head in range(heads):
                soften(head)
                if head < 3:
                    add_out(turn - 1, head + 1)
            up(turn, 0)
            up(turn, 1)
            gelu(turn, 0)
            context(turn)
            up(turn, 2)
            gelu(turn, 1)
            up(turn, 3)
            gelu(turn, 2)
            project(turn + 1, 0)
            gelu(turn, 3)
            project(turn + 1, 1)
            project(turn + 1, 2)
    if before_last_out is not None:
        before_last_out()
    for part in range(heads):
        add_out(len(shards) - 1, part)


def kernel(tp_size, pp_size, heads, x_hbm, ln_ref, wq_hbm, wk_hbm, wv_hbm, wo_hbm, wup_hbm, wdown_hbm, rope, masks, out,
           w_qkv, w_up, w_out, raw, xs, ys, ln_half, h_attn, h_mlp, acc, mixed,
           load_sem, w_send, near_recv, far_recv, x_send, x_recv, x_local, pp_send, pp_recv, o_send, o_recv):
    me = lax.axis_index("tp")
    stage = lax.axis_index("pp")
    right, left = lax.rem(me + 1, tp_size), lax.rem(me + tp_size - 1, tp_size)
    far = lax.rem(me + 2, tp_size)
    nxt = lax.rem(stage + 1, pp_size)
    prv = lax.rem(stage + pp_size - 1, pp_size)
    last_stage = pp_size - 1
    num_micro, num_seq, seq_len, d_model = xs.shape
    tokens = seq_len // tp_size
    width = raw.shape[1]

    barrier = pltpu.get_barrier_semaphore()
    for step in range(1, tp_size):
        pl.semaphore_signal(barrier, inc=1, device_id={"tp": lax.rem(me + step, tp_size)}, device_id_type=MESH)
    for peer in (nxt, prv):
        pl.semaphore_signal(barrier, inc=1, device_id={"pp": peer}, device_id_type=MESH)

    loads = [
        pltpu.make_async_copy(wup_hbm, w_up.at[me], load_sem.at[0]),
        pltpu.make_async_copy(wq_hbm, raw.at[0], load_sem.at[1]),
        pltpu.make_async_copy(wk_hbm, raw.at[1], load_sem.at[2]),
        pltpu.make_async_copy(wv_hbm, raw.at[2], load_sem.at[3]),
        pltpu.make_async_copy(wo_hbm, w_out.at[me, pl.ds(0, width)], load_sem.at[4]),
        pltpu.make_async_copy(wdown_hbm, w_out.at[me, pl.ds(width, wdown_hbm.shape[0])], load_sem.at[5]),
    ]
    for load in loads:
        load.start()
    ln_half[...] = ln_ref[...]
    ln_half[2:4, :] = 0.5 * ln_ref[2:4, :]
    pl.semaphore_wait(barrier, tp_size + 1)

    def token_rows(owner):
        return pl.ds(pl.multiple_of(owner * tokens, tokens), tokens)

    def seq_rows(owner):
        return pl.ds(owner * num_seq, num_seq)

    def x_copy(micro, step, dst, recv_sem):
        peer = lax.rem(me + step, tp_size)
        return pltpu.make_async_remote_copy(
            src_ref=x_hbm.at[micro, seq_rows(peer)], dst_ref=dst.at[micro, :, token_rows(me), :],
            send_sem=x_send, recv_sem=recv_sem, device_id={"tp": peer}, device_id_type=MESH)

    def x_own(micro, dst, sem):
        return pltpu.make_async_copy(x_hbm.at[micro, seq_rows(me)], dst.at[micro, :, token_rows(me), :], sem)

    def collect(micro, dst, local_sem, recv_sem):
        x_own(micro, dst, local_sem).start()
        for step in range(1, tp_size):
            x_copy(micro, step, dst, recv_sem).start()

    def pp_copy(micro, seq):
        return pltpu.make_async_remote_copy(
            src_ref=ys.at[micro, seq], dst_ref=xs.at[micro, seq], send_sem=pp_send,
            recv_sem=pp_recv.at[micro, seq], device_id={"pp": nxt}, device_id_type=MESH)

    @pl.when(stage == last_stage)
    def _():
        def early_input(micro, _):
            collect(micro, ys, x_local, x_recv.at[0])
            return 0
        lax.fori_loop(0, num_micro // 2, early_input, 0)

    def halves(ref):
        rows = ref.shape[1] // 2
        return [(ref, 0, rows), (ref, rows, rows)]

    arrays = (w_up, w_qkv, w_out)
    chunks = [chunk for ref in arrays for chunk in halves(ref)]

    def shard_copy(index, owner, send_sem, recv_sem, peer):
        ref, start, rows = chunks[index]
        piece = ref.at[owner, pl.ds(start, rows)]
        return pltpu.make_async_remote_copy(
            src_ref=piece, dst_ref=piece, send_sem=send_sem, recv_sem=recv_sem, device_id={"tp": peer}, device_id_type=MESH)

    def own_copy(index, way):
        return shard_copy(index, me, w_send, near_recv.at[way, index], right if way == 0 else left)

    def near_copy(index, way):
        return shard_copy(index, left if way == 0 else right, w_send, near_recv.at[way, index],
                          right if way == 0 else left)

    def fwd_copy(index):
        way = index % 2
        return shard_copy(index, left if way == 0 else right, w_send, far_recv.at[index // 2],
                          right if way == 0 else left)

    def take(sem, *refs):
        for ref in refs:
            pltpu.make_async_copy(ref, ref, sem).wait()

    def send_own(first):
        for way in range(2):
            own_copy(first + way, way).start()
        for way in range(2):
            own_copy(first + 1 - way, way).start()

    loads[0].wait()
    send_own(0)
    for load in loads[1:4]:
        load.wait()
    head_dim = width // heads
    part = head_dim // 2
    for which in range(3):
        starts = [head * head_dim + side * part for side in range(2) for head in range(heads)]
        if which == 2:
            starts = list(range(0, width, part))
        for col in range(0, d_model, width):
            block = jnp.concatenate([raw[which, start:start + part, col:col + width] for start in starts], axis=0)
            w_qkv[me, col:col + width, which * width:(which + 1) * width] = block.T

    send_own(2)
    for load in loads[4:]:
        load.wait()
    send_own(4)

    def blocks(ref, micros, count):
        return ref.at[pl.ds(0, micros * count // tp_size)]

    early = num_micro // 2

    @pl.when(stage == last_stage)
    def _():
        take(x_local, blocks(ys, early, 1))
        take(x_recv.at[0], blocks(ys, early, tp_size - 1))

        def hand_on(micro, _):
            for seq in range(num_seq):
                pp_copy(micro, seq).start()
            return 0
        lax.fori_loop(0, early, hand_on, 0)

    for first in (0, 2, 4):
        for way in range(2):
            near_copy(first + way, way).wait_recv()
            fwd_copy(first + way).start()
    for way in range(2):
        for index in range(0, len(chunks), 2):
            near_copy(index + 1 - way, way).wait_recv()

    @pl.when(stage == last_stage)
    def _():
        take(pp_send, blocks(ys, early, tp_size))

    def o_copy(micro, seq, step):
        peer = lax.rem(me + step, tp_size)
        return pltpu.make_async_remote_copy(
            src_ref=ys.at[micro, seq, token_rows(peer), :], dst_ref=out.at[micro, me * num_seq + seq],
            send_sem=o_send, recv_sem=o_recv, device_id={"tp": peer}, device_id_type=MESH)

    def ship(micro, seq):
        @pl.when(stage < last_stage)
        def _():
            pp_copy(micro, seq).start()
        out[micro, me * num_seq + seq] = ys[micro, seq, token_rows(me), :]
        for step in range(1, tp_size):
            o_copy(micro, seq, step).start()

    work = (h_attn, h_mlp, acc, w_qkv, w_up, w_out, rope, masks, mixed)

    pp_copy(0, 0).wait_recv()
    layer_norms(xs[0, 0], ln_half, h_attn, h_mlp, acc)
    add_layer(heads, [me, left, right], *work)
    for index in range(2):
        take(far_recv.at[index], arrays[index].at[far])
    add_layer(heads, [far], *work, before_last_out=lambda: take(far_recv.at[2], w_out.at[far]))
    ys[0, 0] = acc[...].astype(BF16)
    ship(0, 0)

    def unit(index, _):
        micro = index // num_seq
        seq = lax.rem(index, num_seq)

        @pl.when((stage > 0) | (micro < early))
        def _():
            pp_copy(micro, seq).wait_recv()

        @pl.when((stage == 0) & (seq == num_seq - 1) & (micro < early))
        def _():
            collect(micro + early, xs, x_recv.at[1 + micro], x_recv.at[1 + micro])

        @pl.when((stage == 0) & (seq == 0) & (micro >= early))
        def _():
            take(x_recv.at[1 + micro - early], xs.at[micro])

        layer_norms(xs[micro, seq], ln_half, h_attn, h_mlp, acc)
        add_layer(heads, list(range(tp_size)), *work)
        ys[micro, seq] = acc[...].astype(BF16)
        ship(micro, seq)
        return 0

    lax.fori_loop(1, num_micro * num_seq, unit, 0)

    take(w_send, w_out, w_up)

    @pl.when((stage == 0) | (stage == last_stage))
    def _():
        take(x_send, blocks(ys, early, tp_size - 1))

    @pl.when(stage < last_stage)
    def _():
        take(pp_send, ys)
    others = blocks(ys, num_micro, tp_size - 1)
    take(o_send, others)
    take(o_recv, others)


def solution(mesh):
    tp_size, pp_size = mesh.shape["tp"], mesh.shape["pp"]

    def stage_body(x_in, ln_params, w_q, w_k, w_v, w_o, w_up, w_down):
        num_micro, batch, tokens, d_model = x_in.shape
        heads, head_dim = w_k.shape[2:]
        width = heads * head_dim
        hidden = w_up.shape[2]
        seq_len = tokens * tp_size
        num_seq = batch // tp_size
        rope = jnp.asarray(rope_tables(seq_len, head_dim, heads))
        masks = jnp.asarray(head_masks(head_dim, heads), dtype=BF16)
        wq_t = jnp.transpose(w_q[0], (1, 2, 3, 0)).reshape(width, d_model)
        wk_t = jnp.transpose(w_k[0], (1, 2, 0)).reshape(width, d_model)
        wv_t = jnp.transpose(w_v[0], (1, 2, 0)).reshape(width, d_model)
        vmem = pl.BlockSpec(memory_space=pltpu.VMEM)
        hbm = pl.BlockSpec(memory_space=pl.ANY)
        dma = pltpu.SemaphoreType.DMA
        out = pl.pallas_call(
            functools.partial(kernel, tp_size, pp_size, heads),
            out_shape=pltpu.VMEM(x_in.shape, BF16),
            in_specs=[hbm, vmem, hbm, hbm, hbm, hbm, hbm, hbm, vmem, vmem],
            out_specs=vmem,
            scratch_shapes=[
                pltpu.VMEM((tp_size, d_model, 3 * width), BF16),
                pltpu.VMEM((tp_size, d_model, hidden), BF16),
                pltpu.VMEM((tp_size, width + hidden, d_model), BF16),
                pltpu.VMEM((3, width, d_model), BF16),
                pltpu.VMEM((num_micro, num_seq, seq_len, d_model), BF16),
                pltpu.VMEM((num_micro, num_seq, seq_len, d_model), BF16),
                pltpu.VMEM((4, d_model), F32),
                pltpu.VMEM((seq_len, d_model), BF16),
                pltpu.VMEM((seq_len, d_model), BF16),
                pltpu.VMEM((seq_len, d_model), F32),
                pltpu.VMEM((2, seq_len, width + hidden), BF16),
                dma((6,)), dma, dma((2, 6)), dma((3,)), dma, dma((1 + num_micro // 2,)), dma, dma, dma((num_micro, num_seq)), dma, dma,
            ],
            compiler_params=pltpu.CompilerParams(
                collective_id=0, has_side_effects=True, vmem_limit_bytes=54 * 1024 * 1024),
            name="stage",
        )(x_in, ln_params[0], wq_t, wk_t, wv_t, w_o[0].reshape(width, d_model), w_up[0], w_down[0], rope, masks)
        return out[None]

    in_specs = (P(None, "dp", "tp", None), P("pp", None, None), P("pp", None, "tp", None, None), P("pp", None, "tp", None), P("pp", None, "tp", None), P("pp", "tp", None, None, None), P("pp", None, "tp"), P("pp", "tp", None))
    return jax.shard_map(stage_body, mesh=mesh, in_specs=in_specs, out_specs=P("pp", None, "dp", "tp", None), check_vma=False)
```

```python
import functools

import jax
import jax.numpy as jnp
import numpy as np
from jax import lax
from jax.experimental import pallas as pl
from jax.experimental.pallas import tpu as pltpu
from jax.sharding import PartitionSpec as P

LN_EPS = 1e-5
ROPE_BASE = 10000.0
F32, BF16 = jnp.float32, jnp.bfloat16
MESH = pl.DeviceIdType.MESH


def rope_tables(seq_len, head_dim, heads):
    half = head_dim // 2
    inv_freq = (ROPE_BASE ** (-2.0 * np.arange(half) / head_dim)).astype(np.float32)
    angles = np.arange(seq_len, dtype=np.float32)[:, None] * inv_freq[None, :]
    cos = np.tile(np.cos(angles.astype(np.float64)), (1, heads)).astype(np.float32)
    sin = np.tile(np.sin(angles.astype(np.float64)), (1, heads)).astype(np.float32)
    scale = np.float32(head_dim ** -0.5)
    return np.stack([cos * scale, sin * scale, cos, sin])


def head_masks(head_dim, heads):
    half = head_dim // 2
    lanes = np.arange(heads * head_dim)
    roped = np.stack([(lanes % (heads * half)) // half == head for head in range(heads)])
    plain = np.stack([lanes // head_dim == head for head in range(heads)])
    return np.stack([roped, plain]).astype(np.float32)


def dot(lhs, rhs):
    return jnp.dot(lhs, rhs, preferred_element_type=F32)


def layer_norms(x, ln_ref, h_attn, h_mlp, acc):
    x_f32 = x.astype(F32)
    acc[...] = x_f32
    centred = x_f32 - jnp.mean(x_f32, axis=-1, keepdims=True)
    variance = jnp.mean(centred * centred, axis=-1, keepdims=True)
    normed = centred * lax.rsqrt(variance + LN_EPS)
    h_attn[...] = (normed * ln_ref[0:1, :] + ln_ref[1:2, :]).astype(BF16)
    h_mlp[...] = (normed * ln_ref[2:3, :] + ln_ref[3:4, :]).astype(BF16)


def roped(first, second, cos, sin):
    return jnp.concatenate([first * cos - second * sin, second * cos + first * sin], axis=1).astype(BF16)


def causal_softmax(scores, allowed):
    masked = jnp.where(allowed, scores, -1e30)
    weight = jnp.exp(masked - jnp.max(masked, axis=1, keepdims=True))
    return (weight * (1.0 / jnp.sum(weight, axis=1, keepdims=True))).astype(BF16)


def gelu_of_half(half_x):
    return (half_x * (1.0 + lax.erf(half_x * np.float32(2.0 ** 0.5)))).astype(BF16)


def add_layer(heads, shards, h_attn, h_mlp, acc, w_qkv, w_up, w_out, rope, masks, mixed, before_last_out=None):
    seq_len, d_model = acc.shape
    width = w_qkv.shape[2] // 3
    half = width // 2
    cols = d_model // heads
    hidden = w_up.shape[2] // heads
    allowed = lax.broadcasted_iota(jnp.int32, (seq_len, seq_len), 0) >= lax.broadcasted_iota(jnp.int32, (seq_len, seq_len), 1)
    raw, ups, score_pairs, probs = {}, {}, {}, {}

    def project(turn, which):
        if turn < len(shards):
            raw[which] = dot(h_attn[...], w_qkv[shards[turn], :, which * width:(which + 1) * width])

    def score(pair):
        k_pair = jnp.concatenate([raw[1] * masks[0, h:h + 1, :] for h in (2 * pair, 2 * pair + 1)], axis=0)
        score_pairs[pair] = lax.dot_general(raw[0], k_pair, (((1,), (1,)), ((), ())), preferred_element_type=F32)

    def soften(head):
        side = head % 2 * seq_len
        probs[head] = causal_softmax(score_pairs[head // 2][:, side:side + seq_len], allowed)

    def context(turn):
        v_heads = jnp.concatenate([v * masks[1, h:h + 1, :] for h in range(heads)], axis=0)
        mixed[turn % 2, :, :width] = dot(jnp.concatenate([probs[h] for h in range(heads)], axis=1), v_heads).astype(BF16)

    def up(turn, part):
        ups[part] = dot(h_mlp[...], w_up[shards[turn], :, part * hidden:(part + 1) * hidden])

    def gelu(turn, part):
        mixed[turn % 2, :, width + part * hidden:width + (part + 1) * hidden] = gelu_of_half(ups[part])

    def add_out(turn, part):
        piece = slice(part * cols, (part + 1) * cols)
        acc[:, piece] += dot(mixed[turn % 2], w_out[shards[turn], :, piece])

    for which in range(3):
        project(0, which)
    for turn in range(len(shards)):
        raw[0] = roped(raw[0][:, :half], raw[0][:, half:], rope[0], rope[1])
        raw[1] = roped(raw[1][:, :half], raw[1][:, half:], rope[2], rope[3])
        v = raw[2].astype(BF16)
        score(0)
        if turn == 0:
            score(1)
            for head in range(heads):
                up(turn, head)
                if head > 0:
                    gelu(turn, head - 1)
                soften(head)
            project(turn + 1, 0)
            project(turn + 1, 1)
            gelu(turn, 3)
            context(turn)
            project(turn + 1, 2)
        else:
            add_out(turn - 1, 0)
            score(1)
            for head in range(heads):
                soften(head)
                if head < 3:
                    add_out(turn - 1, head + 1)
            up(turn, 0)
            up(turn, 1)
            gelu(turn, 0)
            context(turn)
            up(turn, 2)
            gelu(turn, 1)
            up(turn, 3)
            gelu(turn, 2)
            project(turn + 1, 0)
            gelu(turn, 3)
            project(turn + 1, 1)
            project(turn + 1, 2)
    if before_last_out is not None:
        before_last_out()
    for part in range(heads):
        add_out(len(shards) - 1, part)


def kernel(tp_size, pp_size, heads, x_hbm, ln_ref, wq_hbm, wk_hbm, wv_hbm, wo_hbm, wup_hbm, wdown_hbm, rope, masks, out,
           w_qkv, w_up, w_out, raw, xs, ys, ln_half, h_attn, h_mlp, acc, mixed,
           load_sem, w_send, near_recv, far_recv, x_send, x_recv, x_local, pp_send, pp_recv, o_send, o_recv):
    me = lax.axis_index("tp")
    stage = lax.axis_index("pp")
    right, left = lax.rem(me + 1, tp_size), lax.rem(me + tp_size - 1, tp_size)
    far = lax.rem(me + 2, tp_size)
    nxt = lax.rem(stage + 1, pp_size)
    prv = lax.rem(stage + pp_size - 1, pp_size)
    last_stage = pp_size - 1
    num_micro, num_seq, seq_len, d_model = xs.shape
    tokens = seq_len // tp_size
    width = raw.shape[1]

    barrier = pltpu.get_barrier_semaphore()
    for step in range(1, tp_size):
        pl.semaphore_signal(barrier, inc=1, device_id={"tp": lax.rem(me + step, tp_size)}, device_id_type=MESH)
    for peer in (nxt, prv):
        pl.semaphore_signal(barrier, inc=1, device_id={"pp": peer}, device_id_type=MESH)

    loads = [
        pltpu.make_async_copy(wup_hbm, w_up.at[me], load_sem.at[0]),
        pltpu.make_async_copy(wq_hbm, raw.at[0], load_sem.at[1]),
        pltpu.make_async_copy(wk_hbm, raw.at[1], load_sem.at[2]),
        pltpu.make_async_copy(wv_hbm, raw.at[2], load_sem.at[3]),
        pltpu.make_async_copy(wo_hbm, w_out.at[me, pl.ds(0, width)], load_sem.at[4]),
        pltpu.make_async_copy(wdown_hbm, w_out.at[me, pl.ds(width, wdown_hbm.shape[0])], load_sem.at[5]),
    ]
    for load in loads:
        load.start()
    ln_half[...] = ln_ref[...]
    ln_half[2:4, :] = 0.5 * ln_ref[2:4, :]
    pl.semaphore_wait(barrier, tp_size + 1)

    def token_rows(owner):
        return pl.ds(pl.multiple_of(owner * tokens, tokens), tokens)

    def seq_rows(owner):
        return pl.ds(owner * num_seq, num_seq)

    def collect(micro, _):
        pltpu.make_async_copy(x_hbm.at[micro, seq_rows(me)], ys.at[micro, :, token_rows(me), :], x_local).start()
        for step in range(1, tp_size):
            peer = lax.rem(me + step, tp_size)
            pltpu.make_async_remote_copy(
                src_ref=x_hbm.at[micro, seq_rows(peer)], dst_ref=ys.at[micro, :, token_rows(me), :],
                send_sem=x_send, recv_sem=x_recv, device_id={"tp": peer}, device_id_type=MESH).start()
        return 0

    def pp_copy(micro, seq):
        return pltpu.make_async_remote_copy(
            src_ref=ys.at[micro, seq], dst_ref=xs.at[micro, seq], send_sem=pp_send,
            recv_sem=pp_recv.at[micro, seq], device_id={"pp": nxt}, device_id_type=MESH)

    @pl.when(stage == last_stage)
    def _():
        lax.fori_loop(0, num_micro, collect, 0)

    def halves(ref):
        rows = ref.shape[1] // 2
        return [(ref, 0, rows), (ref, rows, rows)]

    arrays = (w_up, w_qkv, w_out)
    chunks = [chunk for ref in arrays for chunk in halves(ref)]

    def shard_copy(index, owner, send_sem, recv_sem, peer):
        ref, start, rows = chunks[index]
        piece = ref.at[owner, pl.ds(start, rows)]
        return pltpu.make_async_remote_copy(
            src_ref=piece, dst_ref=piece, send_sem=send_sem, recv_sem=recv_sem, device_id={"tp": peer}, device_id_type=MESH)

    def own_copy(index, way):
        return shard_copy(index, me, w_send, near_recv.at[way, index], right if way == 0 else left)

    def near_copy(index, way):
        return shard_copy(index, left if way == 0 else right, w_send, near_recv.at[way, index],
                          right if way == 0 else left)

    def fwd_copy(index):
        way = index % 2
        return shard_copy(index, left if way == 0 else right, w_send, far_recv.at[index // 2],
                          right if way == 0 else left)

    def take(sem, *refs):
        for ref in refs:
            pltpu.make_async_copy(ref, ref, sem).wait()

    def send_own(first):
        for way in range(2):
            own_copy(first + way, way).start()
        for way in range(2):
            own_copy(first + 1 - way, way).start()

    loads[0].wait()
    send_own(0)
    for load in loads[1:4]:
        load.wait()
    head_dim = width // heads
    part = head_dim // 2
    for which in range(3):
        starts = [head * head_dim + side * part for side in range(2) for head in range(heads)]
        if which == 2:
            starts = list(range(0, width, part))
        for col in range(0, d_model, width):
            block = jnp.concatenate([raw[which, start:start + part, col:col + width] for start in starts], axis=0)
            w_qkv[me, col:col + width, which * width:(which + 1) * width] = block.T

    send_own(2)
    for load in loads[4:]:
        load.wait()
    send_own(4)

    own_blocks = ys.at[pl.ds(0, num_micro // tp_size)]
    other_blocks = ys.at[pl.ds(0, num_micro // tp_size * (tp_size - 1))]

    @pl.when(stage == last_stage)
    def _():
        take(x_local, own_blocks)
        take(x_recv, other_blocks)

        def hand_on(micro, _):
            for seq in range(num_seq):
                pp_copy(micro, seq).start()
            return 0
        lax.fori_loop(0, num_micro, hand_on, 0)

    for first in (0, 2, 4):
        for way in range(2):
            near_copy(first + way, way).wait_recv()
            fwd_copy(first + way).start()
    for way in range(2):
        for index in range(0, len(chunks), 2):
            near_copy(index + 1 - way, way).wait_recv()

    @pl.when(stage == last_stage)
    def _():
        take(pp_send, ys)

    def o_copy(micro, seq, step):
        peer = lax.rem(me + step, tp_size)
        return pltpu.make_async_remote_copy(
            src_ref=ys.at[micro, seq, token_rows(peer), :], dst_ref=out.at[micro, me * num_seq + seq],
            send_sem=o_send, recv_sem=o_recv, device_id={"tp": peer}, device_id_type=MESH)

    def hand_over(micro, seq):
        @pl.when(stage < last_stage)
        def _():
            pp_copy(micro, seq).start()

    def put_out(micro, seq):
        out[micro, me * num_seq + seq] = ys[micro, seq, token_rows(me), :]
        for step in range(1, tp_size):
            o_copy(micro, seq, step).start()

    work = (h_attn, h_mlp, acc, w_qkv, w_up, w_out, rope, masks, mixed)

    pp_copy(0, 0).wait_recv()
    layer_norms(xs[0, 0], ln_half, h_attn, h_mlp, acc)
    add_layer(heads, [me, left, right], *work)
    for index in range(2):
        take(far_recv.at[index], arrays[index].at[far])
    add_layer(heads, [far], *work, before_last_out=lambda: take(far_recv.at[2], w_out.at[far]))
    ys[0, 0] = acc[...].astype(BF16)
    hand_over(0, 0)

    def unit(index, _):
        micro, seq = index // num_seq, lax.rem(index, num_seq)
        pp_copy(micro, seq).wait_recv()
        put_out((index - 1) // num_seq, lax.rem(index - 1, num_seq))
        layer_norms(xs[micro, seq], ln_half, h_attn, h_mlp, acc)
        add_layer(heads, list(range(tp_size)), *work)
        ys[micro, seq] = acc[...].astype(BF16)
        hand_over(micro, seq)
        return 0

    lax.fori_loop(1, num_micro * num_seq, unit, 0)
    put_out(num_micro - 1, num_seq - 1)

    take(w_send, w_out, w_up)

    @pl.when(stage == last_stage)
    def _():
        take(x_send, other_blocks)

    @pl.when(stage < last_stage)
    def _():
        take(pp_send, ys)
    take(o_send, other_blocks)
    take(o_recv, other_blocks)


def solution(mesh):
    tp_size, pp_size = mesh.shape["tp"], mesh.shape["pp"]

    def stage_body(x_in, ln_params, w_q, w_k, w_v, w_o, w_up, w_down):
        num_micro, batch, tokens, d_model = x_in.shape
        heads, head_dim = w_k.shape[2:]
        width = heads * head_dim
        hidden = w_up.shape[2]
        seq_len = tokens * tp_size
        num_seq = batch // tp_size
        rope = jnp.asarray(rope_tables(seq_len, head_dim, heads))
        masks = jnp.asarray(head_masks(head_dim, heads), dtype=BF16)
        wq_t = jnp.transpose(w_q[0], (1, 2, 3, 0)).reshape(width, d_model)
        wk_t = jnp.transpose(w_k[0], (1, 2, 0)).reshape(width, d_model)
        wv_t = jnp.transpose(w_v[0], (1, 2, 0)).reshape(width, d_model)
        vmem = pl.BlockSpec(memory_space=pltpu.VMEM)
        hbm = pl.BlockSpec(memory_space=pl.ANY)
        dma = pltpu.SemaphoreType.DMA
        out = pl.pallas_call(
            functools.partial(kernel, tp_size, pp_size, heads),
            out_shape=pltpu.VMEM(x_in.shape, BF16),
            in_specs=[hbm, vmem, hbm, hbm, hbm, hbm, hbm, hbm, vmem, vmem],
            out_specs=vmem,
            scratch_shapes=[
                pltpu.VMEM((tp_size, d_model, 3 * width), BF16),
                pltpu.VMEM((tp_size, d_model, hidden), BF16),
                pltpu.VMEM((tp_size, width + hidden, d_model), BF16),
                pltpu.VMEM((3, width, d_model), BF16),
                pltpu.VMEM((num_micro, num_seq, seq_len, d_model), BF16),
                pltpu.VMEM((num_micro, num_seq, seq_len, d_model), BF16),
                pltpu.VMEM((4, d_model), F32),
                pltpu.VMEM((seq_len, d_model), BF16),
                pltpu.VMEM((seq_len, d_model), BF16),
                pltpu.VMEM((seq_len, d_model), F32),
                pltpu.VMEM((2, seq_len, width + hidden), BF16),
                dma((6,)), dma, dma((2, 6)), dma((3,)), dma, dma, dma, dma, dma((num_micro, num_seq)), dma, dma,
            ],
            compiler_params=pltpu.CompilerParams(
                collective_id=0, has_side_effects=True, vmem_limit_bytes=54 * 1024 * 1024),
            name="stage",
        )(x_in, ln_params[0], wq_t, wk_t, wv_t, w_o[0].reshape(width, d_model), w_up[0], w_down[0], rope, masks)
        return out[None]

    in_specs = (P(None, "dp", "tp", None), P("pp", None, None), P("pp", None, "tp", None, None), P("pp", None, "tp", None), P("pp", None, "tp", None), P("pp", "tp", None, None, None), P("pp", None, "tp"), P("pp", "tp", None))
    return jax.shard_map(stage_body, mesh=mesh, in_specs=in_specs, out_specs=P("pp", None, "dp", "tp", None), check_vma=False)
```

```python
import functools

import jax
import jax.numpy as jnp
import numpy as np
from jax import lax
from jax.experimental import pallas as pl
from jax.experimental.pallas import tpu as pltpu
from jax.sharding import PartitionSpec as P

LN_EPS = 1e-5
ROPE_BASE = 10000.0
F32, BF16 = jnp.float32, jnp.bfloat16
MESH = pl.DeviceIdType.MESH
DETOURS = ((96, 2), (192, 1))


def rope_tables(seq_len, head_dim, heads):
    half = head_dim // 2
    inv_freq = (ROPE_BASE ** (-2.0 * np.arange(half) / head_dim)).astype(np.float32)
    angles = np.arange(seq_len, dtype=np.float32)[:, None] * inv_freq[None, :]
    cos = np.tile(np.cos(angles.astype(np.float64)), (1, heads)).astype(np.float32)
    sin = np.tile(np.sin(angles.astype(np.float64)), (1, heads)).astype(np.float32)
    scale = np.float32(head_dim ** -0.5)
    return np.stack([cos * scale, sin * scale, cos, sin])


def head_masks(head_dim, heads):
    half = head_dim // 2
    lanes = np.arange(heads * head_dim)
    roped = np.stack([(lanes % (heads * half)) // half == head for head in range(heads)])
    plain = np.stack([lanes // head_dim == head for head in range(heads)])
    return np.stack([roped, plain]).astype(np.float32)


def dot(lhs, rhs):
    return jnp.dot(lhs, rhs, preferred_element_type=F32)


def layer_norms(x, ln_ref, h_attn, h_mlp, acc):
    x_f32 = x.astype(F32)
    acc[...] = x_f32
    centred = x_f32 - jnp.mean(x_f32, axis=-1, keepdims=True)
    variance = jnp.mean(centred * centred, axis=-1, keepdims=True)
    normed = centred * lax.rsqrt(variance + LN_EPS)
    h_attn[...] = (normed * ln_ref[0:1, :] + ln_ref[1:2, :]).astype(BF16)
    h_mlp[...] = (normed * ln_ref[2:3, :] + ln_ref[3:4, :]).astype(BF16)


def roped(first, second, cos, sin):
    return jnp.concatenate([first * cos - second * sin, second * cos + first * sin], axis=1).astype(BF16)


def causal_softmax(scores, allowed):
    masked = jnp.where(allowed, scores, -1e30)
    weight = jnp.exp(masked - jnp.max(masked, axis=1, keepdims=True))
    return (weight * (1.0 / jnp.sum(weight, axis=1, keepdims=True))).astype(BF16)


def gelu_of_half(half_x):
    return (half_x * (1.0 + lax.erf(half_x * np.float32(2.0 ** 0.5)))).astype(BF16)


def add_layer(heads, shards, h_attn, h_mlp, acc, w_qkv, w_up, w_out, rope, masks, mixed, before_last_out=None):
    seq_len, d_model = acc.shape
    width = w_qkv.shape[2] // 3
    half = width // 2
    cols = d_model // heads
    hidden = w_up.shape[2] // heads
    allowed = lax.broadcasted_iota(jnp.int32, (seq_len, seq_len), 0) >= lax.broadcasted_iota(jnp.int32, (seq_len, seq_len), 1)
    raw, ups, score_pairs, probs = {}, {}, {}, {}

    def project(turn, which):
        if turn < len(shards):
            raw[which] = dot(h_attn[...], w_qkv[shards[turn], :, which * width:(which + 1) * width])

    def score(pair):
        k_pair = jnp.concatenate([raw[1] * masks[0, h:h + 1, :] for h in (2 * pair, 2 * pair + 1)], axis=0)
        score_pairs[pair] = lax.dot_general(raw[0], k_pair, (((1,), (1,)), ((), ())), preferred_element_type=F32)

    def soften(head):
        side = head % 2 * seq_len
        probs[head] = causal_softmax(score_pairs[head // 2][:, side:side + seq_len], allowed)

    def context(turn):
        v_heads = jnp.concatenate([v * masks[1, h:h + 1, :] for h in range(heads)], axis=0)
        mixed[turn % 2, :, :width] = dot(jnp.concatenate([probs[h] for h in range(heads)], axis=1), v_heads).astype(BF16)

    def up(turn, part):
        ups[part] = dot(h_mlp[...], w_up[shards[turn], :, part * hidden:(part + 1) * hidden])

    def gelu(turn, part):
        mixed[turn % 2, :, width + part * hidden:width + (part + 1) * hidden] = gelu_of_half(ups[part])

    def add_out(turn, part):
        piece = slice(part * cols, (part + 1) * cols)
        acc[:, piece] += dot(mixed[turn % 2], w_out[shards[turn], :, piece])

    for which in range(3):
        project(0, which)
    for turn in range(len(shards)):
        raw[0] = roped(raw[0][:, :half], raw[0][:, half:], rope[0], rope[1])
        raw[1] = roped(raw[1][:, :half], raw[1][:, half:], rope[2], rope[3])
        v = raw[2].astype(BF16)
        score(0)
        if turn == 0:
            score(1)
            for head in range(heads):
                up(turn, head)
                if head > 0:
                    gelu(turn, head - 1)
                soften(head)
            project(turn + 1, 0)
            project(turn + 1, 1)
            gelu(turn, 3)
            context(turn)
            project(turn + 1, 2)
        else:
            add_out(turn - 1, 0)
            score(1)
            for head in range(heads):
                soften(head)
                if head < 3:
                    add_out(turn - 1, head + 1)
            up(turn, 0)
            up(turn, 1)
            gelu(turn, 0)
            context(turn)
            up(turn, 2)
            gelu(turn, 1)
            up(turn, 3)
            gelu(turn, 2)
            project(turn + 1, 0)
            gelu(turn, 3)
            project(turn + 1, 1)
            project(turn + 1, 2)
    if before_last_out is not None:
        before_last_out()
    for part in range(heads):
        add_out(len(shards) - 1, part)


def kernel(tp_size, pp_size, heads, x_hbm, ln_ref, wq_hbm, wk_hbm, wv_hbm, wo_hbm, wup_hbm, wdown_hbm, rope, masks, out,
           w_qkv, w_up, w_out, raw, detour, xs, ys, ln_half, h_attn, h_mlp, acc, mixed,
           load_sem, w_send, near_recv, far_recv, d_send, d_in, d_out, x_send, x_recv, x_local, x_hand, pp_send, pp_recv, o_send, o_recv):
    me = lax.axis_index("tp")
    stage = lax.axis_index("pp")
    right, left = lax.rem(me + 1, tp_size), lax.rem(me + tp_size - 1, tp_size)
    far = lax.rem(me + 2, tp_size)
    nxt = lax.rem(stage + 1, pp_size)
    last_stage = pp_size - 1
    num_micro, num_seq, seq_len, d_model = xs.shape
    tokens = seq_len // tp_size
    width = raw.shape[1]

    barrier = pltpu.get_barrier_semaphore()

    def knock(index, _):
        peer = {"tp": index // pp_size, "pp": lax.rem(index, pp_size)}
        pl.semaphore_signal(barrier, inc=1, device_id=peer, device_id_type=MESH)
        return 0
    lax.fori_loop(0, tp_size * pp_size, knock, 0)

    loads = [
        pltpu.make_async_copy(wup_hbm, w_up.at[me], load_sem.at[0]),
        pltpu.make_async_copy(wq_hbm, raw.at[0], load_sem.at[1]),
        pltpu.make_async_copy(wk_hbm, raw.at[1], load_sem.at[2]),
        pltpu.make_async_copy(wv_hbm, raw.at[2], load_sem.at[3]),
        pltpu.make_async_copy(wo_hbm, w_out.at[me, pl.ds(0, width)], load_sem.at[4]),
        pltpu.make_async_copy(wdown_hbm, w_out.at[me, pl.ds(width, wdown_hbm.shape[0])], load_sem.at[5]),
    ]
    for load in loads:
        load.start()
    ln_half[...] = ln_ref[...]
    ln_half[2:4, :] = 0.5 * ln_ref[2:4, :]
    pl.semaphore_wait(barrier, tp_size * pp_size)

    def token_rows(owner):
        return pl.ds(pl.multiple_of(owner * tokens, tokens), tokens)

    def seq_rows(owner):
        return pl.ds(owner * num_seq, num_seq)

    half_micro = num_micro // 2
    collects = (stage == last_stage) | (stage == last_stage - 2)
    first_micro = jnp.where(stage == last_stage, 0, half_micro)

    def collect(index, _):
        micro = first_micro + index
        pltpu.make_async_copy(x_hbm.at[micro, seq_rows(me)], ys.at[micro, :, token_rows(me), :], x_local).start()
        for step in range(1, tp_size):
            peer = lax.rem(me + step, tp_size)
            pltpu.make_async_remote_copy(
                src_ref=x_hbm.at[micro, seq_rows(peer)], dst_ref=ys.at[micro, :, token_rows(me), :],
                send_sem=x_send, recv_sem=x_recv, device_id={"tp": peer}, device_id_type=MESH).start()
        return 0

    def hand_on(index, _):
        micro = first_micro + index
        for seq in range(num_seq):
            pltpu.make_async_remote_copy(
                src_ref=ys.at[micro, seq], dst_ref=xs.at[micro, seq], send_sem=x_hand,
                recv_sem=pp_recv.at[micro, seq], device_id={"pp": 0}, device_id_type=MESH).start()
        return 0

    def pp_copy(micro, seq):
        return pltpu.make_async_remote_copy(
            src_ref=ys.at[micro, seq], dst_ref=xs.at[micro, seq], send_sem=pp_send,
            recv_sem=pp_recv.at[micro, seq], device_id={"pp": nxt}, device_id_type=MESH)

    @pl.when(collects)
    def _():
        lax.fori_loop(0, half_micro, collect, 0)

    arrays = (w_up, w_qkv, w_out)
    parts = [(w_up, 0, w_up.shape[1], 0), (w_qkv, 0, w_qkv.shape[1], 0)]
    start = 0
    for rows, stages in DETOURS + ((w_out.shape[1] - sum(rows for rows, _ in DETOURS), 0),):
        parts.append((w_out, start, rows, stages))
        start += rows
    chunks = [(ref, start + side * rows // 2, rows // 2) for ref, start, rows, _ in parts for side in range(2)]

    def on_ring(part, action):
        stages = parts[part][3]
        if stages:
            pl.when(stage >= stages)(action)
        else:
            action()

    def shard_copy(index, owner, send_sem, recv_sem, peer):
        ref, start, rows = chunks[index]
        piece = ref.at[owner, pl.ds(start, rows)]
        return pltpu.make_async_remote_copy(
            src_ref=piece, dst_ref=piece, send_sem=send_sem, recv_sem=recv_sem, device_id={"tp": peer}, device_id_type=MESH)

    def own_copy(index, way):
        return shard_copy(index, me, w_send, near_recv.at[way, index], right if way == 0 else left)

    def near_copy(index, way):
        return shard_copy(index, left if way == 0 else right, w_send, near_recv.at[way, index],
                          right if way == 0 else left)

    def fwd_copy(index):
        way = index % 2
        return shard_copy(index, left if way == 0 else right, w_send, far_recv.at[index // 2],
                          right if way == 0 else left)

    def take(sem, *refs):
        for ref in refs:
            pltpu.make_async_copy(ref, ref, sem).wait()

    def send_own(part):
        def send():
            for way in range(2):
                own_copy(2 * part + way, way).start()
            for way in range(2):
                own_copy(2 * part + 1 - way, way).start()
        on_ring(part, send)

    def pass_on(part):
        def forward():
            for way in range(2):
                near_copy(2 * part + way, way).wait_recv()
                fwd_copy(2 * part + way).start()
        on_ring(part, forward)

    def take_near(part):
        def wait():
            for way in range(2):
                near_copy(2 * part + 1 - way, way).wait_recv()
        on_ring(part, wait)

    def take_far(part):
        ref, start, rows, _ = parts[part]
        on_ring(part, lambda: take(far_recv.at[part], ref.at[far, pl.ds(start, rows)]))

    helper_base = pp_size - 2
    detour_parts = [(2 + index, sum(rows for rows, _ in DETOURS[:index]), *DETOURS[index]) for index in range(len(DETOURS))]

    def send_detours():
        for part, start, rows, stages in detour_parts:
            @pl.when(stage < stages)
            def _():
                for step in range(1, tp_size):
                    pltpu.make_async_remote_copy(
                        src_ref=w_out.at[me, pl.ds(start, rows)], dst_ref=detour.at[step - 1, pl.ds(start, rows)],
                        send_sem=w_send, recv_sem=d_in.at[part - 2],
                        device_id={"tp": lax.rem(me + step, tp_size), "pp": stage + helper_base}, device_id_type=MESH).start()

    def pass_detours():
        for part, start, rows, stages in detour_parts:
            @pl.when((stage >= helper_base) & (stage < helper_base + stages))
            def _():
                take(d_in.at[part - 2], detour.at[:, pl.ds(start, rows)])
                for step in range(1, tp_size):
                    pltpu.make_async_remote_copy(
                        src_ref=detour.at[step - 1, pl.ds(start, rows)],
                        dst_ref=w_out.at[lax.rem(me + tp_size - step, tp_size), pl.ds(start, rows)],
                        send_sem=d_send.at[part - 2], recv_sem=d_out.at[part - 2],
                        device_id={"pp": stage - helper_base}, device_id_type=MESH).start()

    def take_detours():
        for part, start, rows, stages in detour_parts:
            @pl.when(stage < stages)
            def _():
                take(d_out.at[part - 2], detour.at[:, pl.ds(start, rows)])

    for load in loads[:1] + loads[4:]:
        load.wait()
    send_detours()
    send_own(0)
    for load in loads[1:4]:
        load.wait()
    head_dim = width // heads
    part = head_dim // 2
    for which in range(3):
        starts = [head * head_dim + side * part for side in range(2) for head in range(heads)]
        if which == 2:
            starts = list(range(0, width, part))
        for col in range(0, d_model, width):
            block = jnp.concatenate([raw[which, start:start + part, col:col + width] for start in starts], axis=0)
            w_qkv[me, col:col + width, which * width:(which + 1) * width] = block.T

    for part in range(1, len(parts)):
        send_own(part)
    pass_detours()

    own_blocks = ys.at[pl.ds(0, num_micro // tp_size)]
    other_blocks = ys.at[pl.ds(0, num_micro // tp_size * (tp_size - 1))]
    half_own, half_others = ys.at[pl.ds(0, half_micro // tp_size)], ys.at[pl.ds(0, half_micro // tp_size * (tp_size - 1))]

    @pl.when(collects)
    def _():
        take(x_local, half_own)
        take(x_recv, half_others)
        lax.fori_loop(0, half_micro, hand_on, 0)

    for part in range(len(parts)):
        pass_on(part)
    for part in range(len(parts)):
        take_near(part)
    take_detours()

    @pl.when(collects)
    def _():
        take(x_hand, ys.at[pl.ds(0, half_micro)])

    def o_copy(micro, seq, step):
        peer = lax.rem(me + step, tp_size)
        return pltpu.make_async_remote_copy(
            src_ref=ys.at[micro, seq, token_rows(peer), :], dst_ref=out.at[micro, me * num_seq + seq],
            send_sem=o_send, recv_sem=o_recv, device_id={"tp": peer}, device_id_type=MESH)

    def hand_over(micro, seq):
        @pl.when(stage < last_stage)
        def _():
            pp_copy(micro, seq).start()

    def put_out(micro, seq):
        out[micro, me * num_seq + seq] = ys[micro, seq, token_rows(me), :]
        for step in range(1, tp_size):
            o_copy(micro, seq, step).start()

    work = (h_attn, h_mlp, acc, w_qkv, w_up, w_out, rope, masks, mixed)

    pp_copy(0, 0).wait_recv()
    layer_norms(xs[0, 0], ln_half, h_attn, h_mlp, acc)
    add_layer(heads, [me, left, right], *work)
    take_far(0)
    take_far(1)

    def rest_of_far():
        for part in range(2, len(parts)):
            take_far(part)
    add_layer(heads, [far], *work, before_last_out=rest_of_far)
    ys[0, 0] = acc[...].astype(BF16)
    hand_over(0, 0)

    def unit(index, _):
        micro, seq = index // num_seq, lax.rem(index, num_seq)
        pp_copy(micro, seq).wait_recv()
        put_out((index - 1) // num_seq, lax.rem(index - 1, num_seq))
        layer_norms(xs[micro, seq], ln_half, h_attn, h_mlp, acc)
        add_layer(heads, list(range(tp_size)), *work)
        ys[micro, seq] = acc[...].astype(BF16)
        hand_over(micro, seq)
        return 0

    lax.fori_loop(1, num_micro * num_seq, unit, 0)
    put_out(num_micro - 1, num_seq - 1)

    take(w_send, w_out, w_up)

    for part, start, rows, stages in detour_parts:
        @pl.when((stage >= helper_base) & (stage < helper_base + stages))
        def _():
            take(d_send.at[part - 2], detour.at[:, pl.ds(start, rows)])

    @pl.when(collects)
    def _():
        take(x_send, half_others)

    @pl.when(stage < last_stage)
    def _():
        take(pp_send, ys)
    take(o_send, other_blocks)
    take(o_recv, other_blocks)


def solution(mesh):
    tp_size, pp_size = mesh.shape["tp"], mesh.shape["pp"]

    def stage_body(x_in, ln_params, w_q, w_k, w_v, w_o, w_up, w_down):
        num_micro, batch, tokens, d_model = x_in.shape
        heads, head_dim = w_k.shape[2:]
        width = heads * head_dim
        hidden = w_up.shape[2]
        seq_len = tokens * tp_size
        num_seq = batch // tp_size
        rope = jnp.asarray(rope_tables(seq_len, head_dim, heads))
        masks = jnp.asarray(head_masks(head_dim, heads), dtype=BF16)
        wq_t = jnp.transpose(w_q[0], (1, 2, 3, 0)).reshape(width, d_model)
        wk_t = jnp.transpose(w_k[0], (1, 2, 0)).reshape(width, d_model)
        wv_t = jnp.transpose(w_v[0], (1, 2, 0)).reshape(width, d_model)
        vmem = pl.BlockSpec(memory_space=pltpu.VMEM)
        hbm = pl.BlockSpec(memory_space=pl.ANY)
        dma = pltpu.SemaphoreType.DMA
        out = pl.pallas_call(
            functools.partial(kernel, tp_size, pp_size, heads),
            out_shape=pltpu.VMEM(x_in.shape, BF16),
            in_specs=[hbm, vmem, hbm, hbm, hbm, hbm, hbm, hbm, vmem, vmem],
            out_specs=vmem,
            scratch_shapes=[
                pltpu.VMEM((tp_size, d_model, 3 * width), BF16),
                pltpu.VMEM((tp_size, d_model, hidden), BF16),
                pltpu.VMEM((tp_size, width + hidden, d_model), BF16),
                pltpu.VMEM((3, width, d_model), BF16),
                pltpu.VMEM((tp_size - 1, sum(rows for rows, _ in DETOURS), d_model), BF16),
                pltpu.VMEM((num_micro, num_seq, seq_len, d_model), BF16),
                pltpu.VMEM((num_micro, num_seq, seq_len, d_model), BF16),
                pltpu.VMEM((4, d_model), F32),
                pltpu.VMEM((seq_len, d_model), BF16),
                pltpu.VMEM((seq_len, d_model), BF16),
                pltpu.VMEM((seq_len, d_model), F32),
                pltpu.VMEM((2, seq_len, width + hidden), BF16),
                dma((6,)), dma, dma((2, 10)), dma((5,)), dma((2,)), dma((2,)), dma((2,)), dma, dma, dma, dma, dma, dma((num_micro, num_seq)), dma, dma,
            ],
            compiler_params=pltpu.CompilerParams(
                collective_id=0, has_side_effects=True, vmem_limit_bytes=54 * 1024 * 1024),
            name="stage",
        )(x_in, ln_params[0], wq_t, wk_t, wv_t, w_o[0].reshape(width, d_model), w_up[0], w_down[0], rope, masks)
        return out[None]

    in_specs = (P(None, "dp", "tp", None), P("pp", None, None), P("pp", None, "tp", None, None), P("pp", None, "tp", None), P("pp", None, "tp", None), P("pp", "tp", None, None, None), P("pp", None, "tp"), P("pp", "tp", None))
    return jax.shard_map(stage_body, mesh=mesh, in_specs=in_specs, out_specs=P("pp", None, "dp", "tp", None), check_vma=False)
```

```python
import functools

import jax
import jax.numpy as jnp
import numpy as np
from jax import lax
from jax.experimental import pallas as pl
from jax.experimental.pallas import tpu as pltpu
from jax.sharding import PartitionSpec as P

LN_EPS = 1e-5
ROPE_BASE = 10000.0
F32, BF16 = jnp.float32, jnp.bfloat16
MESH = pl.DeviceIdType.MESH
DETOURS = ((160, 0, 2, 4), (160, 0, 1, 6), (64, 2, 1, 2))
EARLY_MICRO = 10
HAND_AT, HANDED_AT = 5, 18


def rope_tables(seq_len, head_dim, heads):
    half = head_dim // 2
    inv_freq = (ROPE_BASE ** (-2.0 * np.arange(half) / head_dim)).astype(np.float32)
    angles = np.arange(seq_len, dtype=np.float32)[:, None] * inv_freq[None, :]
    cos = np.tile(np.cos(angles.astype(np.float64)), (1, heads)).astype(np.float32)
    sin = np.tile(np.sin(angles.astype(np.float64)), (1, heads)).astype(np.float32)
    scale = np.float32(head_dim ** -0.5)
    return np.stack([cos * scale, sin * scale, cos, sin])


def head_masks(head_dim, heads):
    half = head_dim // 2
    lanes = np.arange(heads * head_dim)
    roped = np.stack([(lanes % (heads * half)) // half == head for head in range(heads)])
    plain = np.stack([lanes // head_dim == head for head in range(heads)])
    return np.stack([roped, plain]).astype(np.float32)


def dot(lhs, rhs):
    return jnp.dot(lhs, rhs, preferred_element_type=F32)


def layer_norms(x, ln_ref, h_attn, h_mlp, acc):
    x_f32 = x.astype(F32)
    acc[...] = x_f32
    centred = x_f32 - jnp.mean(x_f32, axis=-1, keepdims=True)
    variance = jnp.mean(centred * centred, axis=-1, keepdims=True)
    normed = centred * lax.rsqrt(variance + LN_EPS)
    h_attn[...] = (normed * ln_ref[0:1, :] + ln_ref[1:2, :]).astype(BF16)
    h_mlp[...] = (normed * ln_ref[2:3, :] + ln_ref[3:4, :]).astype(BF16)


def roped(first, second, cos, sin):
    return jnp.concatenate([first * cos - second * sin, second * cos + first * sin], axis=1).astype(BF16)


def causal_softmax(scores, allowed):
    masked = jnp.where(allowed, scores, -1e30)
    weight = jnp.exp(masked - jnp.max(masked, axis=1, keepdims=True))
    return (weight * (1.0 / jnp.sum(weight, axis=1, keepdims=True))).astype(BF16)


def gelu_of_half(half_x):
    return (half_x * (1.0 + lax.erf(half_x * np.float32(2.0 ** 0.5)))).astype(BF16)


def add_layer(heads, shards, h_attn, h_mlp, acc, w_qkv, w_up, w_out, rope, masks, mixed, before_last_out=None):
    seq_len, d_model = acc.shape
    width = w_qkv.shape[2] // 3
    half = width // 2
    cols = d_model // heads
    hidden = w_up.shape[2] // heads
    allowed = lax.broadcasted_iota(jnp.int32, (seq_len, seq_len), 0) >= lax.broadcasted_iota(jnp.int32, (seq_len, seq_len), 1)
    raw, ups, score_pairs, probs = {}, {}, {}, {}

    def project(turn, which):
        if turn < len(shards):
            raw[which] = dot(h_attn[...], w_qkv[shards[turn], :, which * width:(which + 1) * width])

    def score(pair):
        k_pair = jnp.concatenate([raw[1] * masks[0, h:h + 1, :] for h in (2 * pair, 2 * pair + 1)], axis=0)
        score_pairs[pair] = lax.dot_general(raw[0], k_pair, (((1,), (1,)), ((), ())), preferred_element_type=F32)

    def soften(head):
        side = head % 2 * seq_len
        probs[head] = causal_softmax(score_pairs[head // 2][:, side:side + seq_len], allowed)

    def context(turn):
        v_heads = jnp.concatenate([v * masks[1, h:h + 1, :] for h in range(heads)], axis=0)
        mixed[turn % 2, :, :width] = dot(jnp.concatenate([probs[h] for h in range(heads)], axis=1), v_heads).astype(BF16)

    def up(turn, part):
        ups[part] = dot(h_mlp[...], w_up[shards[turn], :, part * hidden:(part + 1) * hidden])

    def gelu(turn, part):
        mixed[turn % 2, :, width + part * hidden:width + (part + 1) * hidden] = gelu_of_half(ups[part])

    def add_out(turn, part):
        piece = slice(part * cols, (part + 1) * cols)
        acc[:, piece] += dot(mixed[turn % 2], w_out[shards[turn], :, piece])

    for which in range(3):
        project(0, which)
    for turn in range(len(shards)):
        raw[0] = roped(raw[0][:, :half], raw[0][:, half:], rope[0], rope[1])
        raw[1] = roped(raw[1][:, :half], raw[1][:, half:], rope[2], rope[3])
        v = raw[2].astype(BF16)
        score(0)
        if turn == 0:
            score(1)
            for head in range(heads):
                up(turn, head)
                if head > 0:
                    gelu(turn, head - 1)
                soften(head)
            project(turn + 1, 0)
            project(turn + 1, 1)
            gelu(turn, 3)
            context(turn)
            project(turn + 1, 2)
        else:
            add_out(turn - 1, 0)
            score(1)
            for head in range(heads):
                soften(head)
                if head < 3:
                    add_out(turn - 1, head + 1)
            up(turn, 0)
            up(turn, 1)
            gelu(turn, 0)
            context(turn)
            up(turn, 2)
            gelu(turn, 1)
            up(turn, 3)
            gelu(turn, 2)
            project(turn + 1, 0)
            gelu(turn, 3)
            project(turn + 1, 1)
            project(turn + 1, 2)
    if before_last_out is not None:
        before_last_out()
    for part in range(heads):
        add_out(len(shards) - 1, part)


def kernel(tp_size, pp_size, heads, x_hbm, ln_ref, wq_hbm, wk_hbm, wv_hbm, wo_hbm, wup_hbm, wdown_hbm, rope, masks, out,
           w_qkv, w_up, w_out, raw, detour, xs, ys, ln_half, h_attn, h_mlp, acc, mixed,
           load_sem, w_send, near_recv, far_recv, d_send, d_in, d_out, x_send, x_recv, x_local, x_hand, pp_send, pp_recv, o_send, o_recv):
    me = lax.axis_index("tp")
    stage = lax.axis_index("pp")
    right, left = lax.rem(me + 1, tp_size), lax.rem(me + tp_size - 1, tp_size)
    far = lax.rem(me + 2, tp_size)
    nxt = lax.rem(stage + 1, pp_size)
    last_stage = pp_size - 1
    num_micro, num_seq, seq_len, d_model = xs.shape
    tokens = seq_len // tp_size
    width = raw.shape[1]

    barrier = pltpu.get_barrier_semaphore()

    def knock(index, _):
        peer = {"tp": index // pp_size, "pp": lax.rem(index, pp_size)}
        pl.semaphore_signal(barrier, inc=1, device_id=peer, device_id_type=MESH)
        return 0
    lax.fori_loop(0, tp_size * pp_size, knock, 0)

    loads = [
        pltpu.make_async_copy(wup_hbm, w_up.at[me], load_sem.at[0]),
        pltpu.make_async_copy(wq_hbm, raw.at[0], load_sem.at[1]),
        pltpu.make_async_copy(wk_hbm, raw.at[1], load_sem.at[2]),
        pltpu.make_async_copy(wv_hbm, raw.at[2], load_sem.at[3]),
        pltpu.make_async_copy(wo_hbm, w_out.at[me, pl.ds(0, width)], load_sem.at[4]),
        pltpu.make_async_copy(wdown_hbm, w_out.at[me, pl.ds(width, wdown_hbm.shape[0])], load_sem.at[5]),
    ]
    for load in loads:
        load.start()
    ln_half[...] = ln_ref[...]
    ln_half[2:4, :] = 0.5 * ln_ref[2:4, :]
    pl.semaphore_wait(barrier, tp_size * pp_size)

    def token_rows(owner):
        return pl.ds(pl.multiple_of(owner * tokens, tokens), tokens)

    def seq_rows(owner):
        return pl.ds(owner * num_seq, num_seq)

    early = (stage == last_stage, 0, EARLY_MICRO)
    late = (stage == last_stage - 2, EARLY_MICRO, num_micro - EARLY_MICRO)

    def collect(group):
        def one(index, _):
            micro = group[1] + index
            pltpu.make_async_copy(x_hbm.at[micro, seq_rows(me)], ys.at[micro, :, token_rows(me), :], x_local).start()
            for step in range(1, tp_size):
                peer = lax.rem(me + step, tp_size)
                pltpu.make_async_remote_copy(
                    src_ref=x_hbm.at[micro, seq_rows(peer)], dst_ref=ys.at[micro, :, token_rows(me), :],
                    send_sem=x_send, recv_sem=x_recv, device_id={"tp": peer}, device_id_type=MESH).start()
            return 0
        lax.fori_loop(0, group[2], one, 0)

    def take_blocks(sem, blocks):
        seqs = blocks * num_seq // tp_size
        take(sem, ys.at[pl.ds(0, seqs // num_seq)] if seqs % num_seq == 0 else ys.at[pl.ds(0, seqs), 0])

    def hand_on(group):
        take_blocks(x_local, group[2])
        take_blocks(x_recv, group[2] * (tp_size - 1))

        def one(index, _):
            micro = group[1] + index
            for seq in range(num_seq):
                pltpu.make_async_remote_copy(
                    src_ref=ys.at[micro, seq], dst_ref=xs.at[micro, seq], send_sem=x_hand,
                    recv_sem=pp_recv.at[micro, seq], device_id={"pp": 0}, device_id_type=MESH).start()
            return 0
        lax.fori_loop(0, group[2], one, 0)

    def handed(group):
        take_blocks(x_hand, group[2] * tp_size)
        take_blocks(x_send, group[2] * (tp_size - 1))

    def pp_copy(micro, seq):
        return pltpu.make_async_remote_copy(
            src_ref=ys.at[micro, seq], dst_ref=xs.at[micro, seq], send_sem=pp_send,
            recv_sem=pp_recv.at[micro, seq], device_id={"pp": nxt}, device_id_type=MESH)

    @pl.when(early[0])
    def _():
        collect(early)

    parts = [(w_up, 0, w_up.shape[1], (0, 0)), (w_qkv, 0, w_qkv.shape[1], (0, 0))]
    detour_parts = []
    start = 0
    for rows, first, count, later in DETOURS:
        detour_parts.append((len(detour_parts), pl.ds(start, rows), first, first + count, later))
        parts.append((w_out, start, rows, (first, first + count)))
        start += rows
    parts.append((w_out, start, w_out.shape[1] - start, (0, 0)))
    chunks = [(ref, start + side * rows // 2, rows // 2) for ref, start, rows, _ in parts for side in range(2)]

    def on_ring(part, action):
        first, end = parts[part][3]
        if end > first:
            pl.when((stage < first) | (stage >= end))(action)
        else:
            action()

    def shard_copy(index, owner, send_sem, recv_sem, peer):
        ref, start, rows = chunks[index]
        piece = ref.at[owner, pl.ds(start, rows)]
        return pltpu.make_async_remote_copy(
            src_ref=piece, dst_ref=piece, send_sem=send_sem, recv_sem=recv_sem, device_id={"tp": peer}, device_id_type=MESH)

    def own_copy(index, way):
        return shard_copy(index, me, w_send, near_recv.at[way, index], right if way == 0 else left)

    def near_copy(index, way):
        return shard_copy(index, left if way == 0 else right, w_send, near_recv.at[way, index],
                          right if way == 0 else left)

    def fwd_copy(index):
        way = index % 2
        return shard_copy(index, left if way == 0 else right, w_send, far_recv.at[index // 2],
                          right if way == 0 else left)

    def take(sem, *refs):
        for ref in refs:
            pltpu.make_async_copy(ref, ref, sem).wait()

    def send_own(part):
        def send():
            for way in range(2):
                own_copy(2 * part + way, way).start()
            for way in range(2):
                own_copy(2 * part + 1 - way, way).start()
        on_ring(part, send)

    def pass_on(part):
        def forward():
            for way in range(2):
                near_copy(2 * part + way, way).wait_recv()
                fwd_copy(2 * part + way).start()
        on_ring(part, forward)

    def take_near(part):
        def wait():
            for way in range(2):
                near_copy(2 * part + 1 - way, way).wait_recv()
        on_ring(part, wait)

    def take_far(part):
        ref, start, rows, _ = parts[part]
        on_ring(part, lambda: take(far_recv.at[part], ref.at[far, pl.ds(start, rows)]))

    def send_detours():
        for part, piece, first, end, later in detour_parts:
            @pl.when((stage >= first) & (stage < end))
            def _():
                for step in range(1, tp_size):
                    pltpu.make_async_remote_copy(
                        src_ref=w_out.at[me, piece], dst_ref=detour.at[step - 1, piece],
                        send_sem=w_send, recv_sem=d_in.at[part],
                        device_id={"tp": lax.rem(me + step, tp_size), "pp": stage + later}, device_id_type=MESH).start()

    def pass_detours():
        for part, piece, first, end, later in detour_parts:
            @pl.when((stage >= first + later) & (stage < end + later))
            def _():
                take(d_in.at[part], detour.at[:, piece])
                for step in range(1, tp_size):
                    pltpu.make_async_remote_copy(
                        src_ref=detour.at[step - 1, piece],
                        dst_ref=w_out.at[lax.rem(me + tp_size - step, tp_size), piece],
                        send_sem=d_send.at[part], recv_sem=d_out.at[part],
                        device_id={"pp": stage - later}, device_id_type=MESH).start()

    def take_detours():
        for part, piece, first, end, _ in detour_parts:
            @pl.when((stage >= first) & (stage < end))
            def _():
                take(d_out.at[part], detour.at[:, piece])

    for load in loads[:1] + loads[4:]:
        load.wait()
    send_detours()
    send_own(0)
    for load in loads[1:4]:
        load.wait()
    head_dim = width // heads
    part = head_dim // 2
    for which in range(3):
        starts = [head * head_dim + side * part for side in range(2) for head in range(heads)]
        if which == 2:
            starts = list(range(0, width, part))
        for col in range(0, d_model, width):
            block = jnp.concatenate([raw[which, start:start + part, col:col + width] for start in starts], axis=0)
            w_qkv[me, col:col + width, which * width:(which + 1) * width] = block.T

    for part in range(1, len(parts)):
        send_own(part)
    pass_detours()

    @pl.when(early[0])
    def _():
        hand_on(early)

    for part in range(len(parts)):
        pass_on(part)
    for part in range(len(parts)):
        take_near(part)
    take_detours()

    @pl.when(early[0])
    def _():
        handed(early)

    @pl.when(late[0])
    def _():
        collect(late)

    def o_copy(micro, seq, step):
        peer = lax.rem(me + step, tp_size)
        return pltpu.make_async_remote_copy(
            src_ref=ys.at[micro, seq, token_rows(peer), :], dst_ref=out.at[micro, me * num_seq + seq],
            send_sem=o_send, recv_sem=o_recv, device_id={"tp": peer}, device_id_type=MESH)

    def hand_over(micro, seq):
        @pl.when(stage < last_stage)
        def _():
            pp_copy(micro, seq).start()

    def put_out(micro, seq):
        out[micro, me * num_seq + seq] = ys[micro, seq, token_rows(me), :]
        for step in range(1, tp_size):
            o_copy(micro, seq, step).start()

    work = (h_attn, h_mlp, acc, w_qkv, w_up, w_out, rope, masks, mixed)

    pp_copy(0, 0).wait_recv()
    layer_norms(xs[0, 0], ln_half, h_attn, h_mlp, acc)
    add_layer(heads, [me, left, right], *work)
    take_far(0)
    take_far(1)

    def rest_of_far():
        for part in range(2, len(parts)):
            take_far(part)
    add_layer(heads, [far], *work, before_last_out=rest_of_far)
    ys[0, 0] = acc[...].astype(BF16)
    hand_over(0, 0)

    def unit(index, _):
        micro, seq = index // num_seq, lax.rem(index, num_seq)
        pp_copy(micro, seq).wait_recv()
        put_out((index - 1) // num_seq, lax.rem(index - 1, num_seq))
        layer_norms(xs[micro, seq], ln_half, h_attn, h_mlp, acc)
        add_layer(heads, list(range(tp_size)), *work)
        ys[micro, seq] = acc[...].astype(BF16)
        hand_over(micro, seq)

        @pl.when(late[0])
        def _():
            pl.when(index == HAND_AT)(lambda: hand_on(late))
            pl.when(index == HANDED_AT)(lambda: handed(late))
        return 0

    lax.fori_loop(1, num_micro * num_seq, unit, 0)
    put_out(num_micro - 1, num_seq - 1)

    take(w_send, w_out, w_up)

    for part, piece, first, end, later in detour_parts:
        @pl.when((stage >= first + later) & (stage < end + later))
        def _():
            take(d_send.at[part], detour.at[:, piece])

    @pl.when(stage < last_stage)
    def _():
        take(pp_send, ys)
    take_blocks(o_send, num_micro * (tp_size - 1))
    take_blocks(o_recv, num_micro * (tp_size - 1))


def solution(mesh):
    tp_size, pp_size = mesh.shape["tp"], mesh.shape["pp"]

    def stage_body(x_in, ln_params, w_q, w_k, w_v, w_o, w_up, w_down):
        num_micro, batch, tokens, d_model = x_in.shape
        heads, head_dim = w_k.shape[2:]
        width = heads * head_dim
        hidden = w_up.shape[2]
        seq_len = tokens * tp_size
        num_seq = batch // tp_size
        rope = jnp.asarray(rope_tables(seq_len, head_dim, heads))
        masks = jnp.asarray(head_masks(head_dim, heads), dtype=BF16)
        wq_t = jnp.transpose(w_q[0], (1, 2, 3, 0)).reshape(width, d_model)
        wk_t = jnp.transpose(w_k[0], (1, 2, 0)).reshape(width, d_model)
        wv_t = jnp.transpose(w_v[0], (1, 2, 0)).reshape(width, d_model)
        vmem = pl.BlockSpec(memory_space=pltpu.VMEM)
        hbm = pl.BlockSpec(memory_space=pl.ANY)
        dma = pltpu.SemaphoreType.DMA
        out = pl.pallas_call(
            functools.partial(kernel, tp_size, pp_size, heads),
            out_shape=pltpu.VMEM(x_in.shape, BF16),
            in_specs=[hbm, vmem, hbm, hbm, hbm, hbm, hbm, hbm, vmem, vmem],
            out_specs=vmem,
            scratch_shapes=[
                pltpu.VMEM((tp_size, d_model, 3 * width), BF16),
                pltpu.VMEM((tp_size, d_model, hidden), BF16),
                pltpu.VMEM((tp_size, width + hidden, d_model), BF16),
                pltpu.VMEM((3, width, d_model), BF16),
                pltpu.VMEM((tp_size - 1, sum(rows for rows, *_ in DETOURS), d_model), BF16),
                pltpu.VMEM((num_micro, num_seq, seq_len, d_model), BF16),
                pltpu.VMEM((num_micro, num_seq, seq_len, d_model), BF16),
                pltpu.VMEM((4, d_model), F32),
                pltpu.VMEM((seq_len, d_model), BF16),
                pltpu.VMEM((seq_len, d_model), BF16),
                pltpu.VMEM((seq_len, d_model), F32),
                pltpu.VMEM((2, seq_len, width + hidden), BF16),
                dma((6,)), dma, dma((2, 12)), dma((6,)), dma((3,)), dma((3,)), dma((3,)), dma, dma, dma, dma, dma, dma((num_micro, num_seq)), dma, dma,
            ],
            compiler_params=pltpu.CompilerParams(
                collective_id=0, has_side_effects=True, vmem_limit_bytes=54 * 1024 * 1024),
            name="stage",
        )(x_in, ln_params[0], wq_t, wk_t, wv_t, w_o[0].reshape(width, d_model), w_up[0], w_down[0], rope, masks)
        return out[None]

    in_specs = (P(None, "dp", "tp", None), P("pp", None, None), P("pp", None, "tp", None, None), P("pp", None, "tp", None), P("pp", None, "tp", None), P("pp", "tp", None, None, None), P("pp", None, "tp"), P("pp", "tp", None))
    return jax.shard_map(stage_body, mesh=mesh, in_specs=in_specs, out_specs=P("pp", None, "dp", "tp", None), check_vma=False)
```

```python
import functools

import jax
import jax.numpy as jnp
import numpy as np
from jax import lax
from jax.experimental import pallas as pl
from jax.experimental.pallas import tpu as pltpu
from jax.sharding import PartitionSpec as P

LN_EPS = 1e-5
ROPE_BASE = 10000.0
F32, BF16 = jnp.float32, jnp.bfloat16
MESH = pl.DeviceIdType.MESH
DETOURS = ((128, 0, 2, 4), (160, 0, 1, 6), (64, 2, 1, 2))
EARLY_MICRO = 10
HAND_AT, HANDED_AT = 9, 18


def rope_tables(seq_len, head_dim, heads):
    half = head_dim // 2
    inv_freq = (ROPE_BASE ** (-2.0 * np.arange(half) / head_dim)).astype(np.float32)
    angles = np.arange(seq_len, dtype=np.float32)[:, None] * inv_freq[None, :]
    cos = np.tile(np.cos(angles.astype(np.float64)), (1, heads)).astype(np.float32)
    sin = np.tile(np.sin(angles.astype(np.float64)), (1, heads)).astype(np.float32)
    scale = np.float32(head_dim ** -0.5)
    return np.stack([cos * scale, sin * scale, cos, sin])


def head_masks(head_dim, heads):
    half = head_dim // 2
    lanes = np.arange(heads * head_dim)
    roped = np.stack([(lanes % (heads * half)) // half == head for head in range(heads)])
    plain = np.stack([lanes // head_dim == head for head in range(heads)])
    return np.stack([roped, plain]).astype(np.float32)


def dot(lhs, rhs):
    return jnp.dot(lhs, rhs, preferred_element_type=F32)


def layer_norms(x, ln_ref, h_attn, h_mlp, acc):
    x_f32 = x.astype(F32)
    acc[...] = x_f32
    centred = x_f32 - jnp.mean(x_f32, axis=-1, keepdims=True)
    variance = jnp.mean(centred * centred, axis=-1, keepdims=True)
    normed = centred * lax.rsqrt(variance + LN_EPS)
    h_attn[...] = (normed * ln_ref[0:1, :] + ln_ref[1:2, :]).astype(BF16)
    h_mlp[...] = (normed * ln_ref[2:3, :] + ln_ref[3:4, :]).astype(BF16)


def roped(first, second, cos, sin):
    return jnp.concatenate([first * cos - second * sin, second * cos + first * sin], axis=1).astype(BF16)


def causal_softmax(scores, allowed):
    masked = jnp.where(allowed, scores, -1e30)
    weight = jnp.exp(masked - jnp.max(masked, axis=1, keepdims=True))
    return (weight * (1.0 / jnp.sum(weight, axis=1, keepdims=True))).astype(BF16)


def gelu_of_half(half_x):
    return (half_x * (1.0 + lax.erf(half_x * np.float32(2.0 ** 0.5)))).astype(BF16)


def add_layer(heads, shards, h_attn, h_mlp, acc, w_qkv, w_up, w_out, rope, masks, mixed, before_last_out=None):
    seq_len, d_model = acc.shape
    width = w_qkv.shape[2] // 3
    half = width // 2
    cols = d_model // heads
    hidden = w_up.shape[2] // heads
    allowed = lax.broadcasted_iota(jnp.int32, (seq_len, seq_len), 0) >= lax.broadcasted_iota(jnp.int32, (seq_len, seq_len), 1)
    raw, ups, score_pairs, probs = {}, {}, {}, {}

    def project(turn, which):
        if turn < len(shards):
            raw[which] = dot(h_attn[...], w_qkv[shards[turn], :, which * width:(which + 1) * width])

    def score(pair):
        k_pair = jnp.concatenate([raw[1] * masks[0, h:h + 1, :] for h in (2 * pair, 2 * pair + 1)], axis=0)
        score_pairs[pair] = lax.dot_general(raw[0], k_pair, (((1,), (1,)), ((), ())), preferred_element_type=F32)

    def soften(head):
        side = head % 2 * seq_len
        probs[head] = causal_softmax(score_pairs[head // 2][:, side:side + seq_len], allowed)

    def context(turn):
        v_heads = jnp.concatenate([v * masks[1, h:h + 1, :] for h in range(heads)], axis=0)
        mixed[turn % 2, :, :width] = dot(jnp.concatenate([probs[h] for h in range(heads)], axis=1), v_heads).astype(BF16)

    def up(turn, part):
        ups[part] = dot(h_mlp[...], w_up[shards[turn], :, part * hidden:(part + 1) * hidden])

    def gelu(turn, part):
        mixed[turn % 2, :, width + part * hidden:width + (part + 1) * hidden] = gelu_of_half(ups[part])

    def add_out(turn, part):
        piece = slice(part * cols, (part + 1) * cols)
        acc[:, piece] += dot(mixed[turn % 2], w_out[shards[turn], :, piece])

    for which in range(3):
        project(0, which)
    for turn in range(len(shards)):
        raw[0] = roped(raw[0][:, :half], raw[0][:, half:], rope[0], rope[1])
        raw[1] = roped(raw[1][:, :half], raw[1][:, half:], rope[2], rope[3])
        v = raw[2].astype(BF16)
        score(0)
        if turn == 0:
            score(1)
            for head in range(heads):
                up(turn, head)
                if head > 0:
                    gelu(turn, head - 1)
                soften(head)
            project(turn + 1, 0)
            project(turn + 1, 1)
            gelu(turn, 3)
            context(turn)
            project(turn + 1, 2)
        else:
            add_out(turn - 1, 0)
            score(1)
            for head in range(heads):
                soften(head)
                if head < 3:
                    add_out(turn - 1, head + 1)
            up(turn, 0)
            up(turn, 1)
            gelu(turn, 0)
            context(turn)
            up(turn, 2)
            gelu(turn, 1)
            up(turn, 3)
            gelu(turn, 2)
            project(turn + 1, 0)
            gelu(turn, 3)
            project(turn + 1, 1)
            project(turn + 1, 2)
    if before_last_out is not None:
        before_last_out()
    for part in range(heads):
        add_out(len(shards) - 1, part)


def kernel(tp_size, pp_size, heads, x_hbm, ln_ref, wq_hbm, wk_hbm, wv_hbm, wo_hbm, wup_hbm, wdown_hbm, rope, masks, out,
           w_qkv, w_up, w_out, raw, detour, xs, ys, ln_half, h_attn, h_mlp, acc, mixed,
           load_sem, w_send, near_recv, far_recv, d_send, d_in, d_out, x_send, x_recv, x_local, x_hand, pp_send, pp_recv, o_send, o_recv):
    me = lax.axis_index("tp")
    stage = lax.axis_index("pp")
    right, left = lax.rem(me + 1, tp_size), lax.rem(me + tp_size - 1, tp_size)
    far = lax.rem(me + 2, tp_size)
    nxt = lax.rem(stage + 1, pp_size)
    last_stage = pp_size - 1
    num_micro, num_seq, seq_len, d_model = xs.shape
    tokens = seq_len // tp_size
    width = raw.shape[1]

    barrier = pltpu.get_barrier_semaphore()

    def knock(index, _):
        peer = {"tp": index // pp_size, "pp": lax.rem(index, pp_size)}
        pl.semaphore_signal(barrier, inc=1, device_id=peer, device_id_type=MESH)
        return 0
    lax.fori_loop(0, tp_size * pp_size, knock, 0)

    loads = [
        pltpu.make_async_copy(wup_hbm, w_up.at[me], load_sem.at[0]),
        pltpu.make_async_copy(wq_hbm, raw.at[0], load_sem.at[1]),
        pltpu.make_async_copy(wk_hbm, raw.at[1], load_sem.at[2]),
        pltpu.make_async_copy(wv_hbm, raw.at[2], load_sem.at[3]),
        pltpu.make_async_copy(wo_hbm, w_out.at[me, pl.ds(0, width)], load_sem.at[4]),
        pltpu.make_async_copy(wdown_hbm, w_out.at[me, pl.ds(width, wdown_hbm.shape[0])], load_sem.at[5]),
    ]
    for load in loads:
        load.start()
    ln_half[...] = ln_ref[...]
    ln_half[2:4, :] = 0.5 * ln_ref[2:4, :]
    pl.semaphore_wait(barrier, tp_size * pp_size)

    def token_rows(owner):
        return pl.ds(pl.multiple_of(owner * tokens, tokens), tokens)

    def seq_rows(owner):
        return pl.ds(owner * num_seq, num_seq)

    early = (stage == last_stage, 0, EARLY_MICRO)
    late = (stage == last_stage - 4, EARLY_MICRO, num_micro - EARLY_MICRO)

    def collect(group):
        micros = pl.ds(group[1], group[2])
        pltpu.make_async_copy(x_hbm.at[micros, seq_rows(me)], ys.at[micros, :, token_rows(me), :], x_local).start()
        for step in range(1, tp_size):
            peer = lax.rem(me + step, tp_size)
            pltpu.make_async_remote_copy(
                src_ref=x_hbm.at[micros, seq_rows(peer)], dst_ref=ys.at[micros, :, token_rows(me), :],
                send_sem=x_send, recv_sem=x_recv, device_id={"tp": peer}, device_id_type=MESH).start()

    def take_blocks(sem, blocks):
        seqs = blocks * num_seq // tp_size
        take(sem, ys.at[pl.ds(0, seqs // num_seq)] if seqs % num_seq == 0 else ys.at[pl.ds(0, seqs), 0])

    def hand_on(group):
        take_blocks(x_local, group[2])
        take_blocks(x_recv, group[2] * (tp_size - 1))

        def one(index, _):
            micro = group[1] + index
            for seq in range(num_seq):
                pltpu.make_async_remote_copy(
                    src_ref=ys.at[micro, seq], dst_ref=xs.at[micro, seq], send_sem=x_hand,
                    recv_sem=pp_recv.at[micro, seq], device_id={"pp": 0}, device_id_type=MESH).start()
            return 0
        lax.fori_loop(0, group[2], one, 0)

    def handed(group):
        take_blocks(x_hand, group[2] * tp_size)
        take_blocks(x_send, group[2] * (tp_size - 1))

    def pp_copy(micro, seq):
        return pltpu.make_async_remote_copy(
            src_ref=ys.at[micro, seq], dst_ref=xs.at[micro, seq], send_sem=pp_send,
            recv_sem=pp_recv.at[micro, seq], device_id={"pp": nxt}, device_id_type=MESH)

    @pl.when(early[0])
    def _():
        collect(early)

    parts = [(w_up, 0, w_up.shape[1], (0, 0)), (w_qkv, 0, w_qkv.shape[1], (0, 0))]
    detour_parts = []
    start = 0
    for rows, first, count, later in DETOURS:
        detour_parts.append((len(detour_parts), pl.ds(start, rows), first, first + count, later))
        parts.append((w_out, start, rows, (first, first + count)))
        start += rows
    parts.append((w_out, start, w_out.shape[1] - start, (0, 0)))
    chunks = [(ref, start + side * rows // 2, rows // 2) for ref, start, rows, _ in parts for side in range(2)]

    def on_ring(part, action):
        first, end = parts[part][3]
        if end > first:
            pl.when((stage < first) | (stage >= end))(action)
        else:
            action()

    def shard_copy(index, owner, send_sem, recv_sem, peer):
        ref, start, rows = chunks[index]
        piece = ref.at[owner, pl.ds(start, rows)]
        return pltpu.make_async_remote_copy(
            src_ref=piece, dst_ref=piece, send_sem=send_sem, recv_sem=recv_sem, device_id={"tp": peer}, device_id_type=MESH)

    def own_copy(index, way):
        return shard_copy(index, me, w_send, near_recv.at[way, index], right if way == 0 else left)

    def near_copy(index, way):
        return shard_copy(index, left if way == 0 else right, w_send, near_recv.at[way, index],
                          right if way == 0 else left)

    def fwd_copy(index):
        way = index % 2
        return shard_copy(index, left if way == 0 else right, w_send, far_recv.at[index // 2],
                          right if way == 0 else left)

    def take(sem, *refs):
        for ref in refs:
            pltpu.make_async_copy(ref, ref, sem).wait()

    def send_own(part):
        def send():
            for way in range(2):
                own_copy(2 * part + way, way).start()
            for way in range(2):
                own_copy(2 * part + 1 - way, way).start()
        on_ring(part, send)

    def pass_on(part):
        def forward():
            for way in range(2):
                near_copy(2 * part + way, way).wait_recv()
                fwd_copy(2 * part + way).start()
        on_ring(part, forward)

    def take_near(part):
        def wait():
            for way in range(2):
                near_copy(2 * part + 1 - way, way).wait_recv()
        on_ring(part, wait)

    def take_far(part):
        ref, start, rows, _ = parts[part]
        on_ring(part, lambda: take(far_recv.at[part], ref.at[far, pl.ds(start, rows)]))

    def send_detours():
        for part, piece, first, end, later in detour_parts:
            @pl.when((stage >= first) & (stage < end))
            def _():
                for step in range(1, tp_size):
                    pltpu.make_async_remote_copy(
                        src_ref=w_out.at[me, piece], dst_ref=detour.at[step - 1, piece],
                        send_sem=w_send, recv_sem=d_in.at[part],
                        device_id={"tp": lax.rem(me + step, tp_size), "pp": stage + later}, device_id_type=MESH).start()

    def pass_detours():
        for part, piece, first, end, later in detour_parts:
            @pl.when((stage >= first + later) & (stage < end + later))
            def _():
                take(d_in.at[part], detour.at[:, piece])
                for step in range(1, tp_size):
                    pltpu.make_async_remote_copy(
                        src_ref=detour.at[step - 1, piece],
                        dst_ref=w_out.at[lax.rem(me + tp_size - step, tp_size), piece],
                        send_sem=d_send.at[part], recv_sem=d_out.at[part],
                        device_id={"pp": stage - later}, device_id_type=MESH).start()

    def take_detours():
        for part, piece, first, end, _ in detour_parts:
            @pl.when((stage >= first) & (stage < end))
            def _():
                take(d_out.at[part], detour.at[:, piece])

    for load in loads[:1] + loads[4:]:
        load.wait()
    send_detours()
    send_own(0)
    for load in loads[1:4]:
        load.wait()
    head_dim = width // heads
    part = head_dim // 2
    for which in range(3):
        starts = [head * head_dim + side * part for side in range(2) for head in range(heads)]
        if which == 2:
            starts = list(range(0, width, part))
        for col in range(0, d_model, width):
            block = jnp.concatenate([raw[which, start:start + part, col:col + width] for start in starts], axis=0)
            w_qkv[me, col:col + width, which * width:(which + 1) * width] = block.T

    for part in range(1, len(parts)):
        send_own(part)
    pass_detours()

    @pl.when(early[0])
    def _():
        hand_on(early)

    for part in range(len(parts)):
        pass_on(part)
    for part in range(len(parts)):
        take_near(part)
    take_detours()

    @pl.when(early[0])
    def _():
        handed(early)

    @pl.when(late[0])
    def _():
        collect(late)

    def o_copy(micro, seq, step):
        peer = lax.rem(me + step, tp_size)
        return pltpu.make_async_remote_copy(
            src_ref=ys.at[micro, seq, token_rows(peer), :], dst_ref=out.at[micro, me * num_seq + seq],
            send_sem=o_send, recv_sem=o_recv, device_id={"tp": peer}, device_id_type=MESH)

    def hand_over(micro, seq):
        @pl.when(stage < last_stage)
        def _():
            pp_copy(micro, seq).start()

    def put_out(micro, seq):
        out[micro, me * num_seq + seq] = ys[micro, seq, token_rows(me), :]
        for step in range(1, tp_size):
            o_copy(micro, seq, step).start()

    work = (h_attn, h_mlp, acc, w_qkv, w_up, w_out, rope, masks, mixed)

    pp_copy(0, 0).wait_recv()
    layer_norms(xs[0, 0], ln_half, h_attn, h_mlp, acc)
    add_layer(heads, [me, left, right], *work)
    take_far(0)
    take_far(1)

    def rest_of_far():
        for part in range(2, len(parts)):
            take_far(part)
    add_layer(heads, [far], *work, before_last_out=rest_of_far)
    ys[0, 0] = acc[...].astype(BF16)
    hand_over(0, 0)

    def unit(index, _):
        micro, seq = index // num_seq, lax.rem(index, num_seq)
        pp_copy(micro, seq).wait_recv()
        put_out((index - 1) // num_seq, lax.rem(index - 1, num_seq))
        layer_norms(xs[micro, seq], ln_half, h_attn, h_mlp, acc)
        add_layer(heads, list(range(tp_size)), *work)
        ys[micro, seq] = acc[...].astype(BF16)
        hand_over(micro, seq)

        @pl.when(late[0])
        def _():
            pl.when(index == HAND_AT)(lambda: hand_on(late))
            pl.when(index == HANDED_AT)(lambda: handed(late))
        return 0

    lax.fori_loop(1, num_micro * num_seq, unit, 0)
    put_out(num_micro - 1, num_seq - 1)

    take(w_send, w_out, w_up)

    for part, piece, first, end, later in detour_parts:
        @pl.when((stage >= first + later) & (stage < end + later))
        def _():
            take(d_send.at[part], detour.at[:, piece])

    @pl.when(stage < last_stage)
    def _():
        take(pp_send, ys)
    take_blocks(o_send, num_micro * (tp_size - 1))
    take_blocks(o_recv, num_micro * (tp_size - 1))


def solution(mesh):
    tp_size, pp_size = mesh.shape["tp"], mesh.shape["pp"]

    def stage_body(x_in, ln_params, w_q, w_k, w_v, w_o, w_up, w_down):
        num_micro, batch, tokens, d_model = x_in.shape
        heads, head_dim = w_k.shape[2:]
        width = heads * head_dim
        hidden = w_up.shape[2]
        seq_len = tokens * tp_size
        num_seq = batch // tp_size
        rope = jnp.asarray(rope_tables(seq_len, head_dim, heads))
        masks = jnp.asarray(head_masks(head_dim, heads), dtype=BF16)
        wq_t = jnp.transpose(w_q[0], (1, 2, 3, 0)).reshape(width, d_model)
        wk_t = jnp.transpose(w_k[0], (1, 2, 0)).reshape(width, d_model)
        wv_t = jnp.transpose(w_v[0], (1, 2, 0)).reshape(width, d_model)
        vmem = pl.BlockSpec(memory_space=pltpu.VMEM)
        hbm = pl.BlockSpec(memory_space=pl.ANY)
        dma = pltpu.SemaphoreType.DMA
        out = pl.pallas_call(
            functools.partial(kernel, tp_size, pp_size, heads),
            out_shape=pltpu.VMEM(x_in.shape, BF16),
            in_specs=[hbm, vmem, hbm, hbm, hbm, hbm, hbm, hbm, vmem, vmem],
            out_specs=vmem,
            scratch_shapes=[
                pltpu.VMEM((tp_size, d_model, 3 * width), BF16),
                pltpu.VMEM((tp_size, d_model, hidden), BF16),
                pltpu.VMEM((tp_size, width + hidden, d_model), BF16),
                pltpu.VMEM((3, width, d_model), BF16),
                pltpu.VMEM((tp_size - 1, sum(rows for rows, *_ in DETOURS), d_model), BF16),
                pltpu.VMEM((num_micro, num_seq, seq_len, d_model), BF16),
                pltpu.VMEM((num_micro, num_seq, seq_len, d_model), BF16),
                pltpu.VMEM((4, d_model), F32),
                pltpu.VMEM((seq_len, d_model), BF16),
                pltpu.VMEM((seq_len, d_model), BF16),
                pltpu.VMEM((seq_len, d_model), F32),
                pltpu.VMEM((2, seq_len, width + hidden), BF16),
                dma((6,)), dma, dma((2, 12)), dma((6,)), dma((3,)), dma((3,)), dma((3,)), dma, dma, dma, dma, dma, dma((num_micro, num_seq)), dma, dma,
            ],
            compiler_params=pltpu.CompilerParams(
                collective_id=0, has_side_effects=True, vmem_limit_bytes=54 * 1024 * 1024),
            name="stage",
        )(x_in, ln_params[0], wq_t, wk_t, wv_t, w_o[0].reshape(width, d_model), w_up[0], w_down[0], rope, masks)
        return out[None]

    in_specs = (P(None, "dp", "tp", None), P("pp", None, None), P("pp", None, "tp", None, None), P("pp", None, "tp", None), P("pp", None, "tp", None), P("pp", "tp", None, None, None), P("pp", None, "tp"), P("pp", "tp", None))
    return jax.shard_map(stage_body, mesh=mesh, in_specs=in_specs, out_specs=P("pp", None, "dp", "tp", None), check_vma=False)
```

```python
import functools

import jax
import jax.numpy as jnp
import numpy as np
from jax import lax
from jax.experimental import pallas as pl
from jax.experimental.pallas import tpu as pltpu
from jax.sharding import PartitionSpec as P

LN_EPS = 1e-5
ROPE_BASE = 10000.0
F32, BF16 = jnp.float32, jnp.bfloat16
MESH = pl.DeviceIdType.MESH
DETOURS = ((128, 0, 2, 4), (160, 0, 1, 6), (64, 2, 1, 2))
EARLY_MICRO = 10
HAND_AT, HANDED_AT = 9, 18


def rope_tables(seq_len, head_dim, heads):
    half = head_dim // 2
    inv_freq = (ROPE_BASE ** (-2.0 * np.arange(half) / head_dim)).astype(np.float32)
    angles = np.arange(seq_len, dtype=np.float32)[:, None] * inv_freq[None, :]
    cos = np.tile(np.cos(angles.astype(np.float64)), (1, heads)).astype(np.float32)
    sin = np.tile(np.sin(angles.astype(np.float64)), (1, heads)).astype(np.float32)
    scale = np.float32(head_dim ** -0.5)
    return np.stack([cos * scale, sin * scale, cos, sin])


def head_masks(head_dim, heads):
    half = head_dim // 2
    lanes = np.arange(heads * head_dim)
    roped = np.stack([(lanes % (heads * half)) // half == head for head in range(heads)])
    plain = np.stack([lanes // head_dim == head for head in range(heads)])
    return np.stack([roped, plain]).astype(np.float32)


def dot(lhs, rhs):
    return jnp.dot(lhs, rhs, preferred_element_type=F32)


def layer_norms(x, ln_ref, h_attn, h_mlp):
    x_f32 = x.astype(F32)
    centred = x_f32 - jnp.mean(x_f32, axis=-1, keepdims=True)
    variance = jnp.mean(centred * centred, axis=-1, keepdims=True)
    normed = centred * lax.rsqrt(variance + LN_EPS)
    h_attn[...] = (normed * ln_ref[0:1, :] + ln_ref[1:2, :]).astype(BF16)
    h_mlp[...] = (normed * ln_ref[2:3, :] + ln_ref[3:4, :]).astype(BF16)


def roped(first, second, cos, sin):
    return jnp.concatenate([first * cos - second * sin, second * cos + first * sin], axis=1).astype(BF16)


def causal_softmax(scores, allowed):
    masked = jnp.where(allowed, scores, -1e30)
    weight = jnp.exp(masked - jnp.max(masked, axis=1, keepdims=True))
    return (weight * (1.0 / jnp.sum(weight, axis=1, keepdims=True))).astype(BF16)


def gelu_of_half(half_x):
    return (half_x * (1.0 + lax.erf(half_x * np.float32(2.0 ** 0.5)))).astype(BF16)


def add_layer(heads, shards, h_attn, h_mlp, acc, w_qkv, w_up, w_out, rope, masks, mixed, x=None, y=None, fresh=True, before_last_out=None):
    seq_len, d_model = acc.shape
    width = w_qkv.shape[2] // 3
    half = width // 2
    cols = d_model // heads
    hidden = w_up.shape[2] // heads
    allowed = lax.broadcasted_iota(jnp.int32, (seq_len, seq_len), 0) >= lax.broadcasted_iota(jnp.int32, (seq_len, seq_len), 1)
    raw, ups, score_pairs, probs = {}, {}, {}, {}

    def project(turn, which):
        if turn < len(shards):
            raw[which] = dot(h_attn[...], w_qkv[shards[turn], :, which * width:(which + 1) * width])

    def score(pair):
        k_pair = jnp.concatenate([raw[1] * masks[0, h:h + 1, :] for h in (2 * pair, 2 * pair + 1)], axis=0)
        score_pairs[pair] = lax.dot_general(raw[0], k_pair, (((1,), (1,)), ((), ())), preferred_element_type=F32)

    def soften(head):
        side = head % 2 * seq_len
        probs[head] = causal_softmax(score_pairs[head // 2][:, side:side + seq_len], allowed)

    def context(turn):
        v_heads = jnp.concatenate([v * masks[1, h:h + 1, :] for h in range(heads)], axis=0)
        mixed[turn % 2, :, :width] = dot(jnp.concatenate([probs[h] for h in range(heads)], axis=1), v_heads).astype(BF16)

    def up(turn, part):
        ups[part] = dot(h_mlp[...], w_up[shards[turn], :, part * hidden:(part + 1) * hidden])

    def gelu(turn, part):
        mixed[turn % 2, :, width + part * hidden:width + (part + 1) * hidden] = gelu_of_half(ups[part])

    def add_out(turn, part):
        piece = slice(part * cols, (part + 1) * cols)
        term = dot(mixed[turn % 2], w_out[shards[turn], :, piece])
        if turn > 0 or not fresh:
            term += acc[:, piece]
        if y is not None and turn == len(shards) - 1:
            y[:, piece] = (term + x[:, piece].astype(F32)).astype(BF16)
        else:
            acc[:, piece] = term

    for which in range(3):
        project(0, which)
    for turn in range(len(shards)):
        raw[0] = roped(raw[0][:, :half], raw[0][:, half:], rope[0], rope[1])
        raw[1] = roped(raw[1][:, :half], raw[1][:, half:], rope[2], rope[3])
        v = raw[2].astype(BF16)
        score(0)
        if turn == 0:
            score(1)
            for head in range(heads):
                up(turn, head)
                if head > 0:
                    gelu(turn, head - 1)
                soften(head)
            project(turn + 1, 0)
            project(turn + 1, 1)
            gelu(turn, 3)
            context(turn)
            project(turn + 1, 2)
        else:
            add_out(turn - 1, 0)
            score(1)
            for head in range(heads):
                soften(head)
                if head < 3:
                    add_out(turn - 1, head + 1)
            up(turn, 0)
            up(turn, 1)
            gelu(turn, 0)
            context(turn)
            up(turn, 2)
            gelu(turn, 1)
            up(turn, 3)
            gelu(turn, 2)
            project(turn + 1, 0)
            gelu(turn, 3)
            project(turn + 1, 1)
            project(turn + 1, 2)
    if before_last_out is not None:
        before_last_out()
    for part in range(heads):
        add_out(len(shards) - 1, part)


def kernel(tp_size, pp_size, heads, x_hbm, ln_hbm, wq_hbm, wk_hbm, wv_hbm, wo_hbm, wup_hbm, wdown_hbm, rope_hbm, masks_hbm, out,
           w_qkv, w_up, w_out, raw, detour, xs, ys, ln_half, rope, masks, h_attn, h_mlp, acc, mixed,
           load_sem, w_send, near_recv, far_recv, d_send, d_in, d_out, x_send, x_recv, x_local, x_hand, pp_send, pp_recv, o_send, o_recv):
    me = lax.axis_index("tp")
    stage = lax.axis_index("pp")
    right, left = lax.rem(me + 1, tp_size), lax.rem(me + tp_size - 1, tp_size)
    far = lax.rem(me + 2, tp_size)
    nxt = lax.rem(stage + 1, pp_size)
    last_stage = pp_size - 1
    num_micro, num_seq, seq_len, d_model = xs.shape
    tokens = seq_len // tp_size
    width = raw.shape[1]

    loads = [
        pltpu.make_async_copy(wup_hbm, w_up.at[me], load_sem.at[0]),
        pltpu.make_async_copy(wq_hbm, raw.at[0], load_sem.at[1]),
        pltpu.make_async_copy(wk_hbm, raw.at[1], load_sem.at[2]),
        pltpu.make_async_copy(wv_hbm, raw.at[2], load_sem.at[3]),
        pltpu.make_async_copy(wo_hbm, w_out.at[me, pl.ds(0, width)], load_sem.at[4]),
        pltpu.make_async_copy(wdown_hbm, w_out.at[me, pl.ds(width, wdown_hbm.shape[0])], load_sem.at[5]),
        pltpu.make_async_copy(ln_hbm, ln_half, load_sem.at[6]),
        pltpu.make_async_copy(rope_hbm, rope, load_sem.at[7]),
        pltpu.make_async_copy(masks_hbm, masks, load_sem.at[8]),
    ]
    for load in loads:
        load.start()

    barrier = pltpu.get_barrier_semaphore()

    def knock(index, _):
        peer = {"tp": index // pp_size, "pp": lax.rem(index, pp_size)}
        pl.semaphore_signal(barrier, inc=1, device_id=peer, device_id_type=MESH)
        return 0
    lax.fori_loop(0, tp_size * pp_size, knock, 0)
    pl.semaphore_wait(barrier, tp_size * pp_size)

    def token_rows(owner):
        return pl.ds(pl.multiple_of(owner * tokens, tokens), tokens)

    def seq_rows(owner):
        return pl.ds(owner * num_seq, num_seq)

    early = (stage == last_stage, 0, EARLY_MICRO)
    late = (stage == last_stage - 4, EARLY_MICRO, num_micro - EARLY_MICRO)

    def collect(group):
        micros = pl.ds(group[1], group[2])
        pltpu.make_async_copy(x_hbm.at[micros, seq_rows(me)], ys.at[micros, :, token_rows(me), :], x_local).start()
        for step in range(1, tp_size):
            peer = lax.rem(me + step, tp_size)
            pltpu.make_async_remote_copy(
                src_ref=x_hbm.at[micros, seq_rows(peer)], dst_ref=ys.at[micros, :, token_rows(me), :],
                send_sem=x_send, recv_sem=x_recv, device_id={"tp": peer}, device_id_type=MESH).start()

    def take_blocks(sem, blocks):
        seqs = blocks * num_seq // tp_size
        take(sem, ys.at[pl.ds(0, seqs // num_seq)] if seqs % num_seq == 0 else ys.at[pl.ds(0, seqs), 0])

    def hand_on(group):
        take_blocks(x_local, group[2])
        take_blocks(x_recv, group[2] * (tp_size - 1))

        def one(index, _):
            micro = group[1] + index
            for seq in range(num_seq):
                pltpu.make_async_remote_copy(
                    src_ref=ys.at[micro, seq], dst_ref=xs.at[micro, seq], send_sem=x_hand,
                    recv_sem=pp_recv.at[micro, seq], device_id={"pp": 0}, device_id_type=MESH).start()
            return 0
        lax.fori_loop(0, group[2], one, 0)

    def handed(group):
        take_blocks(x_hand, group[2] * tp_size)
        take_blocks(x_send, group[2] * (tp_size - 1))

    def pp_copy(micro, seq):
        return pltpu.make_async_remote_copy(
            src_ref=ys.at[micro, seq], dst_ref=xs.at[micro, seq], send_sem=pp_send,
            recv_sem=pp_recv.at[micro, seq], device_id={"pp": nxt}, device_id_type=MESH)

    @pl.when(early[0])
    def _():
        collect(early)

    parts = [(w_up, 0, w_up.shape[1], (0, 0)), (w_qkv, 0, w_qkv.shape[1], (0, 0))]
    detour_parts = []
    start = 0
    for rows, first, count, later in DETOURS:
        detour_parts.append((len(detour_parts), pl.ds(start, rows), first, first + count, later))
        parts.append((w_out, start, rows, (first, first + count)))
        start += rows
    parts.append((w_out, start, w_out.shape[1] - start, (0, 0)))
    chunks = [(ref, start + side * rows // 2, rows // 2) for ref, start, rows, _ in parts for side in range(2)]

    def on_ring(part, action):
        first, end = parts[part][3]
        if end > first:
            pl.when((stage < first) | (stage >= end))(action)
        else:
            action()

    def shard_copy(index, owner, send_sem, recv_sem, peer):
        ref, start, rows = chunks[index]
        piece = ref.at[owner, pl.ds(start, rows)]
        return pltpu.make_async_remote_copy(
            src_ref=piece, dst_ref=piece, send_sem=send_sem, recv_sem=recv_sem, device_id={"tp": peer}, device_id_type=MESH)

    def own_copy(index, way):
        return shard_copy(index, me, w_send, near_recv.at[way, index], right if way == 0 else left)

    def near_copy(index, way):
        return shard_copy(index, left if way == 0 else right, w_send, near_recv.at[way, index],
                          right if way == 0 else left)

    def fwd_copy(index):
        way = index % 2
        return shard_copy(index, left if way == 0 else right, w_send, far_recv.at[index // 2],
                          right if way == 0 else left)

    def take(sem, *refs):
        for ref in refs:
            pltpu.make_async_copy(ref, ref, sem).wait()

    def send_own(part):
        def send():
            for way in range(2):
                own_copy(2 * part + way, way).start()
            for way in range(2):
                own_copy(2 * part + 1 - way, way).start()
        on_ring(part, send)

    def pass_on(part):
        def forward():
            for way in range(2):
                near_copy(2 * part + way, way).wait_recv()
                fwd_copy(2 * part + way).start()
        on_ring(part, forward)

    def take_near(part):
        def wait():
            for way in range(2):
                near_copy(2 * part + 1 - way, way).wait_recv()
        on_ring(part, wait)

    def take_far(part):
        ref, start, rows, _ = parts[part]
        on_ring(part, lambda: take(far_recv.at[part], ref.at[far, pl.ds(start, rows)]))

    def send_detours():
        for part, piece, first, end, later in detour_parts:
            @pl.when((stage >= first) & (stage < end))
            def _():
                for step in range(1, tp_size):
                    pltpu.make_async_remote_copy(
                        src_ref=w_out.at[me, piece], dst_ref=detour.at[step - 1, piece],
                        send_sem=w_send, recv_sem=d_in.at[part],
                        device_id={"tp": lax.rem(me + step, tp_size), "pp": stage + later}, device_id_type=MESH).start()

    def pass_detours():
        for part, piece, first, end, later in detour_parts:
            @pl.when((stage >= first + later) & (stage < end + later))
            def _():
                take(d_in.at[part], detour.at[:, piece])
                for step in range(1, tp_size):
                    pltpu.make_async_remote_copy(
                        src_ref=detour.at[step - 1, piece],
                        dst_ref=w_out.at[lax.rem(me + tp_size - step, tp_size), piece],
                        send_sem=d_send.at[part], recv_sem=d_out.at[part],
                        device_id={"pp": stage - later}, device_id_type=MESH).start()

    def take_detours():
        for part, piece, first, end, _ in detour_parts:
            @pl.when((stage >= first) & (stage < end))
            def _():
                take(d_out.at[part], detour.at[:, piece])

    loads[0].wait()
    send_own(0)
    for load in loads[4:6]:
        load.wait()
    send_detours()
    for load in loads[1:4]:
        load.wait()
    head_dim = width // heads
    part = head_dim // 2
    for which in range(3):
        starts = [head * head_dim + side * part for side in range(2) for head in range(heads)]
        if which == 2:
            starts = list(range(0, width, part))
        for col in range(0, d_model, width):
            block = jnp.concatenate([raw[which, start:start + part, col:col + width] for start in starts], axis=0)
            w_qkv[me, col:col + width, which * width:(which + 1) * width] = block.T

    for part in range(1, len(parts)):
        send_own(part)
    for load in loads[6:]:
        load.wait()
    ln_half[2:4, :] = 0.5 * ln_half[2:4, :]
    pass_detours()

    @pl.when(early[0])
    def _():
        hand_on(early)

    for part in range(len(parts)):
        pass_on(part)
    for part in range(len(parts)):
        take_near(part)
    take_detours()

    @pl.when(early[0])
    def _():
        handed(early)

    @pl.when(late[0])
    def _():
        collect(late)

    def o_copy(micro, seq, step):
        peer = lax.rem(me + step, tp_size)
        return pltpu.make_async_remote_copy(
            src_ref=ys.at[micro, seq, token_rows(peer), :], dst_ref=out.at[micro, me * num_seq + seq],
            send_sem=o_send, recv_sem=o_recv, device_id={"tp": peer}, device_id_type=MESH)

    def hand_over(micro, seq):
        @pl.when(stage < last_stage)
        def _():
            pp_copy(micro, seq).start()

    def put_out(micro, seq):
        out[micro, me * num_seq + seq] = ys[micro, seq, token_rows(me), :]
        for step in range(1, tp_size):
            o_copy(micro, seq, step).start()

    work = (h_attn, h_mlp, acc, w_qkv, w_up, w_out, rope, masks, mixed)

    pp_copy(0, 0).wait_recv()
    layer_norms(xs[0, 0], ln_half, h_attn, h_mlp)
    add_layer(heads, [me, left, right], *work)
    take_far(0)
    take_far(1)

    def rest_of_far():
        for part in range(2, len(parts)):
            take_far(part)
    add_layer(heads, [far], *work, xs.at[0, 0], ys.at[0, 0], fresh=False, before_last_out=rest_of_far)
    hand_over(0, 0)

    def unit(index, _):
        micro, seq = index // num_seq, lax.rem(index, num_seq)
        pp_copy(micro, seq).wait_recv()
        put_out((index - 1) // num_seq, lax.rem(index - 1, num_seq))
        layer_norms(xs[micro, seq], ln_half, h_attn, h_mlp)
        add_layer(heads, list(range(tp_size)), *work, xs.at[micro, seq], ys.at[micro, seq])
        hand_over(micro, seq)

        @pl.when(late[0])
        def _():
            pl.when(index == HAND_AT)(lambda: hand_on(late))
            pl.when(index == HANDED_AT)(lambda: handed(late))
        return 0

    lax.fori_loop(1, num_micro * num_seq, unit, 0)
    put_out(num_micro - 1, num_seq - 1)

    take(w_send, w_out, w_up)

    for part, piece, first, end, later in detour_parts:
        @pl.when((stage >= first + later) & (stage < end + later))
        def _():
            take(d_send.at[part], detour.at[:, piece])

    @pl.when(stage < last_stage)
    def _():
        take(pp_send, ys)
    take_blocks(o_send, num_micro * (tp_size - 1))
    take_blocks(o_recv, num_micro * (tp_size - 1))


def solution(mesh):
    tp_size, pp_size = mesh.shape["tp"], mesh.shape["pp"]

    def stage_body(x_in, ln_params, w_q, w_k, w_v, w_o, w_up, w_down):
        num_micro, batch, tokens, d_model = x_in.shape
        heads, head_dim = w_k.shape[2:]
        width = heads * head_dim
        hidden = w_up.shape[2]
        seq_len = tokens * tp_size
        num_seq = batch // tp_size
        rope = jnp.asarray(rope_tables(seq_len, head_dim, heads))
        masks = jnp.asarray(head_masks(head_dim, heads), dtype=BF16)
        wq_t = jnp.transpose(w_q[0], (1, 2, 3, 0)).reshape(width, d_model)
        wk_t = jnp.transpose(w_k[0], (1, 2, 0)).reshape(width, d_model)
        wv_t = jnp.transpose(w_v[0], (1, 2, 0)).reshape(width, d_model)
        vmem = pl.BlockSpec(memory_space=pltpu.VMEM)
        hbm = pl.BlockSpec(memory_space=pl.ANY)
        dma = pltpu.SemaphoreType.DMA
        out = pl.pallas_call(
            functools.partial(kernel, tp_size, pp_size, heads),
            out_shape=pltpu.VMEM(x_in.shape, BF16),
            in_specs=[hbm] * 10,
            out_specs=vmem,
            scratch_shapes=[
                pltpu.VMEM((tp_size, d_model, 3 * width), BF16),
                pltpu.VMEM((tp_size, d_model, hidden), BF16),
                pltpu.VMEM((tp_size, width + hidden, d_model), BF16),
                pltpu.VMEM((3, width, d_model), BF16),
                pltpu.VMEM((tp_size - 1, sum(rows for rows, *_ in DETOURS), d_model), BF16),
                pltpu.VMEM((num_micro, num_seq, seq_len, d_model), BF16),
                pltpu.VMEM((num_micro, num_seq, seq_len, d_model), BF16),
                pltpu.VMEM((4, d_model), F32),
                pltpu.VMEM(rope.shape, F32),
                pltpu.VMEM(masks.shape, BF16),
                pltpu.VMEM((seq_len, d_model), BF16),
                pltpu.VMEM((seq_len, d_model), BF16),
                pltpu.VMEM((seq_len, d_model), F32),
                pltpu.VMEM((2, seq_len, width + hidden), BF16),
                dma((9,)), dma, dma((2, 12)), dma((6,)), dma((3,)), dma((3,)), dma((3,)), dma, dma, dma, dma, dma, dma((num_micro, num_seq)), dma, dma,
            ],
            compiler_params=pltpu.CompilerParams(
                collective_id=0, has_side_effects=True, vmem_limit_bytes=54 * 1024 * 1024),
            name="stage",
        )(x_in, ln_params[0], wq_t, wk_t, wv_t, w_o[0].reshape(width, d_model), w_up[0], w_down[0], rope, masks)
        return out[None]

    in_specs = (P(None, "dp", "tp", None), P("pp", None, None), P("pp", None, "tp", None, None), P("pp", None, "tp", None), P("pp", None, "tp", None), P("pp", "tp", None, None, None), P("pp", None, "tp"), P("pp", "tp", None))
    return jax.shard_map(stage_body, mesh=mesh, in_specs=in_specs, out_specs=P("pp", None, "dp", "tp", None), check_vma=False)
```

```python
import functools

import jax
import jax.numpy as jnp
import numpy as np
from jax import lax
from jax.experimental import pallas as pl
from jax.experimental.pallas import tpu as pltpu
from jax.sharding import PartitionSpec as P

LN_EPS = 1e-5
ROPE_BASE = 10000.0
F32, BF16 = jnp.float32, jnp.bfloat16
MESH = pl.DeviceIdType.MESH
DETOURS = ((128, 0, 2, 4), (160, 0, 1, 6), (64, 2, 1, 2))
EARLY_MICRO = 8
HAND_AT, HANDED_AT = 8, 14


def rope_tables(seq_len, head_dim, heads):
    half = head_dim // 2
    inv_freq = (ROPE_BASE ** (-2.0 * np.arange(half) / head_dim)).astype(np.float32)
    angles = np.arange(seq_len, dtype=np.float32)[:, None] * inv_freq[None, :]
    cos = np.tile(np.cos(angles.astype(np.float64)), (1, heads)).astype(np.float32)
    sin = np.tile(np.sin(angles.astype(np.float64)), (1, heads)).astype(np.float32)
    scale = np.float32(head_dim ** -0.5)
    return np.stack([cos * scale, sin * scale, cos, sin])


def head_masks(head_dim, heads):
    half = head_dim // 2
    lanes = np.arange(heads * head_dim)
    roped = np.stack([(lanes % (heads * half)) // half == head for head in range(heads)])
    plain = np.stack([lanes // head_dim == head for head in range(heads)])
    return np.stack([roped, plain]).astype(np.float32)


def dot(lhs, rhs):
    return jnp.dot(lhs, rhs, preferred_element_type=F32)


def layer_norms(x, ln_ref, h_attn, h_mlp):
    x_f32 = x.astype(F32)
    centred = x_f32 - jnp.mean(x_f32, axis=-1, keepdims=True)
    variance = jnp.mean(centred * centred, axis=-1, keepdims=True)
    normed = centred * lax.rsqrt(variance + LN_EPS)
    h_attn[...] = (normed * ln_ref[0:1, :] + ln_ref[1:2, :]).astype(BF16)
    h_mlp[...] = (normed * ln_ref[2:3, :] + ln_ref[3:4, :]).astype(BF16)


def roped(first, second, cos, sin):
    return jnp.concatenate([first * cos - second * sin, second * cos + first * sin], axis=1).astype(BF16)


def causal_softmax(scores, allowed):
    masked = jnp.where(allowed, scores, -1e30)
    weight = jnp.exp(masked - jnp.max(masked, axis=1, keepdims=True))
    return (weight * (1.0 / jnp.sum(weight, axis=1, keepdims=True))).astype(BF16)


def gelu_of_half(half_x):
    return (half_x * (1.0 + lax.erf(half_x * np.float32(2.0 ** 0.5)))).astype(BF16)


def add_layer(heads, shards, h_attn, h_mlp, acc, w_qkv, w_up, w_out, rope, masks, mixed, x=None, y=None, fresh=True, before_last_out=None):
    seq_len, d_model = acc.shape
    width = w_qkv.shape[2] // 3
    half = width // 2
    cols = d_model // heads
    hidden = w_up.shape[2] // heads
    allowed = lax.broadcasted_iota(jnp.int32, (seq_len, seq_len), 0) >= lax.broadcasted_iota(jnp.int32, (seq_len, seq_len), 1)
    raw, ups, score_pairs, probs = {}, {}, {}, {}

    def project(turn, which):
        if turn < len(shards):
            raw[which] = dot(h_attn[...], w_qkv[shards[turn], :, which * width:(which + 1) * width])

    def score(pair):
        k_pair = jnp.concatenate([raw[1] * masks[0, h:h + 1, :] for h in (2 * pair, 2 * pair + 1)], axis=0)
        score_pairs[pair] = lax.dot_general(raw[0], k_pair, (((1,), (1,)), ((), ())), preferred_element_type=F32)

    def soften(head):
        side = head % 2 * seq_len
        probs[head] = causal_softmax(score_pairs[head // 2][:, side:side + seq_len], allowed)

    def context(turn):
        v_heads = jnp.concatenate([v * masks[1, h:h + 1, :] for h in range(heads)], axis=0)
        mixed[turn % 2, :, :width] = dot(jnp.concatenate([probs[h] for h in range(heads)], axis=1), v_heads).astype(BF16)

    def up(turn, part):
        ups[part] = dot(h_mlp[...], w_up[shards[turn], :, part * hidden:(part + 1) * hidden])

    def gelu(turn, part):
        mixed[turn % 2, :, width + part * hidden:width + (part + 1) * hidden] = gelu_of_half(ups[part])

    def add_out(turn, part):
        piece = slice(part * cols, (part + 1) * cols)
        term = dot(mixed[turn % 2], w_out[shards[turn], :, piece])
        if turn > 0 or not fresh:
            term += acc[:, piece]
        if y is not None and turn == len(shards) - 1:
            y[:, piece] = (term + x[:, piece].astype(F32)).astype(BF16)
        else:
            acc[:, piece] = term

    for which in range(3):
        project(0, which)
    for turn in range(len(shards)):
        raw[0] = roped(raw[0][:, :half], raw[0][:, half:], rope[0], rope[1])
        raw[1] = roped(raw[1][:, :half], raw[1][:, half:], rope[2], rope[3])
        v = raw[2].astype(BF16)
        score(0)
        if turn == 0:
            score(1)
            for head in range(heads):
                up(turn, head)
                if head > 0:
                    gelu(turn, head - 1)
                soften(head)
            project(turn + 1, 0)
            project(turn + 1, 1)
            gelu(turn, 3)
            context(turn)
            project(turn + 1, 2)
        else:
            add_out(turn - 1, 0)
            score(1)
            for head in range(heads):
                soften(head)
                if head < 3:
                    add_out(turn - 1, head + 1)
            up(turn, 0)
            up(turn, 1)
            gelu(turn, 0)
            context(turn)
            up(turn, 2)
            gelu(turn, 1)
            up(turn, 3)
            gelu(turn, 2)
            project(turn + 1, 0)
            gelu(turn, 3)
            project(turn + 1, 1)
            project(turn + 1, 2)
    if before_last_out is not None:
        before_last_out()
    for part in range(heads):
        add_out(len(shards) - 1, part)


def kernel(tp_size, pp_size, heads, x_hbm, ln_hbm, wq_hbm, wk_hbm, wv_hbm, wo_hbm, wup_hbm, wdown_hbm, rope_hbm, masks_hbm, out,
           w_qkv, w_up, w_out, raw, detour, xs, ys, ln_half, rope, masks, h_attn, h_mlp, acc, mixed,
           load_sem, w_send, near_recv, far_recv, d_send, d_in, d_out, x_send, x_recv, x_local, x_hand, pp_send, pp_recv, o_send, o_recv):
    me = lax.axis_index("tp")
    stage = lax.axis_index("pp")
    right, left = lax.rem(me + 1, tp_size), lax.rem(me + tp_size - 1, tp_size)
    far = lax.rem(me + 2, tp_size)
    nxt = lax.rem(stage + 1, pp_size)
    last_stage = pp_size - 1
    num_micro, num_seq, seq_len, d_model = xs.shape
    tokens = seq_len // tp_size
    width = raw.shape[1]

    loads = [
        pltpu.make_async_copy(wup_hbm, w_up.at[me], load_sem.at[0]),
        pltpu.make_async_copy(wq_hbm, raw.at[0], load_sem.at[1]),
        pltpu.make_async_copy(wk_hbm, raw.at[1], load_sem.at[2]),
        pltpu.make_async_copy(wv_hbm, raw.at[2], load_sem.at[3]),
        pltpu.make_async_copy(wo_hbm, w_out.at[me, pl.ds(0, width)], load_sem.at[4]),
        pltpu.make_async_copy(wdown_hbm, w_out.at[me, pl.ds(width, wdown_hbm.shape[0])], load_sem.at[5]),
        pltpu.make_async_copy(ln_hbm, ln_half, load_sem.at[6]),
        pltpu.make_async_copy(rope_hbm, rope, load_sem.at[7]),
        pltpu.make_async_copy(masks_hbm, masks, load_sem.at[8]),
    ]
    for load in loads:
        load.start()

    barrier = pltpu.get_barrier_semaphore()

    def knock(index, _):
        peer = {"tp": index // pp_size, "pp": lax.rem(index, pp_size)}
        pl.semaphore_signal(barrier, inc=1, device_id=peer, device_id_type=MESH)
        return 0
    lax.fori_loop(0, tp_size * pp_size, knock, 0)
    pl.semaphore_wait(barrier, tp_size * pp_size)

    def token_rows(owner):
        return pl.ds(pl.multiple_of(owner * tokens, tokens), tokens)

    def seq_rows(owner):
        return pl.ds(owner * num_seq, num_seq)

    early = (stage == last_stage, 0, EARLY_MICRO)
    late = (stage == last_stage - 4, EARLY_MICRO, num_micro - EARLY_MICRO)

    def collect(group):
        micros = pl.ds(group[1], group[2])
        pltpu.make_async_copy(x_hbm.at[micros, seq_rows(me)], ys.at[micros, :, token_rows(me), :], x_local).start()
        for step in range(1, tp_size):
            peer = lax.rem(me + step, tp_size)
            pltpu.make_async_remote_copy(
                src_ref=x_hbm.at[micros, seq_rows(peer)], dst_ref=ys.at[micros, :, token_rows(me), :],
                send_sem=x_send, recv_sem=x_recv, device_id={"tp": peer}, device_id_type=MESH).start()

    def take_blocks(sem, blocks):
        seqs = blocks * num_seq // tp_size
        take(sem, ys.at[pl.ds(0, seqs // num_seq)] if seqs % num_seq == 0 else ys.at[pl.ds(0, seqs), 0])

    def hand_on(group):
        take_blocks(x_local, group[2])
        take_blocks(x_recv, group[2] * (tp_size - 1))

        def one(index, _):
            micro = group[1] + index
            for seq in range(num_seq):
                pltpu.make_async_remote_copy(
                    src_ref=ys.at[micro, seq], dst_ref=xs.at[micro, seq], send_sem=x_hand,
                    recv_sem=pp_recv.at[micro, seq], device_id={"pp": 0}, device_id_type=MESH).start()
            return 0
        lax.fori_loop(0, group[2], one, 0)

    def handed(group):
        take_blocks(x_hand, group[2] * tp_size)
        take_blocks(x_send, group[2] * (tp_size - 1))

    def pp_copy(micro, seq):
        return pltpu.make_async_remote_copy(
            src_ref=ys.at[micro, seq], dst_ref=xs.at[micro, seq], send_sem=pp_send,
            recv_sem=pp_recv.at[micro, seq], device_id={"pp": nxt}, device_id_type=MESH)

    @pl.when(early[0])
    def _():
        collect(early)

    parts = [(w_up, 0, w_up.shape[1], (0, 0)), (w_qkv, 0, w_qkv.shape[1], (0, 0))]
    detour_parts = []
    start = 0
    for rows, first, count, later in DETOURS:
        detour_parts.append((len(detour_parts), pl.ds(start, rows), first, first + count, later))
        parts.append((w_out, start, rows, (first, first + count)))
        start += rows
    parts.append((w_out, start, w_out.shape[1] - start, (0, 0)))
    chunks = [(ref, start + side * rows // 2, rows // 2) for ref, start, rows, _ in parts for side in range(2)]

    def on_ring(part, action):
        first, end = parts[part][3]
        if end > first:
            pl.when((stage < first) | (stage >= end))(action)
        else:
            action()

    def shard_copy(index, owner, send_sem, recv_sem, peer):
        ref, start, rows = chunks[index]
        piece = ref.at[owner, pl.ds(start, rows)]
        return pltpu.make_async_remote_copy(
            src_ref=piece, dst_ref=piece, send_sem=send_sem, recv_sem=recv_sem, device_id={"tp": peer}, device_id_type=MESH)

    def own_copy(index, way):
        return shard_copy(index, me, w_send, near_recv.at[way, index], right if way == 0 else left)

    def near_copy(index, way):
        return shard_copy(index, left if way == 0 else right, w_send, near_recv.at[way, index],
                          right if way == 0 else left)

    def fwd_copy(index):
        way = index % 2
        return shard_copy(index, left if way == 0 else right, w_send, far_recv.at[index // 2],
                          right if way == 0 else left)

    def take(sem, *refs):
        for ref in refs:
            pltpu.make_async_copy(ref, ref, sem).wait()

    def send_own(part):
        def send():
            for way in range(2):
                own_copy(2 * part + way, way).start()
            for way in range(2):
                own_copy(2 * part + 1 - way, way).start()
        on_ring(part, send)

    def pass_on(part):
        def forward():
            for way in range(2):
                near_copy(2 * part + way, way).wait_recv()
                fwd_copy(2 * part + way).start()
        on_ring(part, forward)

    def take_near(part):
        def wait():
            for way in range(2):
                near_copy(2 * part + 1 - way, way).wait_recv()
        on_ring(part, wait)

    def take_far(part):
        ref, start, rows, _ = parts[part]
        on_ring(part, lambda: take(far_recv.at[part], ref.at[far, pl.ds(start, rows)]))

    def send_detours():
        for part, piece, first, end, later in detour_parts:
            @pl.when((stage >= first) & (stage < end))
            def _():
                for step in range(1, tp_size):
                    pltpu.make_async_remote_copy(
                        src_ref=w_out.at[me, piece], dst_ref=detour.at[step - 1, piece],
                        send_sem=w_send, recv_sem=d_in.at[part],
                        device_id={"tp": lax.rem(me + step, tp_size), "pp": stage + later}, device_id_type=MESH).start()

    def pass_detours():
        for part, piece, first, end, later in detour_parts:
            @pl.when((stage >= first + later) & (stage < end + later))
            def _():
                take(d_in.at[part], detour.at[:, piece])
                for step in range(1, tp_size):
                    pltpu.make_async_remote_copy(
                        src_ref=detour.at[step - 1, piece],
                        dst_ref=w_out.at[lax.rem(me + tp_size - step, tp_size), piece],
                        send_sem=d_send.at[part], recv_sem=d_out.at[part],
                        device_id={"pp": stage - later}, device_id_type=MESH).start()

    def take_detours():
        for part, piece, first, end, _ in detour_parts:
            @pl.when((stage >= first) & (stage < end))
            def _():
                take(d_out.at[part], detour.at[:, piece])

    loads[0].wait()
    send_own(0)
    for load in loads[4:6]:
        load.wait()
    send_detours()
    for load in loads[1:4]:
        load.wait()
    head_dim = width // heads
    part = head_dim // 2
    for which in range(3):
        starts = [head * head_dim + side * part for side in range(2) for head in range(heads)]
        if which == 2:
            starts = list(range(0, width, part))
        for col in range(0, d_model, width):
            block = jnp.concatenate([raw[which, start:start + part, col:col + width] for start in starts], axis=0)
            w_qkv[me, col:col + width, which * width:(which + 1) * width] = block.T

    for part in range(1, len(parts)):
        send_own(part)
    for load in loads[6:]:
        load.wait()
    ln_half[2:4, :] = 0.5 * ln_half[2:4, :]
    pass_detours()

    @pl.when(early[0])
    def _():
        hand_on(early)

    for part in range(len(parts)):
        pass_on(part)
    for part in range(len(parts)):
        take_near(part)
    take_detours()

    @pl.when(early[0])
    def _():
        handed(early)

    @pl.when(late[0])
    def _():
        collect(late)

    def o_copy(micro, seq, step):
        peer = lax.rem(me + step, tp_size)
        return pltpu.make_async_remote_copy(
            src_ref=ys.at[micro, seq, token_rows(peer), :], dst_ref=out.at[micro, me * num_seq + seq],
            send_sem=o_send, recv_sem=o_recv, device_id={"tp": peer}, device_id_type=MESH)

    def hand_over(micro, seq):
        @pl.when(stage < last_stage)
        def _():
            pp_copy(micro, seq).start()

    def put_out(micro, seq):
        out[micro, me * num_seq + seq] = ys[micro, seq, token_rows(me), :]
        for step in range(1, tp_size):
            o_copy(micro, seq, step).start()

    work = (h_attn, h_mlp, acc, w_qkv, w_up, w_out, rope, masks, mixed)

    pp_copy(0, 0).wait_recv()
    layer_norms(xs[0, 0], ln_half, h_attn, h_mlp)
    add_layer(heads, [me, left, right], *work)
    take_far(0)
    take_far(1)

    def rest_of_far():
        for part in range(2, len(parts)):
            take_far(part)
    add_layer(heads, [far], *work, xs.at[0, 0], ys.at[0, 0], fresh=False, before_last_out=rest_of_far)
    hand_over(0, 0)

    def unit(index, _):
        micro, seq = index // num_seq, lax.rem(index, num_seq)
        pp_copy(micro, seq).wait_recv()
        put_out((index - 1) // num_seq, lax.rem(index - 1, num_seq))
        layer_norms(xs[micro, seq], ln_half, h_attn, h_mlp)
        add_layer(heads, list(range(tp_size)), *work, xs.at[micro, seq], ys.at[micro, seq])
        hand_over(micro, seq)

        @pl.when(late[0])
        def _():
            pl.when(index == HAND_AT)(lambda: hand_on(late))
            pl.when(index == HANDED_AT)(lambda: handed(late))
        return 0

    lax.fori_loop(1, num_micro * num_seq, unit, 0)
    put_out(num_micro - 1, num_seq - 1)

    take(w_send, w_out, w_up)

    for part, piece, first, end, later in detour_parts:
        @pl.when((stage >= first + later) & (stage < end + later))
        def _():
            take(d_send.at[part], detour.at[:, piece])

    @pl.when(stage < last_stage)
    def _():
        take(pp_send, ys)
    take_blocks(o_send, num_micro * (tp_size - 1))
    take_blocks(o_recv, num_micro * (tp_size - 1))


def solution(mesh):
    tp_size, pp_size = mesh.shape["tp"], mesh.shape["pp"]

    def stage_body(x_in, ln_params, w_q, w_k, w_v, w_o, w_up, w_down):
        num_micro, batch, tokens, d_model = x_in.shape
        heads, head_dim = w_k.shape[2:]
        width = heads * head_dim
        hidden = w_up.shape[2]
        seq_len = tokens * tp_size
        num_seq = batch // tp_size
        rope = jnp.asarray(rope_tables(seq_len, head_dim, heads))
        masks = jnp.asarray(head_masks(head_dim, heads), dtype=BF16)
        wq_t = jnp.transpose(w_q[0], (1, 2, 3, 0)).reshape(width, d_model)
        wk_t = jnp.transpose(w_k[0], (1, 2, 0)).reshape(width, d_model)
        wv_t = jnp.transpose(w_v[0], (1, 2, 0)).reshape(width, d_model)
        vmem = pl.BlockSpec(memory_space=pltpu.VMEM)
        hbm = pl.BlockSpec(memory_space=pl.ANY)
        dma = pltpu.SemaphoreType.DMA
        out = pl.pallas_call(
            functools.partial(kernel, tp_size, pp_size, heads),
            out_shape=pltpu.VMEM(x_in.shape, BF16),
            in_specs=[hbm] * 10,
            out_specs=vmem,
            scratch_shapes=[
                pltpu.VMEM((tp_size, d_model, 3 * width), BF16),
                pltpu.VMEM((tp_size, d_model, hidden), BF16),
                pltpu.VMEM((tp_size, width + hidden, d_model), BF16),
                pltpu.VMEM((3, width, d_model), BF16),
                pltpu.VMEM((tp_size - 1, sum(rows for rows, *_ in DETOURS), d_model), BF16),
                pltpu.VMEM((num_micro, num_seq, seq_len, d_model), BF16),
                pltpu.VMEM((num_micro, num_seq, seq_len, d_model), BF16),
                pltpu.VMEM((4, d_model), F32),
                pltpu.VMEM(rope.shape, F32),
                pltpu.VMEM(masks.shape, BF16),
                pltpu.VMEM((seq_len, d_model), BF16),
                pltpu.VMEM((seq_len, d_model), BF16),
                pltpu.VMEM((seq_len, d_model), F32),
                pltpu.VMEM((2, seq_len, width + hidden), BF16),
                dma((9,)), dma, dma((2, 12)), dma((6,)), dma((3,)), dma((3,)), dma((3,)), dma, dma, dma, dma, dma, dma((num_micro, num_seq)), dma, dma,
            ],
            compiler_params=pltpu.CompilerParams(
                collective_id=0, has_side_effects=True, vmem_limit_bytes=54 * 1024 * 1024),
            name="stage",
        )(x_in, ln_params[0], wq_t, wk_t, wv_t, w_o[0].reshape(width, d_model), w_up[0], w_down[0], rope, masks)
        return out[None]

    in_specs = (P(None, "dp", "tp", None), P("pp", None, None), P("pp", None, "tp", None, None), P("pp", None, "tp", None), P("pp", None, "tp", None), P("pp", "tp", None, None, None), P("pp", None, "tp"), P("pp", "tp", None))
    return jax.shard_map(stage_body, mesh=mesh, in_specs=in_specs, out_specs=P("pp", None, "dp", "tp", None), check_vma=False)
```

```python
import functools

import jax
import jax.numpy as jnp
import numpy as np
from jax import lax
from jax.experimental import pallas as pl
from jax.experimental.pallas import tpu as pltpu
from jax.sharding import PartitionSpec as P

LN_EPS = 1e-5
ROPE_BASE = 10000.0
F32, BF16 = jnp.float32, jnp.bfloat16
MESH = pl.DeviceIdType.MESH
FIRST = (
    "q", "k", "r", "v", "s0", "s1", "u0", "m0", "g0", "u1", "u2", "m1", "g1", "m2", "u3", "m3", "g2", "K", "g3", "Q",
    "c", "V",
)
LATER = (
    (
        "r", "s0", "o0", "s1", "m0", "o1", "m1", "o2", "m2", "o3", "m3", "u0", "g0", "c", "u1", "u2", "g1", "Q", "u3",
        "g3", "g2", "K", "V",
    ),
    (
        "r", "s0", "o0", "s1", "m0", "o1", "m1", "o2", "m2", "o3", "m3", "u0", "g0", "c", "u1", "g1", "Q", "u2", "u3",
        "g3", "g2", "K", "V",
    ),
    (
        "o0", "r", "s0", "s1", "m0", "o1", "m1", "o2", "m2", "o3", "m3", "u0", "g0", "c", "u2", "u1", "g1", "Q", "u3",
        "g3", "g2", "K", "V",
    ),
)
DETOURS = ((128, 0, 2, 4), (160, 0, 1, 6), (64, 2, 1, 2))
EARLY_MICRO = 9
HAND_AT, HANDED_AT = 11, 16


def rope_tables(seq_len, head_dim, heads):
    half = head_dim // 2
    inv_freq = (ROPE_BASE ** (-2.0 * np.arange(half) / head_dim)).astype(np.float32)
    angles = np.arange(seq_len, dtype=np.float32)[:, None] * inv_freq[None, :]
    cos = np.tile(np.cos(angles.astype(np.float64)), (1, heads)).astype(np.float32)
    sin = np.tile(np.sin(angles.astype(np.float64)), (1, heads)).astype(np.float32)
    scale = np.float32(head_dim ** -0.5)
    return np.stack([cos * scale, sin * scale, cos, sin])


def head_masks(head_dim, heads):
    half = head_dim // 2
    lanes = np.arange(heads * head_dim)
    roped = np.stack([(lanes % (heads * half)) // half == head for head in range(heads)])
    plain = np.stack([lanes // head_dim == head for head in range(heads)])
    return np.stack([roped, plain]).astype(np.float32)


def dot(lhs, rhs):
    return jnp.dot(lhs, rhs, preferred_element_type=F32)


def layer_norms(x, ln_ref, h_attn, h_mlp):
    x_f32 = x.astype(F32)
    centred = x_f32 - jnp.mean(x_f32, axis=-1, keepdims=True)
    variance = jnp.mean(centred * centred, axis=-1, keepdims=True)
    normed = centred * lax.rsqrt(variance + LN_EPS)
    h_attn[...] = (normed * ln_ref[0:1, :] + ln_ref[1:2, :]).astype(BF16)
    h_mlp[...] = (normed * ln_ref[2:3, :] + ln_ref[3:4, :]).astype(BF16)


def roped(first, second, cos, sin):
    return jnp.concatenate([first * cos - second * sin, second * cos + first * sin], axis=1).astype(BF16)


def causal_softmax(scores, allowed):
    masked = jnp.where(allowed, scores, -1e30)
    weight = jnp.exp(masked - jnp.max(masked, axis=1, keepdims=True))
    return (weight * (1.0 / jnp.sum(weight, axis=1, keepdims=True))).astype(BF16)


def gelu_of_half(half_x):
    return (half_x * (1.0 + lax.erf(half_x * np.float32(2.0 ** 0.5)))).astype(BF16)


def add_layer(heads, shards, h_attn, h_mlp, acc, w_qkv, w_up, w_out, rope, masks, mixed, x=None, y=None, fresh=True, before_last_out=None):
    seq_len, d_model = acc.shape
    width = w_qkv.shape[2] // 3
    half = width // 2
    cols = d_model // heads
    hidden = w_up.shape[2] // heads
    allowed = lax.broadcasted_iota(jnp.int32, (seq_len, seq_len), 0) >= lax.broadcasted_iota(jnp.int32, (seq_len, seq_len), 1)
    values = {}

    def project(turn, name):
        if turn < len(shards):
            which = "qkv".index(name)
            values[name, turn] = dot(h_attn[...], w_qkv[shards[turn], :, which * width:(which + 1) * width])

    def rotate(turn):
        for name, table in (("q", 0), ("k", 2)):
            value = values[name, turn]
            values[name, turn] = roped(value[:, :half], value[:, half:], rope[table], rope[table + 1])

    def score(turn, pair):
        k = values["k", turn]
        k_pair = jnp.concatenate([k * masks[0, h:h + 1, :] for h in (2 * pair, 2 * pair + 1)], axis=0)
        values["s", pair] = lax.dot_general(values["q", turn], k_pair, (((1,), (1,)), ((), ())), preferred_element_type=F32)

    def soften(head):
        side = head % 2 * seq_len
        values["m", head] = causal_softmax(values["s", head // 2][:, side:side + seq_len], allowed)

    def context(turn):
        v = values["v", turn].astype(BF16)
        v_heads = jnp.concatenate([v * masks[1, h:h + 1, :] for h in range(heads)], axis=0)
        probs = jnp.concatenate([values["m", h] for h in range(heads)], axis=1)
        mixed[turn % 2, :, :width] = dot(probs, v_heads).astype(BF16)

    def up(turn, part):
        values["u", part] = dot(h_mlp[...], w_up[shards[turn], :, part * hidden:(part + 1) * hidden])

    def gelu(turn, part):
        mixed[turn % 2, :, width + part * hidden:width + (part + 1) * hidden] = gelu_of_half(values["u", part])

    def add_out(turn, part):
        piece = slice(part * cols, (part + 1) * cols)
        term = dot(mixed[turn % 2], w_out[shards[turn], :, piece])
        if turn > 0 or not fresh:
            term += acc[:, piece]
        if y is not None and turn == len(shards) - 1:
            y[:, piece] = (term + x[:, piece].astype(F32)).astype(BF16)
        else:
            acc[:, piece] = term

    for turn in range(len(shards)):
        for step in FIRST if turn == 0 else LATER[turn - 1]:
            kind, number = step[0], int(step[1:] or 0)
            if kind in "qkv":
                project(turn, kind)
            elif kind in "QKV":
                project(turn + 1, kind.lower())
            elif kind == "r":
                rotate(turn)
            elif kind == "s":
                score(turn, number)
            elif kind == "m":
                soften(number)
            elif kind == "c":
                context(turn)
            elif kind == "u":
                up(turn, number)
            elif kind == "g":
                gelu(turn, number)
            else:
                add_out(turn - 1, number)
    if before_last_out is not None:
        before_last_out()
    for part in range(heads):
        add_out(len(shards) - 1, part)


def kernel(tp_size, pp_size, heads, x_hbm, ln_hbm, wq_hbm, wk_hbm, wv_hbm, wo_hbm, wup_hbm, wdown_hbm, rope_hbm, masks_hbm, out,
           w_qkv, w_up, w_out, raw, detour, xs, ys, ln_half, rope, masks, h_attn, h_mlp, acc, mixed,
           load_sem, w_send, near_recv, far_recv, d_send, d_in, d_out, x_send, x_recv, x_local, x_hand, pp_send, pp_recv, o_send, o_recv):
    me = lax.axis_index("tp")
    stage = lax.axis_index("pp")
    right, left = lax.rem(me + 1, tp_size), lax.rem(me + tp_size - 1, tp_size)
    far = lax.rem(me + 2, tp_size)
    nxt = lax.rem(stage + 1, pp_size)
    last_stage = pp_size - 1
    num_micro, num_seq, seq_len, d_model = xs.shape
    tokens = seq_len // tp_size
    width = raw.shape[1]

    loads = [
        pltpu.make_async_copy(wup_hbm, w_up.at[me], load_sem.at[0]),
        pltpu.make_async_copy(wq_hbm, raw.at[0], load_sem.at[1]),
        pltpu.make_async_copy(wk_hbm, raw.at[1], load_sem.at[2]),
        pltpu.make_async_copy(wv_hbm, raw.at[2], load_sem.at[3]),
        pltpu.make_async_copy(wo_hbm, w_out.at[me, pl.ds(0, width)], load_sem.at[4]),
        pltpu.make_async_copy(wdown_hbm, w_out.at[me, pl.ds(width, wdown_hbm.shape[0])], load_sem.at[5]),
        pltpu.make_async_copy(ln_hbm, ln_half, load_sem.at[6]),
        pltpu.make_async_copy(rope_hbm, rope, load_sem.at[7]),
        pltpu.make_async_copy(masks_hbm, masks, load_sem.at[8]),
    ]
    for load in loads:
        load.start()

    barrier = pltpu.get_barrier_semaphore()

    def knock(index, _):
        peer = {"tp": index // pp_size, "pp": lax.rem(index, pp_size)}
        pl.semaphore_signal(barrier, inc=1, device_id=peer, device_id_type=MESH)
        return 0
    lax.fori_loop(0, tp_size * pp_size, knock, 0)
    pl.semaphore_wait(barrier, tp_size * pp_size)

    def token_rows(owner):
        return pl.ds(pl.multiple_of(owner * tokens, tokens), tokens)

    def seq_rows(owner):
        return pl.ds(owner * num_seq, num_seq)

    early = (stage == last_stage, 0, EARLY_MICRO)
    late = (stage == last_stage - 4, EARLY_MICRO, num_micro - EARLY_MICRO)

    def collect(group):
        micros = pl.ds(group[1], group[2])
        pltpu.make_async_copy(x_hbm.at[micros, seq_rows(me)], ys.at[micros, :, token_rows(me), :], x_local).start()
        for step in range(1, tp_size):
            peer = lax.rem(me + step, tp_size)
            pltpu.make_async_remote_copy(
                src_ref=x_hbm.at[micros, seq_rows(peer)], dst_ref=ys.at[micros, :, token_rows(me), :],
                send_sem=x_send, recv_sem=x_recv, device_id={"tp": peer}, device_id_type=MESH).start()

    def take_blocks(sem, micros, blocks):
        take(sem, ys.at[pl.ds(0, micros), :, pl.ds(0, blocks * tokens), :])

    def hand_on(group):
        take_blocks(x_local, group[2], 1)
        take_blocks(x_recv, group[2], tp_size - 1)

        def one(index, _):
            micro = group[1] + index
            for seq in range(num_seq):
                pltpu.make_async_remote_copy(
                    src_ref=ys.at[micro, seq], dst_ref=xs.at[micro, seq], send_sem=x_hand,
                    recv_sem=pp_recv.at[micro, seq], device_id={"pp": 0}, device_id_type=MESH).start()
            return 0
        lax.fori_loop(0, group[2], one, 0)

    def handed(group):
        take_blocks(x_hand, group[2], tp_size)
        take_blocks(x_send, group[2], tp_size - 1)

    def pp_copy(micro, seq):
        return pltpu.make_async_remote_copy(
            src_ref=ys.at[micro, seq], dst_ref=xs.at[micro, seq], send_sem=pp_send,
            recv_sem=pp_recv.at[micro, seq], device_id={"pp": nxt}, device_id_type=MESH)

    @pl.when(early[0])
    def _():
        collect(early)

    parts = [(w_up, 0, w_up.shape[1], (0, 0)), (w_qkv, 0, w_qkv.shape[1], (0, 0))]
    detour_parts = []
    start = 0
    for rows, first, count, later in DETOURS:
        detour_parts.append((len(detour_parts), pl.ds(start, rows), first, first + count, later))
        parts.append((w_out, start, rows, (first, first + count)))
        start += rows
    parts.append((w_out, start, w_out.shape[1] - start, (0, 0)))
    chunks = [(ref, start + side * rows // 2, rows // 2) for ref, start, rows, _ in parts for side in range(2)]

    def on_ring(part, action):
        first, end = parts[part][3]
        if end > first:
            pl.when((stage < first) | (stage >= end))(action)
        else:
            action()

    def shard_copy(index, owner, send_sem, recv_sem, peer):
        ref, start, rows = chunks[index]
        piece = ref.at[owner, pl.ds(start, rows)]
        return pltpu.make_async_remote_copy(
            src_ref=piece, dst_ref=piece, send_sem=send_sem, recv_sem=recv_sem, device_id={"tp": peer}, device_id_type=MESH)

    def own_copy(index, way):
        return shard_copy(index, me, w_send, near_recv.at[way, index], right if way == 0 else left)

    def near_copy(index, way):
        return shard_copy(index, left if way == 0 else right, w_send, near_recv.at[way, index],
                          right if way == 0 else left)

    def fwd_copy(index):
        way = index % 2
        return shard_copy(index, left if way == 0 else right, w_send, far_recv.at[index // 2],
                          right if way == 0 else left)

    def take(sem, *refs):
        for ref in refs:
            pltpu.make_async_copy(ref, ref, sem).wait()

    def send_own(part):
        def send():
            for way in range(2):
                own_copy(2 * part + way, way).start()
            for way in range(2):
                own_copy(2 * part + 1 - way, way).start()
        on_ring(part, send)

    def pass_on(part):
        def forward():
            for way in range(2):
                near_copy(2 * part + way, way).wait_recv()
                fwd_copy(2 * part + way).start()
        on_ring(part, forward)

    def take_near(part):
        def wait():
            for way in range(2):
                near_copy(2 * part + 1 - way, way).wait_recv()
        on_ring(part, wait)

    def take_far(part):
        ref, start, rows, _ = parts[part]
        on_ring(part, lambda: take(far_recv.at[part], ref.at[far, pl.ds(start, rows)]))

    def send_detours():
        for part, piece, first, end, later in detour_parts:
            @pl.when((stage >= first) & (stage < end))
            def _():
                for step in range(1, tp_size):
                    pltpu.make_async_remote_copy(
                        src_ref=w_out.at[me, piece], dst_ref=detour.at[step - 1, piece],
                        send_sem=w_send, recv_sem=d_in.at[part],
                        device_id={"tp": lax.rem(me + step, tp_size), "pp": stage + later}, device_id_type=MESH).start()

    def pass_detours():
        for part, piece, first, end, later in detour_parts:
            @pl.when((stage >= first + later) & (stage < end + later))
            def _():
                take(d_in.at[part], detour.at[:, piece])
                for step in range(1, tp_size):
                    pltpu.make_async_remote_copy(
                        src_ref=detour.at[step - 1, piece],
                        dst_ref=w_out.at[lax.rem(me + tp_size - step, tp_size), piece],
                        send_sem=d_send.at[part], recv_sem=d_out.at[part],
                        device_id={"pp": stage - later}, device_id_type=MESH).start()

    def take_detours():
        for part, piece, first, end, _ in detour_parts:
            @pl.when((stage >= first) & (stage < end))
            def _():
                take(d_out.at[part], detour.at[:, piece])

    loads[0].wait()
    send_own(0)
    for load in loads[4:6]:
        load.wait()
    send_detours()
    for load in loads[1:4]:
        load.wait()
    head_dim = width // heads
    part = head_dim // 2
    for which in range(3):
        starts = [head * head_dim + side * part for side in range(2) for head in range(heads)]
        if which == 2:
            starts = list(range(0, width, part))
        for col in range(0, d_model, width):
            block = jnp.concatenate([raw[which, start:start + part, col:col + width] for start in starts], axis=0)
            w_qkv[me, col:col + width, which * width:(which + 1) * width] = block.T

    for part in range(1, len(parts)):
        send_own(part)
    for load in loads[6:]:
        load.wait()
    ln_half[2:4, :] = 0.5 * ln_half[2:4, :]
    pass_detours()

    @pl.when(early[0])
    def _():
        hand_on(early)

    for part in range(len(parts)):
        pass_on(part)
    for part in range(len(parts)):
        take_near(part)
    take_detours()

    @pl.when(early[0])
    def _():
        handed(early)

    @pl.when(late[0])
    def _():
        collect(late)

    def put_out(micro, first, count):
        seqs, place = pl.ds(first, count), pl.ds(me * num_seq + first, count)
        out[micro, place] = ys[micro, seqs, token_rows(me), :]
        for step in range(1, tp_size):
            peer = lax.rem(me + step, tp_size)
            pltpu.make_async_remote_copy(
                src_ref=ys.at[micro, seqs, token_rows(peer), :], dst_ref=out.at[micro, place],
                send_sem=o_send, recv_sem=o_recv, device_id={"tp": peer}, device_id_type=MESH).start()

    def hand_over(micro, seq):
        @pl.when(stage < last_stage)
        def _():
            pp_copy(micro, seq).start()

    work = (h_attn, h_mlp, acc, w_qkv, w_up, w_out, rope, masks, mixed)

    pp_copy(0, 0).wait_recv()
    layer_norms(xs[0, 0], ln_half, h_attn, h_mlp)
    add_layer(heads, [me, left, right], *work)
    take_far(0)
    take_far(1)

    def rest_of_far():
        for part in range(2, len(parts)):
            take_far(part)
    add_layer(heads, [far], *work, xs.at[0, 0], ys.at[0, 0], fresh=False, before_last_out=rest_of_far)
    hand_over(0, 0)

    def unit(index, _):
        micro, seq = index // num_seq, lax.rem(index, num_seq)
        pp_copy(micro, seq).wait_recv()

        @pl.when(seq == 0)
        def _():
            put_out(micro - 1, 0, num_seq)

        @pl.when(index == num_micro * num_seq - 1)
        def _():
            put_out(num_micro - 1, 0, num_seq - 1)

        layer_norms(xs[micro, seq], ln_half, h_attn, h_mlp)
        add_layer(heads, list(range(tp_size)), *work, xs.at[micro, seq], ys.at[micro, seq])
        hand_over(micro, seq)

        @pl.when(late[0])
        def _():
            pl.when(index == HAND_AT)(lambda: hand_on(late))
            pl.when(index == HANDED_AT)(lambda: handed(late))
        return 0

    lax.fori_loop(1, num_micro * num_seq, unit, 0)
    put_out(num_micro - 1, num_seq - 1, 1)

    take(w_send, w_out, w_up)

    for part, piece, first, end, later in detour_parts:
        @pl.when((stage >= first + later) & (stage < end + later))
        def _():
            take(d_send.at[part], detour.at[:, piece])

    @pl.when(stage < last_stage)
    def _():
        take(pp_send, ys)
    take_blocks(o_send, num_micro, tp_size - 1)
    take_blocks(o_recv, num_micro, tp_size - 1)


def solution(mesh):
    tp_size, pp_size = mesh.shape["tp"], mesh.shape["pp"]

    def stage_body(x_in, ln_params, w_q, w_k, w_v, w_o, w_up, w_down):
        num_micro, batch, tokens, d_model = x_in.shape
        heads, head_dim = w_k.shape[2:]
        width = heads * head_dim
        hidden = w_up.shape[2]
        seq_len = tokens * tp_size
        num_seq = batch // tp_size
        rope = jnp.asarray(rope_tables(seq_len, head_dim, heads))
        masks = jnp.asarray(head_masks(head_dim, heads), dtype=BF16)
        wq_t = jnp.transpose(w_q[0], (1, 2, 3, 0)).reshape(width, d_model)
        wk_t = jnp.transpose(w_k[0], (1, 2, 0)).reshape(width, d_model)
        wv_t = jnp.transpose(w_v[0], (1, 2, 0)).reshape(width, d_model)
        vmem = pl.BlockSpec(memory_space=pltpu.VMEM)
        hbm = pl.BlockSpec(memory_space=pl.ANY)
        dma = pltpu.SemaphoreType.DMA
        out = pl.pallas_call(
            functools.partial(kernel, tp_size, pp_size, heads),
            out_shape=pltpu.VMEM(x_in.shape, BF16),
            in_specs=[hbm] * 10,
            out_specs=vmem,
            scratch_shapes=[
                pltpu.VMEM((tp_size, d_model, 3 * width), BF16),
                pltpu.VMEM((tp_size, d_model, hidden), BF16),
                pltpu.VMEM((tp_size, width + hidden, d_model), BF16),
                pltpu.VMEM((3, width, d_model), BF16),
                pltpu.VMEM((tp_size - 1, sum(rows for rows, *_ in DETOURS), d_model), BF16),
                pltpu.VMEM((num_micro, num_seq, seq_len, d_model), BF16),
                pltpu.VMEM((num_micro, num_seq, seq_len, d_model), BF16),
                pltpu.VMEM((4, d_model), F32),
                pltpu.VMEM(rope.shape, F32),
                pltpu.VMEM(masks.shape, BF16),
                pltpu.VMEM((seq_len, d_model), BF16),
                pltpu.VMEM((seq_len, d_model), BF16),
                pltpu.VMEM((seq_len, d_model), F32),
                pltpu.VMEM((2, seq_len, width + hidden), BF16),
                dma((9,)), dma, dma((2, 12)), dma((6,)), dma((3,)), dma((3,)), dma((3,)), dma, dma, dma, dma, dma, dma((num_micro, num_seq)), dma, dma,
            ],
            compiler_params=pltpu.CompilerParams(
                collective_id=0, has_side_effects=True, vmem_limit_bytes=54 * 1024 * 1024),
            name="stage",
        )(x_in, ln_params[0], wq_t, wk_t, wv_t, w_o[0].reshape(width, d_model), w_up[0], w_down[0], rope, masks)
        return out[None]

    in_specs = (P(None, "dp", "tp", None), P("pp", None, None), P("pp", None, "tp", None, None), P("pp", None, "tp", None), P("pp", None, "tp", None), P("pp", "tp", None, None, None), P("pp", None, "tp"), P("pp", "tp", None))
    return jax.shard_map(stage_body, mesh=mesh, in_specs=in_specs, out_specs=P("pp", None, "dp", "tp", None), check_vma=False)
```

```python
import functools

import jax
import jax.numpy as jnp
import numpy as np
from jax import lax
from jax.experimental import pallas as pl
from jax.experimental.pallas import tpu as pltpu
from jax.sharding import PartitionSpec as P

LN_EPS = 1e-5
ROPE_BASE = 10000.0
F32, BF16 = jnp.float32, jnp.bfloat16
MESH = pl.DeviceIdType.MESH
DETOURS = ((128, 0, 2, 4), (160, 0, 1, 6), (64, 2, 1, 2))
EARLY_MICRO = 9
HAND_AT = 10


def rope_tables(seq_len, head_dim, heads):
    half = head_dim // 2
    inv_freq = (ROPE_BASE ** (-2.0 * np.arange(half) / head_dim)).astype(np.float32)
    angles = np.arange(seq_len, dtype=np.float32)[:, None] * inv_freq[None, :]
    cos = np.tile(np.cos(angles.astype(np.float64)), (1, heads)).astype(np.float32)
    sin = np.tile(np.sin(angles.astype(np.float64)), (1, heads)).astype(np.float32)
    scale = np.float32(head_dim ** -0.5)
    return np.stack([cos * scale, sin * scale, cos, sin])


def head_masks(head_dim, heads):
    half = head_dim // 2
    lanes = np.arange(heads * head_dim)
    roped = np.stack([(lanes % (heads * half)) // half == head for head in range(heads)])
    plain = np.stack([lanes // head_dim == head for head in range(heads)])
    return np.stack([roped, plain]).astype(np.float32)


def dot(lhs, rhs):
    return jnp.dot(lhs, rhs, preferred_element_type=F32)


def layer_norms(x, ln_ref, h_attn, h_mlp):
    x_f32 = x.astype(F32)
    centred = x_f32 - jnp.mean(x_f32, axis=-1, keepdims=True)
    variance = jnp.mean(centred * centred, axis=-1, keepdims=True)
    normed = centred * lax.rsqrt(variance + LN_EPS)
    h_attn[...] = (normed * ln_ref[0:1, :] + ln_ref[1:2, :]).astype(BF16)
    h_mlp[...] = (normed * ln_ref[2:3, :] + ln_ref[3:4, :]).astype(BF16)


def roped(first, second, cos, sin):
    return jnp.concatenate([first * cos - second * sin, second * cos + first * sin], axis=1).astype(BF16)


def causal_softmax(scores, allowed):
    masked = jnp.where(allowed, scores, -1e30)
    weight = jnp.exp(masked - jnp.max(masked, axis=1, keepdims=True))
    return (weight * (1.0 / jnp.sum(weight, axis=1, keepdims=True))).astype(BF16)


def gelu_of_half(half_x):
    return (half_x * (1.0 + lax.erf(half_x * np.float32(2.0 ** 0.5)))).astype(BF16)


def add_layer(heads, shards, h_attn, h_mlp, acc, w_qkv, w_up, w_out, rope, masks, mixed, x=None, y=None, fresh=True, before_last_out=None):
    seq_len, d_model = acc.shape
    width = w_qkv.shape[2] // 3
    half = width // 2
    cols = d_model // heads
    hidden = w_up.shape[2] // heads
    allowed = lax.broadcasted_iota(jnp.int32, (seq_len, seq_len), 0) >= lax.broadcasted_iota(jnp.int32, (seq_len, seq_len), 1)
    raw, ups, score_pairs, probs = {}, {}, {}, {}

    def project(turn, which):
        if turn < len(shards):
            raw[which] = dot(h_attn[...], w_qkv[shards[turn], :, which * width:(which + 1) * width])

    def score(pair):
        k_pair = jnp.concatenate([raw[1] * masks[0, h:h + 1, :] for h in (2 * pair, 2 * pair + 1)], axis=0)
        score_pairs[pair] = lax.dot_general(raw[0], k_pair, (((1,), (1,)), ((), ())), preferred_element_type=F32)

    def soften(head):
        side = head % 2 * seq_len
        probs[head] = causal_softmax(score_pairs[head // 2][:, side:side + seq_len], allowed)

    def context(turn):
        v_heads = jnp.concatenate([v * masks[1, h:h + 1, :] for h in range(heads)], axis=0)
        mixed[turn % 2, :, :width] = dot(jnp.concatenate([probs[h] for h in range(heads)], axis=1), v_heads).astype(BF16)

    def up(turn, part):
        ups[part] = dot(h_mlp[...], w_up[shards[turn], :, part * hidden:(part + 1) * hidden])

    def gelu(turn, part):
        mixed[turn % 2, :, width + part * hidden:width + (part + 1) * hidden] = gelu_of_half(ups[part])

    def add_out(turn, part):
        piece = slice(part * cols, (part + 1) * cols)
        term = dot(mixed[turn % 2], w_out[shards[turn], :, piece])
        if turn > 0 or not fresh:
            term += acc[:, piece]
        if y is not None and turn == len(shards) - 1:
            y[:, piece] = (term + x[:, piece].astype(F32)).astype(BF16)
        else:
            acc[:, piece] = term

    for which in range(3):
        project(0, which)
    for turn in range(len(shards)):
        raw[0] = roped(raw[0][:, :half], raw[0][:, half:], rope[0], rope[1])
        raw[1] = roped(raw[1][:, :half], raw[1][:, half:], rope[2], rope[3])
        v = raw[2].astype(BF16)
        score(0)
        if turn == 0:
            score(1)
            for head in range(heads):
                up(turn, head)
                if head > 0:
                    gelu(turn, head - 1)
                soften(head)
            project(turn + 1, 0)
            project(turn + 1, 1)
            gelu(turn, 3)
            context(turn)
            project(turn + 1, 2)
        else:
            add_out(turn - 1, 0)
            score(1)
            for head in range(heads):
                soften(head)
                if head < 3:
                    add_out(turn - 1, head + 1)
            up(turn, 0)
            up(turn, 1)
            gelu(turn, 0)
            context(turn)
            up(turn, 2)
            gelu(turn, 1)
            up(turn, 3)
            gelu(turn, 2)
            project(turn + 1, 0)
            gelu(turn, 3)
            project(turn + 1, 1)
            project(turn + 1, 2)
    if before_last_out is not None:
        before_last_out()
    for part in range(heads):
        add_out(len(shards) - 1, part)


def kernel(tp_size, pp_size, heads, x_hbm, ln_hbm, wq_hbm, wk_hbm, wv_hbm, wo_hbm, wup_hbm, wdown_hbm, rope_hbm, masks_hbm, out,
           w_qkv, w_up, w_out, raw, detour, xs, ys, ln_half, rope, masks, h_attn, h_mlp, acc, mixed,
           load_sem, w_send, near_recv, far_recv, d_send, d_in, d_out, x_send, x_recv, x_local, x_hand, pp_send, pp_recv, o_send, o_recv):
    me = lax.axis_index("tp")
    stage = lax.axis_index("pp")
    right, left = lax.rem(me + 1, tp_size), lax.rem(me + tp_size - 1, tp_size)
    far = lax.rem(me + 2, tp_size)
    nxt = lax.rem(stage + 1, pp_size)
    last_stage = pp_size - 1
    num_micro, num_seq, seq_len, d_model = xs.shape
    tokens = seq_len // tp_size
    width = raw.shape[1]

    loads = [
        pltpu.make_async_copy(wup_hbm, w_up.at[me], load_sem.at[0]),
        pltpu.make_async_copy(wq_hbm, raw.at[0], load_sem.at[1]),
        pltpu.make_async_copy(wk_hbm, raw.at[1], load_sem.at[2]),
        pltpu.make_async_copy(wv_hbm, raw.at[2], load_sem.at[3]),
        pltpu.make_async_copy(wo_hbm, w_out.at[me, pl.ds(0, width)], load_sem.at[4]),
        pltpu.make_async_copy(wdown_hbm, w_out.at[me, pl.ds(width, wdown_hbm.shape[0])], load_sem.at[5]),
        pltpu.make_async_copy(ln_hbm, ln_half, load_sem.at[6]),
        pltpu.make_async_copy(rope_hbm, rope, load_sem.at[7]),
        pltpu.make_async_copy(masks_hbm, masks, load_sem.at[8]),
    ]
    for load in loads:
        load.start()

    barrier = pltpu.get_barrier_semaphore()

    def knock(index, _):
        peer = {"tp": index // pp_size, "pp": lax.rem(index, pp_size)}
        pl.semaphore_signal(barrier, inc=1, device_id=peer, device_id_type=MESH)
        return 0
    lax.fori_loop(0, tp_size * pp_size, knock, 0)
    pl.semaphore_wait(barrier, tp_size * pp_size)

    def token_rows(owner):
        return pl.ds(pl.multiple_of(owner * tokens, tokens), tokens)

    def seq_rows(owner):
        return pl.ds(owner * num_seq, num_seq)

    early = (stage == last_stage, 0, EARLY_MICRO)
    late = (stage == last_stage - 4, EARLY_MICRO, num_micro - EARLY_MICRO)

    def collect(group):
        micros = pl.ds(group[1], group[2])
        pltpu.make_async_copy(x_hbm.at[micros, seq_rows(me)], ys.at[micros, :, token_rows(me), :], x_local).start()
        for step in range(1, tp_size):
            peer = lax.rem(me + step, tp_size)
            pltpu.make_async_remote_copy(
                src_ref=x_hbm.at[micros, seq_rows(peer)], dst_ref=ys.at[micros, :, token_rows(me), :],
                send_sem=x_send, recv_sem=x_recv, device_id={"tp": peer}, device_id_type=MESH).start()

    def take_blocks(sem, micros, blocks):
        take(sem, ys.at[pl.ds(0, micros), :, pl.ds(0, blocks * tokens), :])

    def hand_on(group):
        take_blocks(x_local, group[2], 1)
        take_blocks(x_recv, group[2], tp_size - 1)

        def one(index, _):
            micro = group[1] + index
            for seq in range(num_seq):
                pltpu.make_async_remote_copy(
                    src_ref=ys.at[micro, seq], dst_ref=xs.at[micro, seq], send_sem=x_hand.at[micro],
                    recv_sem=pp_recv.at[micro, seq], device_id={"pp": 0}, device_id_type=MESH).start()
            return 0
        lax.fori_loop(0, group[2], one, 0)

    def handed(micro):
        take(x_hand.at[micro], ys.at[micro])

    def pp_copy(micro, seq):
        return pltpu.make_async_remote_copy(
            src_ref=ys.at[micro, seq], dst_ref=xs.at[micro, seq], send_sem=pp_send,
            recv_sem=pp_recv.at[micro, seq], device_id={"pp": nxt}, device_id_type=MESH)

    @pl.when(early[0])
    def _():
        collect(early)

    parts = [(w_up, 0, w_up.shape[1], (0, 0)), (w_qkv, 0, w_qkv.shape[1], (0, 0))]
    detour_parts = []
    start = 0
    for rows, first, count, later in DETOURS:
        detour_parts.append((len(detour_parts), pl.ds(start, rows), first, first + count, later))
        parts.append((w_out, start, rows, (first, first + count)))
        start += rows
    parts.append((w_out, start, w_out.shape[1] - start, (0, 0)))
    chunks = [(ref, start + side * rows // 2, rows // 2) for ref, start, rows, _ in parts for side in range(2)]

    def on_ring(part, action):
        first, end = parts[part][3]
        if end > first:
            pl.when((stage < first) | (stage >= end))(action)
        else:
            action()

    def shard_copy(index, owner, send_sem, recv_sem, peer):
        ref, start, rows = chunks[index]
        piece = ref.at[owner, pl.ds(start, rows)]
        return pltpu.make_async_remote_copy(
            src_ref=piece, dst_ref=piece, send_sem=send_sem, recv_sem=recv_sem, device_id={"tp": peer}, device_id_type=MESH)

    def own_copy(index, way):
        return shard_copy(index, me, w_send, near_recv.at[way, index], right if way == 0 else left)

    def near_copy(index, way):
        return shard_copy(index, left if way == 0 else right, w_send, near_recv.at[way, index],
                          right if way == 0 else left)

    def fwd_copy(index):
        way = index % 2
        return shard_copy(index, left if way == 0 else right, w_send, far_recv.at[index // 2],
                          right if way == 0 else left)

    def take(sem, *refs):
        for ref in refs:
            pltpu.make_async_copy(ref, ref, sem).wait()

    def send_own(part):
        def send():
            for way in range(2):
                own_copy(2 * part + way, way).start()
            for way in range(2):
                own_copy(2 * part + 1 - way, way).start()
        on_ring(part, send)

    def pass_on(part):
        def forward():
            for way in range(2):
                near_copy(2 * part + way, way).wait_recv()
                fwd_copy(2 * part + way).start()
        on_ring(part, forward)

    def take_near(part):
        def wait():
            for way in range(2):
                near_copy(2 * part + 1 - way, way).wait_recv()
        on_ring(part, wait)

    def take_far(part):
        ref, start, rows, _ = parts[part]
        on_ring(part, lambda: take(far_recv.at[part], ref.at[far, pl.ds(start, rows)]))

    def send_detours():
        for part, piece, first, end, later in detour_parts:
            @pl.when((stage >= first) & (stage < end))
            def _():
                for step in range(1, tp_size):
                    pltpu.make_async_remote_copy(
                        src_ref=w_out.at[me, piece], dst_ref=detour.at[step - 1, piece],
                        send_sem=w_send, recv_sem=d_in.at[part],
                        device_id={"tp": lax.rem(me + step, tp_size), "pp": stage + later}, device_id_type=MESH).start()

    def pass_detours():
        for part, piece, first, end, later in detour_parts:
            @pl.when((stage >= first + later) & (stage < end + later))
            def _():
                take(d_in.at[part], detour.at[:, piece])
                for step in range(1, tp_size):
                    pltpu.make_async_remote_copy(
                        src_ref=detour.at[step - 1, piece],
                        dst_ref=w_out.at[lax.rem(me + tp_size - step, tp_size), piece],
                        send_sem=d_send.at[part], recv_sem=d_out.at[part],
                        device_id={"pp": stage - later}, device_id_type=MESH).start()

    def take_detours():
        for part, piece, first, end, _ in detour_parts:
            @pl.when((stage >= first) & (stage < end))
            def _():
                take(d_out.at[part], detour.at[:, piece])

    loads[0].wait()
    send_own(0)
    for load in loads[4:6]:
        load.wait()
    send_detours()
    for load in loads[1:4]:
        load.wait()
    head_dim = width // heads
    part = head_dim // 2
    for which in range(3):
        starts = [head * head_dim + side * part for side in range(2) for head in range(heads)]
        if which == 2:
            starts = list(range(0, width, part))
        for col in range(0, d_model, width):
            block = jnp.concatenate([raw[which, start:start + part, col:col + width] for start in starts], axis=0)
            w_qkv[me, col:col + width, which * width:(which + 1) * width] = block.T

    for part in range(1, len(parts)):
        send_own(part)
    for load in loads[6:]:
        load.wait()
    ln_half[2:4, :] = 0.5 * ln_half[2:4, :]
    pass_detours()

    @pl.when(early[0])
    def _():
        hand_on(early)

    for part in range(len(parts)):
        pass_on(part)
    for part in range(len(parts)):
        take_near(part)
    take_detours()

    @pl.when(early[0])
    def _():
        for micro in range(EARLY_MICRO):
            handed(micro)

    @pl.when(late[0])
    def _():
        collect(late)

    def o_copy(micro, seq, step):
        peer = lax.rem(me + step, tp_size)
        return pltpu.make_async_remote_copy(
            src_ref=ys.at[micro, seq, token_rows(peer), :], dst_ref=out.at[micro, me * num_seq + seq],
            send_sem=o_send, recv_sem=o_recv, device_id={"tp": peer}, device_id_type=MESH)

    def hand_over(micro, seq):
        @pl.when(stage < last_stage)
        def _():
            pp_copy(micro, seq).start()

    def put_out(micro, seq):
        out[micro, me * num_seq + seq] = ys[micro, seq, token_rows(me), :]
        for step in range(1, tp_size):
            o_copy(micro, seq, step).start()

    work = (h_attn, h_mlp, acc, w_qkv, w_up, w_out, rope, masks, mixed)

    pp_copy(0, 0).wait_recv()
    layer_norms(xs[0, 0], ln_half, h_attn, h_mlp)
    add_layer(heads, [me, left, right], *work)
    take_far(0)
    take_far(1)

    def rest_of_far():
        for part in range(2, len(parts)):
            take_far(part)
    add_layer(heads, [far], *work, xs.at[0, 0], ys.at[0, 0], fresh=False, before_last_out=rest_of_far)
    hand_over(0, 0)

    def unit(index, _):
        micro, seq = index // num_seq, lax.rem(index, num_seq)
        pp_copy(micro, seq).wait_recv()
        put_out((index - 1) // num_seq, lax.rem(index - 1, num_seq))
        layer_norms(xs[micro, seq], ln_half, h_attn, h_mlp)
        add_layer(heads, list(range(tp_size)), *work, xs.at[micro, seq], ys.at[micro, seq])
        hand_over(micro, seq)

        @pl.when(late[0])
        def _():
            pl.when(index == HAND_AT)(lambda: hand_on(late))
            pl.when((seq == num_seq - 1) & (micro >= EARLY_MICRO - 1) & (micro < num_micro - 1))(lambda: handed(micro + 1))
        return 0

    lax.fori_loop(1, num_micro * num_seq, unit, 0)
    put_out(num_micro - 1, num_seq - 1)

    take(w_send, w_out, w_up)

    for part, piece, first, end, later in detour_parts:
        @pl.when((stage >= first + later) & (stage < end + later))
        def _():
            take(d_send.at[part], detour.at[:, piece])

    for group in (early, late):
        @pl.when(group[0])
        def _():
            take_blocks(x_send, group[2], tp_size - 1)

    @pl.when(stage < last_stage)
    def _():
        take(pp_send, ys)
    take_blocks(o_send, num_micro, tp_size - 1)
    take_blocks(o_recv, num_micro, tp_size - 1)


def solution(mesh):
    tp_size, pp_size = mesh.shape["tp"], mesh.shape["pp"]

    def stage_body(x_in, ln_params, w_q, w_k, w_v, w_o, w_up, w_down):
        num_micro, batch, tokens, d_model = x_in.shape
        heads, head_dim = w_k.shape[2:]
        width = heads * head_dim
        hidden = w_up.shape[2]
        seq_len = tokens * tp_size
        num_seq = batch // tp_size
        rope = jnp.asarray(rope_tables(seq_len, head_dim, heads))
        masks = jnp.asarray(head_masks(head_dim, heads), dtype=BF16)
        wq_t = jnp.transpose(w_q[0], (1, 2, 3, 0)).reshape(width, d_model)
        wk_t = jnp.transpose(w_k[0], (1, 2, 0)).reshape(width, d_model)
        wv_t = jnp.transpose(w_v[0], (1, 2, 0)).reshape(width, d_model)
        vmem = pl.BlockSpec(memory_space=pltpu.VMEM)
        hbm = pl.BlockSpec(memory_space=pl.ANY)
        dma = pltpu.SemaphoreType.DMA
        out = pl.pallas_call(
            functools.partial(kernel, tp_size, pp_size, heads),
            out_shape=pltpu.VMEM(x_in.shape, BF16),
            in_specs=[hbm] * 10,
            out_specs=vmem,
            scratch_shapes=[
                pltpu.VMEM((tp_size, d_model, 3 * width), BF16),
                pltpu.VMEM((tp_size, d_model, hidden), BF16),
                pltpu.VMEM((tp_size, width + hidden, d_model), BF16),
                pltpu.VMEM((3, width, d_model), BF16),
                pltpu.VMEM((tp_size - 1, sum(rows for rows, *_ in DETOURS), d_model), BF16),
                pltpu.VMEM((num_micro, num_seq, seq_len, d_model), BF16),
                pltpu.VMEM((num_micro, num_seq, seq_len, d_model), BF16),
                pltpu.VMEM((4, d_model), F32),
                pltpu.VMEM(rope.shape, F32),
                pltpu.VMEM(masks.shape, BF16),
                pltpu.VMEM((seq_len, d_model), BF16),
                pltpu.VMEM((seq_len, d_model), BF16),
                pltpu.VMEM((seq_len, d_model), F32),
                pltpu.VMEM((2, seq_len, width + hidden), BF16),
                dma((9,)), dma, dma((2, 12)), dma((6,)), dma((3,)), dma((3,)), dma((3,)), dma, dma, dma, dma((num_micro,)), dma, dma((num_micro, num_seq)), dma, dma,
            ],
            compiler_params=pltpu.CompilerParams(
                collective_id=0, has_side_effects=True, vmem_limit_bytes=54 * 1024 * 1024),
            name="stage",
        )(x_in, ln_params[0], wq_t, wk_t, wv_t, w_o[0].reshape(width, d_model), w_up[0], w_down[0], rope, masks)
        return out[None]

    in_specs = (P(None, "dp", "tp", None), P("pp", None, None), P("pp", None, "tp", None, None), P("pp", None, "tp", None), P("pp", None, "tp", None), P("pp", "tp", None, None, None), P("pp", None, "tp"), P("pp", "tp", None))
    return jax.shard_map(stage_body, mesh=mesh, in_specs=in_specs, out_specs=P("pp", None, "dp", "tp", None), check_vma=False)
```

```python
import functools

import jax
import jax.numpy as jnp
import numpy as np
from jax import lax
from jax.experimental import pallas as pl
from jax.experimental.pallas import tpu as pltpu
from jax.sharding import PartitionSpec as P

LN_EPS = 1e-5
ROPE_BASE = 10000.0
F32, BF16 = jnp.float32, jnp.bfloat16
MESH = pl.DeviceIdType.MESH
DETOURS = ((128, 0, 2, 4), (160, 0, 1, 6), (64, 2, 1, 2))
EARLY_MICRO = 9
HAND_AT = 10


def rope_tables(seq_len, head_dim, heads):
    half = head_dim // 2
    inv_freq = (ROPE_BASE ** (-2.0 * np.arange(half) / head_dim)).astype(np.float32)
    angles = np.arange(seq_len, dtype=np.float32)[:, None] * inv_freq[None, :]
    cos = np.tile(np.cos(angles.astype(np.float64)), (1, heads)).astype(np.float32)
    sin = np.tile(np.sin(angles.astype(np.float64)), (1, heads)).astype(np.float32)
    scale = np.float32(head_dim ** -0.5)
    return np.stack([cos * scale, sin * scale, cos, sin])


def head_masks(head_dim, heads):
    half = head_dim // 2
    lanes = np.arange(heads * head_dim)
    roped, plain = lanes % (heads * half) // half, lanes // head_dim
    rows = [roped // 2 == 0, roped // 2 == 1, roped % 2 == 0, roped % 2 == 1, plain % 2 == 0, plain % 2 == 1]
    return np.stack(rows).astype(np.float32)


def dot(lhs, rhs):
    return jnp.dot(lhs, rhs, preferred_element_type=F32)


def layer_norms(x, ln_ref, h_attn, h_mlp):
    x_f32 = x.astype(F32)
    centred = x_f32 - jnp.mean(x_f32, axis=-1, keepdims=True)
    variance = jnp.mean(centred * centred, axis=-1, keepdims=True)
    normed = centred * lax.rsqrt(variance + LN_EPS)
    h_attn[...] = (normed * ln_ref[0:1, :] + ln_ref[1:2, :]).astype(BF16)
    h_mlp[...] = (normed * ln_ref[2:3, :] + ln_ref[3:4, :]).astype(BF16)


def roped(first, second, cos, sin):
    return jnp.concatenate([first * cos - second * sin, second * cos + first * sin], axis=1).astype(BF16)


def causal_softmax(scores, allowed):
    masked = jnp.where(allowed, scores, -1e30)
    weight = jnp.exp(masked - jnp.max(masked, axis=1, keepdims=True))
    return (weight * (1.0 / jnp.sum(weight, axis=1, keepdims=True))).astype(BF16)


def gelu_of_half(half_x):
    return (half_x * (1.0 + lax.erf(half_x * np.float32(2.0 ** 0.5)))).astype(BF16)


def add_layer(heads, shards, h_attn, h_mlp, acc, w_qkv, w_up, w_out, rope, masks, mixed, x=None, y=None, fresh=True, before_last_out=None):
    seq_len, d_model = acc.shape
    width = w_qkv.shape[2] // 3
    half = width // 2
    cols = d_model // heads
    hidden = w_up.shape[2] // heads
    allowed = lax.broadcasted_iota(jnp.int32, (seq_len, seq_len), 0) >= lax.broadcasted_iota(jnp.int32, (seq_len, seq_len), 1)
    raw, ups, score_pairs, probs = {}, {}, {}, {}

    def project(turn, which):
        if turn < len(shards):
            raw[which] = dot(h_attn[...], w_qkv[shards[turn], :, which * width:(which + 1) * width])

    def two(value, mask):
        return jnp.concatenate([value * masks[mask:mask + 1, :], value * masks[mask + 1:mask + 2, :]], axis=0)

    def score():
        pairs = lax.dot_general(two(raw[0], 0), two(raw[1], 2), (((1,), (1,)), ((), ())), preferred_element_type=F32)
        score_pairs[0], score_pairs[1] = pairs[:seq_len], pairs[seq_len:]

    def soften(head):
        side = head % 2 * seq_len
        probs[head] = causal_softmax(score_pairs[head // 2][:, side:side + seq_len], allowed)

    def context(turn):
        pairs = jnp.concatenate([jnp.concatenate([probs[h], probs[h + 1]], axis=1) for h in (0, 2)], axis=0)
        both = dot(pairs, two(v, 4))
        mixed[turn % 2, :, :half] = both[:seq_len, :half].astype(BF16)
        mixed[turn % 2, :, half:width] = both[seq_len:, half:].astype(BF16)

    def up(turn, part):
        ups[part] = dot(h_mlp[...], w_up[shards[turn], :, part * hidden:(part + 1) * hidden])

    def gelu(turn, part):
        mixed[turn % 2, :, width + part * hidden:width + (part + 1) * hidden] = gelu_of_half(ups[part])

    def add_out(turn, part):
        piece = slice(part * cols, (part + 1) * cols)
        term = dot(mixed[turn % 2], w_out[shards[turn], :, piece])
        if turn > 0 or not fresh:
            term += acc[:, piece]
        if y is not None and turn == len(shards) - 1:
            y[:, piece] = (term + x[:, piece].astype(F32)).astype(BF16)
        else:
            acc[:, piece] = term

    for which in range(3):
        project(0, which)
    for turn in range(len(shards)):
        raw[0] = roped(raw[0][:, :half], raw[0][:, half:], rope[0], rope[1])
        raw[1] = roped(raw[1][:, :half], raw[1][:, half:], rope[2], rope[3])
        v = raw[2].astype(BF16)
        score()
        if turn == 0:
            for head in range(heads):
                up(turn, head)
                if head > 0:
                    gelu(turn, head - 1)
                soften(head)
            project(turn + 1, 0)
            project(turn + 1, 1)
            gelu(turn, 3)
            context(turn)
            project(turn + 1, 2)
        else:
            add_out(turn - 1, 0)
            for head in range(heads):
                soften(head)
                if head < 3:
                    add_out(turn - 1, head + 1)
            up(turn, 0)
            up(turn, 1)
            gelu(turn, 0)
            context(turn)
            up(turn, 2)
            gelu(turn, 1)
            up(turn, 3)
            gelu(turn, 2)
            project(turn + 1, 0)
            gelu(turn, 3)
            project(turn + 1, 1)
            project(turn + 1, 2)
    if before_last_out is not None:
        before_last_out()
    for part in range(heads):
        add_out(len(shards) - 1, part)


def kernel(tp_size, pp_size, heads, x_hbm, ln_hbm, wq_hbm, wk_hbm, wv_hbm, wo_hbm, wup_hbm, wdown_hbm, rope_hbm, masks_hbm, out,
           w_qkv, w_up, w_out, raw, detour, xs, ys, ln_half, rope, masks, h_attn, h_mlp, acc, mixed,
           load_sem, w_send, near_recv, far_recv, d_send, d_in, d_out, x_send, x_recv, x_local, x_hand, pp_send, pp_recv, o_send, o_recv):
    me = lax.axis_index("tp")
    stage = lax.axis_index("pp")
    right, left = lax.rem(me + 1, tp_size), lax.rem(me + tp_size - 1, tp_size)
    far = lax.rem(me + 2, tp_size)
    nxt = lax.rem(stage + 1, pp_size)
    last_stage = pp_size - 1
    num_micro, num_seq, seq_len, d_model = xs.shape
    tokens = seq_len // tp_size
    width = raw.shape[1]

    loads = [
        pltpu.make_async_copy(wup_hbm, w_up.at[me], load_sem.at[0]),
        pltpu.make_async_copy(wq_hbm, raw.at[0], load_sem.at[1]),
        pltpu.make_async_copy(wk_hbm, raw.at[1], load_sem.at[2]),
        pltpu.make_async_copy(wv_hbm, raw.at[2], load_sem.at[3]),
        pltpu.make_async_copy(wo_hbm, w_out.at[me, pl.ds(0, width)], load_sem.at[4]),
        pltpu.make_async_copy(wdown_hbm, w_out.at[me, pl.ds(width, wdown_hbm.shape[0])], load_sem.at[5]),
        pltpu.make_async_copy(ln_hbm, ln_half, load_sem.at[6]),
        pltpu.make_async_copy(rope_hbm, rope, load_sem.at[7]),
        pltpu.make_async_copy(masks_hbm, masks, load_sem.at[8]),
    ]
    for load in loads:
        load.start()

    barrier = pltpu.get_barrier_semaphore()

    def knock(index, _):
        peer = {"tp": index // pp_size, "pp": lax.rem(index, pp_size)}
        pl.semaphore_signal(barrier, inc=1, device_id=peer, device_id_type=MESH)
        return 0
    lax.fori_loop(0, tp_size * pp_size, knock, 0)
    pl.semaphore_wait(barrier, tp_size * pp_size)

    def token_rows(owner):
        return pl.ds(pl.multiple_of(owner * tokens, tokens), tokens)

    def seq_rows(owner):
        return pl.ds(owner * num_seq, num_seq)

    early = (stage == last_stage, 0, EARLY_MICRO)
    late = (stage == last_stage - 4, EARLY_MICRO, num_micro - EARLY_MICRO)

    def collect(group):
        micros = pl.ds(group[1], group[2])
        pltpu.make_async_copy(x_hbm.at[micros, seq_rows(me)], ys.at[micros, :, token_rows(me), :], x_local).start()
        for step in range(1, tp_size):
            peer = lax.rem(me + step, tp_size)
            pltpu.make_async_remote_copy(
                src_ref=x_hbm.at[micros, seq_rows(peer)], dst_ref=ys.at[micros, :, token_rows(me), :],
                send_sem=x_send, recv_sem=x_recv, device_id={"tp": peer}, device_id_type=MESH).start()

    def take_blocks(sem, micros, blocks):
        take(sem, ys.at[pl.ds(0, micros), :, pl.ds(0, blocks * tokens), :])

    def hand_on(group):
        take_blocks(x_local, group[2], 1)
        take_blocks(x_recv, group[2], tp_size - 1)

        def one(index, _):
            micro = group[1] + index
            for seq in range(num_seq):
                pltpu.make_async_remote_copy(
                    src_ref=ys.at[micro, seq], dst_ref=xs.at[micro, seq], send_sem=x_hand.at[micro],
                    recv_sem=pp_recv.at[micro, seq], device_id={"pp": 0}, device_id_type=MESH).start()
            return 0
        lax.fori_loop(0, group[2], one, 0)

    def handed(micro):
        take(x_hand.at[micro], ys.at[micro])

    def pp_copy(micro, seq):
        return pltpu.make_async_remote_copy(
            src_ref=ys.at[micro, seq], dst_ref=xs.at[micro, seq], send_sem=pp_send,
            recv_sem=pp_recv.at[micro, seq], device_id={"pp": nxt}, device_id_type=MESH)

    @pl.when(early[0])
    def _():
        collect(early)

    parts = [(w_up, 0, w_up.shape[1], (0, 0)), (w_qkv, 0, w_qkv.shape[1], (0, 0))]
    detour_parts = []
    start = 0
    for rows, first, count, later in DETOURS:
        detour_parts.append((len(detour_parts), pl.ds(start, rows), first, first + count, later))
        parts.append((w_out, start, rows, (first, first + count)))
        start += rows
    parts.append((w_out, start, w_out.shape[1] - start, (0, 0)))
    chunks = [(ref, start + side * rows // 2, rows // 2) for ref, start, rows, _ in parts for side in range(2)]

    def on_ring(part, action):
        first, end = parts[part][3]
        if end > first:
            pl.when((stage < first) | (stage >= end))(action)
        else:
            action()

    def shard_copy(index, owner, send_sem, recv_sem, peer):
        ref, start, rows = chunks[index]
        piece = ref.at[owner, pl.ds(start, rows)]
        return pltpu.make_async_remote_copy(
            src_ref=piece, dst_ref=piece, send_sem=send_sem, recv_sem=recv_sem, device_id={"tp": peer}, device_id_type=MESH)

    def own_copy(index, way):
        return shard_copy(index, me, w_send, near_recv.at[way, index], right if way == 0 else left)

    def near_copy(index, way):
        return shard_copy(index, left if way == 0 else right, w_send, near_recv.at[way, index],
                          right if way == 0 else left)

    def fwd_copy(index):
        way = index % 2
        return shard_copy(index, left if way == 0 else right, w_send, far_recv.at[index // 2],
                          right if way == 0 else left)

    def take(sem, *refs):
        for ref in refs:
            pltpu.make_async_copy(ref, ref, sem).wait()

    def send_own(part):
        def send():
            for way in range(2):
                own_copy(2 * part + way, way).start()
            for way in range(2):
                own_copy(2 * part + 1 - way, way).start()
        on_ring(part, send)

    def pass_on(part):
        def forward():
            for way in range(2):
                near_copy(2 * part + way, way).wait_recv()
                fwd_copy(2 * part + way).start()
        on_ring(part, forward)

    def take_near(part):
        def wait():
            for way in range(2):
                near_copy(2 * part + 1 - way, way).wait_recv()
        on_ring(part, wait)

    def take_far(part):
        ref, start, rows, _ = parts[part]
        on_ring(part, lambda: take(far_recv.at[part], ref.at[far, pl.ds(start, rows)]))

    def send_detours():
        for part, piece, first, end, later in detour_parts:
            @pl.when((stage >= first) & (stage < end))
            def _():
                for step in range(1, tp_size):
                    pltpu.make_async_remote_copy(
                        src_ref=w_out.at[me, piece], dst_ref=detour.at[step - 1, piece],
                        send_sem=w_send, recv_sem=d_in.at[part],
                        device_id={"tp": lax.rem(me + step, tp_size), "pp": stage + later}, device_id_type=MESH).start()

    def pass_detours():
        for part, piece, first, end, later in detour_parts:
            @pl.when((stage >= first + later) & (stage < end + later))
            def _():
                take(d_in.at[part], detour.at[:, piece])
                for step in range(1, tp_size):
                    pltpu.make_async_remote_copy(
                        src_ref=detour.at[step - 1, piece],
                        dst_ref=w_out.at[lax.rem(me + tp_size - step, tp_size), piece],
                        send_sem=d_send.at[part], recv_sem=d_out.at[part],
                        device_id={"pp": stage - later}, device_id_type=MESH).start()

    def take_detours():
        for part, piece, first, end, _ in detour_parts:
            @pl.when((stage >= first) & (stage < end))
            def _():
                take(d_out.at[part], detour.at[:, piece])

    loads[0].wait()
    send_own(0)
    for load in loads[4:6]:
        load.wait()
    send_detours()
    for load in loads[1:4]:
        load.wait()
    head_dim = width // heads
    part = head_dim // 2
    for which in range(3):
        starts = [head * head_dim + side * part for side in range(2) for head in range(heads)]
        if which == 2:
            starts = list(range(0, width, part))
        for col in range(0, d_model, width):
            block = jnp.concatenate([raw[which, start:start + part, col:col + width] for start in starts], axis=0)
            w_qkv[me, col:col + width, which * width:(which + 1) * width] = block.T

    for part in range(1, len(parts)):
        send_own(part)
    for load in loads[6:]:
        load.wait()
    ln_half[2:4, :] = 0.5 * ln_half[2:4, :]
    pass_detours()

    @pl.when(early[0])
    def _():
        hand_on(early)

    for part in range(len(parts)):
        pass_on(part)
    for part in range(len(parts)):
        take_near(part)
    take_detours()

    @pl.when(early[0])
    def _():
        for micro in range(EARLY_MICRO):
            handed(micro)

    @pl.when(late[0])
    def _():
        collect(late)

    def o_copy(micro, seq, step):
        peer = lax.rem(me + step, tp_size)
        return pltpu.make_async_remote_copy(
            src_ref=ys.at[micro, seq, token_rows(peer), :], dst_ref=out.at[micro, me * num_seq + seq],
            send_sem=o_send, recv_sem=o_recv, device_id={"tp": peer}, device_id_type=MESH)

    def hand_over(micro, seq):
        @pl.when(stage < last_stage)
        def _():
            pp_copy(micro, seq).start()

    def put_out(micro, seq):
        out[micro, me * num_seq + seq] = ys[micro, seq, token_rows(me), :]
        for step in range(1, tp_size):
            o_copy(micro, seq, step).start()

    work = (h_attn, h_mlp, acc, w_qkv, w_up, w_out, rope, masks, mixed)

    pp_copy(0, 0).wait_recv()
    layer_norms(xs[0, 0], ln_half, h_attn, h_mlp)
    add_layer(heads, [me, left, right], *work)
    take_far(0)
    take_far(1)

    def rest_of_far():
        for part in range(2, len(parts)):
            take_far(part)
    add_layer(heads, [far], *work, xs.at[0, 0], ys.at[0, 0], fresh=False, before_last_out=rest_of_far)
    hand_over(0, 0)

    def unit(index, _):
        micro, seq = index // num_seq, lax.rem(index, num_seq)
        pp_copy(micro, seq).wait_recv()
        put_out((index - 1) // num_seq, lax.rem(index - 1, num_seq))
        layer_norms(xs[micro, seq], ln_half, h_attn, h_mlp)
        add_layer(heads, list(range(tp_size)), *work, xs.at[micro, seq], ys.at[micro, seq])
        hand_over(micro, seq)

        @pl.when(late[0])
        def _():
            pl.when(index == HAND_AT)(lambda: hand_on(late))
            pl.when((seq == num_seq - 1) & (micro >= EARLY_MICRO - 1) & (micro < num_micro - 1))(lambda: handed(micro + 1))
        return 0

    lax.fori_loop(1, num_micro * num_seq, unit, 0)
    put_out(num_micro - 1, num_seq - 1)

    take(w_send, w_out, w_up)

    for part, piece, first, end, later in detour_parts:
        @pl.when((stage >= first + later) & (stage < end + later))
        def _():
            take(d_send.at[part], detour.at[:, piece])

    for group in (early, late):
        @pl.when(group[0])
        def _():
            take_blocks(x_send, group[2], tp_size - 1)

    @pl.when(stage < last_stage)
    def _():
        take(pp_send, ys)
    take_blocks(o_send, num_micro, tp_size - 1)
    take_blocks(o_recv, num_micro, tp_size - 1)


def solution(mesh):
    tp_size, pp_size = mesh.shape["tp"], mesh.shape["pp"]

    def stage_body(x_in, ln_params, w_q, w_k, w_v, w_o, w_up, w_down):
        num_micro, batch, tokens, d_model = x_in.shape
        heads, head_dim = w_k.shape[2:]
        width = heads * head_dim
        hidden = w_up.shape[2]
        seq_len = tokens * tp_size
        num_seq = batch // tp_size
        rope = jnp.asarray(rope_tables(seq_len, head_dim, heads))
        masks = jnp.asarray(head_masks(head_dim, heads), dtype=BF16)
        wq_t = jnp.transpose(w_q[0], (1, 2, 3, 0)).reshape(width, d_model)
        wk_t = jnp.transpose(w_k[0], (1, 2, 0)).reshape(width, d_model)
        wv_t = jnp.transpose(w_v[0], (1, 2, 0)).reshape(width, d_model)
        vmem = pl.BlockSpec(memory_space=pltpu.VMEM)
        hbm = pl.BlockSpec(memory_space=pl.ANY)
        dma = pltpu.SemaphoreType.DMA
        out = pl.pallas_call(
            functools.partial(kernel, tp_size, pp_size, heads),
            out_shape=pltpu.VMEM(x_in.shape, BF16),
            in_specs=[hbm] * 10,
            out_specs=vmem,
            scratch_shapes=[
                pltpu.VMEM((tp_size, d_model, 3 * width), BF16),
                pltpu.VMEM((tp_size, d_model, hidden), BF16),
                pltpu.VMEM((tp_size, width + hidden, d_model), BF16),
                pltpu.VMEM((3, width, d_model), BF16),
                pltpu.VMEM((tp_size - 1, sum(rows for rows, *_ in DETOURS), d_model), BF16),
                pltpu.VMEM((num_micro, num_seq, seq_len, d_model), BF16),
                pltpu.VMEM((num_micro, num_seq, seq_len, d_model), BF16),
                pltpu.VMEM((4, d_model), F32),
                pltpu.VMEM(rope.shape, F32),
                pltpu.VMEM(masks.shape, BF16),
                pltpu.VMEM((seq_len, d_model), BF16),
                pltpu.VMEM((seq_len, d_model), BF16),
                pltpu.VMEM((seq_len, d_model), F32),
                pltpu.VMEM((2, seq_len, width + hidden), BF16),
                dma((9,)), dma, dma((2, 12)), dma((6,)), dma((3,)), dma((3,)), dma((3,)), dma, dma, dma, dma((num_micro,)), dma, dma((num_micro, num_seq)), dma, dma,
            ],
            compiler_params=pltpu.CompilerParams(
                collective_id=0, has_side_effects=True, vmem_limit_bytes=54 * 1024 * 1024),
            name="stage",
        )(x_in, ln_params[0], wq_t, wk_t, wv_t, w_o[0].reshape(width, d_model), w_up[0], w_down[0], rope, masks)
        return out[None]

    in_specs = (P(None, "dp", "tp", None), P("pp", None, None), P("pp", None, "tp", None, None), P("pp", None, "tp", None), P("pp", None, "tp", None), P("pp", "tp", None, None, None), P("pp", None, "tp"), P("pp", "tp", None))
    return jax.shard_map(stage_body, mesh=mesh, in_specs=in_specs, out_specs=P("pp", None, "dp", "tp", None), check_vma=False)
```
